32 devices in a mesh: dp: 1 (over z), cp: 32 (over y, x, core).
Axes of the slice: x: 4, y: 4, z: 1, core: 2. Of those that a mesh axis runs over, the one named last changes fastest.
The devices are a block of a 4x4x8 slice.
Arguments:
- query: bfloat16 [2, 1024, 32, 256], P('dp', 'cp')
- key: bfloat16 [2, 1024, 256], P('dp', 'cp')
- value: bfloat16 [2, 1024, 256], P('dp', 'cp')
- positions: int32 [1024], P(('dp', 'cp'))
- grad_out: bfloat16 [2, 1024, 32, 256], P('dp', 'cp')
Outputs:
- output 1: bfloat16 [2, 1024, 32, 256], P('dp', 'cp')
- output 2: bfloat16 [2, 1024, 32, 256], P('dp', 'cp')
- output 3: bfloat16 [2, 1024, 256], P('dp', 'cp')
- output 4: bfloat16 [2, 1024, 256], P('dp', 'cp')
All inputs are finite; a program needn't handle non-finite values.
Results may differ from the reference program's by a relative error of at most 0.00819063.
Values are sent between devices in bfloat16 or wider.
A program may use at most 768 MiB of HBM per device.

```python
import jax
import jax.numpy as jnp
from jax import lax

BATCH = 2
SEQ = 1024
HEADS = 32
HEAD = 256
QROWS = 8
ROPE_BASE = 10000


def setup_inputs(seed: int = 0, part: int = 0) -> dict:
    part_key = jax.random.fold_in(jax.random.key(seed), part)
    rng_keys = jax.random.split(part_key, 6)
    query = jax.random.normal(rng_keys[0], (BATCH, SEQ, HEADS, HEAD), jnp.float32)
    key = jax.random.normal(rng_keys[1], (BATCH, SEQ, HEAD), jnp.float32)
    value = jax.random.normal(rng_keys[2], (BATCH, SEQ, HEAD), jnp.float32)
    start = jax.random.randint(rng_keys[3], (), 0, 256)
    increments = jax.random.randint(rng_keys[4], (SEQ,), 0, 2)
    positions = (start + jnp.cumsum(increments)).astype(jnp.int32)
    grad_out = jax.random.normal(rng_keys[5], (BATCH, SEQ, HEADS, HEAD), jnp.float32)
    return {'query': query.astype(jnp.bfloat16), 'key': key.astype(jnp.bfloat16), 'value': value.astype(jnp.bfloat16), 'positions': positions, 'grad_out': grad_out.astype(jnp.bfloat16)}


def rope_tables(positions):
    half_dim = HEAD // 2
    inv_freq = jnp.power(jnp.float32(ROPE_BASE), -2.0 * jnp.arange(half_dim, dtype=jnp.float32) / HEAD)
    angles = positions.astype(jnp.float32)[..., None] * inv_freq
    angles = jnp.concatenate([angles, angles], axis=-1)
    return jnp.cos(angles), jnp.sin(angles)


def rotate(values, cos_tab, sin_tab):
    half_dim = values.shape[-1] // 2
    turned = jnp.concatenate([-values[..., half_dim:], values[..., :half_dim]], axis=-1)
    return values * cos_tab + turned * sin_tab


def reference(query, key, value, positions, grad_out):
    cos_tab, sin_tab = rope_tables(positions)
    cos_q = cos_tab[None, :, None, :]
    sin_q = sin_tab[None, :, None, :]
    query_rot = rotate(query.astype(jnp.float32), cos_q, sin_q).astype(jnp.bfloat16)
    key_rot = rotate(key.astype(jnp.float32), cos_tab[None], sin_tab[None]).astype(jnp.bfloat16)
    scale = HEAD ** -0.5
    key_f = key_rot.astype(jnp.float32)
    value_f = value.astype(jnp.float32)
    key_idx = jnp.arange(SEQ)
    block_count = SEQ // QROWS
    query_blocks = query_rot.reshape(BATCH, block_count, QROWS, HEADS, HEAD).transpose(1, 0, 2, 3, 4)
    grad_blocks = grad_out.reshape(BATCH, block_count, QROWS, HEADS, HEAD).transpose(1, 0, 2, 3, 4)

    def one_block(carry, block):
        dkey_acc, dvalue_acc = carry
        query_blk, grad_blk, block_idx = block
        query_f = query_blk.astype(jnp.float32)
        grad_f = grad_blk.astype(jnp.float32)
        query_idx = block_idx * QROWS + jnp.arange(QROWS)
        causal_mask = (key_idx[None, :] <= query_idx[:, None])[None, :, None, :]
        scores = jnp.where(causal_mask, jnp.einsum('bqhd,bkd->bqhk', query_f, key_f) * scale, -jnp.inf)
        row_max = jnp.max(scores, axis=-1, keepdims=True)
        weights = jnp.exp(scores - row_max)
        row_sum = jnp.sum(weights, axis=-1, keepdims=True)
        attn_f = jnp.einsum('bqhk,bkd->bqhd', weights.astype(jnp.bfloat16).astype(jnp.float32), value_f) / row_sum
        attn_blk = attn_f.astype(jnp.bfloat16)
        probs_f = jnp.exp(scores - (row_max + jnp.log(row_sum)))
        delta = jnp.sum(grad_f * attn_blk.astype(jnp.float32), axis=-1, keepdims=True)
        dprobs = jnp.einsum('bqhd,bkd->bqhk', grad_f, value_f)
        dscore = (probs_f * (dprobs - delta)).astype(jnp.bfloat16).astype(jnp.float32)
        dquery_blk = jnp.einsum('bqhk,bkd->bqhd', dscore, key_f) * scale
        dkey_acc = dkey_acc + jnp.einsum('bqhk,bqhd->bkd', dscore, query_f) * scale
        dvalue_acc = dvalue_acc + jnp.einsum('bqhk,bqhd->bkd', probs_f.astype(jnp.bfloat16).astype(jnp.float32), grad_f)
        return (dkey_acc, dvalue_acc), (attn_blk, dquery_blk)

    zero_kv = jnp.zeros((BATCH, SEQ, HEAD), jnp.float32)
    sums, outs = lax.scan(one_block, (zero_kv, zero_kv), (query_blocks, grad_blocks, jnp.arange(block_count)))
    attn_out = outs[0].transpose(1, 0, 2, 3, 4).reshape(BATCH, SEQ, HEADS, HEAD)
    dquery_rot = outs[1].transpose(1, 0, 2, 3, 4).reshape(BATCH, SEQ, HEADS, HEAD)
    grad_query = rotate(dquery_rot, cos_q, -sin_q).astype(jnp.bfloat16)
    grad_key = rotate(sums[0], cos_tab[None], -sin_tab[None]).astype(jnp.bfloat16)
    grad_value = sums[1].astype(jnp.bfloat16)
    return (attn_out, grad_query, grad_key, grad_value)
```

```python
import functools
import math

import jax
import jax.numpy as jnp
from jax import lax
from jax.experimental import pallas as pl
from jax.experimental.pallas import tpu as pltpu
from jax.sharding import PartitionSpec as P

ROPE_BASE = 10000
CORES = 2
LOG2E = math.log2(math.e)


def rope_tables(positions, head):
    half_dim = head // 2
    inv_freq = jnp.power(jnp.float32(ROPE_BASE), -2.0 * jnp.arange(half_dim, dtype=jnp.float32) / head)
    angles = positions.astype(jnp.float32)[..., None] * inv_freq
    return jnp.cos(angles), jnp.sin(angles)


def rot_halves(x1, x2, c, s):
    return x1 * c - x2 * s, x2 * c + x1 * s


def kernel(side, tokens, heads, head,
           tab_in, key_in, val_in, q_hbm, do_hbm,
           out_hbm, dq_hbm, gk_hbm, gv_hbm,
           tabs, qbuf, dobuf, kst, kbuf, vbuf, sbuf, dpbuf, dsbuf, pbf, rinv, delta, obuf, dqbuf,
           dk_part, dv_part, rk, rv, vsum, rvy, ksum, rkx, gkb, gvb,
           sem_loc, sem_px_s, sem_px_r, sem_kx, sem_ky, sem_vy, sem_vx,
           sem_dv_s, sem_dv_r, sem_dk_s, sem_dk_r, sem_dvy_s, sem_dvy_r, sem_dkx_s, sem_dkx_r,
           sem_o_s, sem_o_r):
    n = side
    half = head // 2
    blk = CORES * tokens
    tile = n * blk
    nrow = tokens * heads
    scale = head ** -0.5
    me = lax.axis_index('cp')
    k = lax.rem(me, CORES)
    chip = lax.div(me, CORES)
    x = lax.rem(chip, n)
    y = lax.div(chip, n)
    other = 1 - k

    def dev(yy, xx, kk):
        return (yy * n + xx) * CORES + kk

    partner = dev(y, x, other)

    def rcopy(src, dst, ssem, rsem, target):
        return pltpu.make_async_remote_copy(src_ref=src, dst_ref=dst, send_sem=ssem, recv_sem=rsem,
                                            device_id={'cp': target}, device_id_type=pl.DeviceIdType.MESH)

    lq = pltpu.make_async_copy(q_hbm.at[k], qbuf.at[k], sem_loc.at[0])
    ld = pltpu.make_async_copy(do_hbm.at[k], dobuf.at[k], sem_loc.at[1])
    lq.start()
    ld.start()

    bar = pltpu.get_barrier_semaphore()
    peers = [partner]
    for d in range(1, n):
        peers.append(dev(y, lax.rem(x + d, n), k))
        peers.append(dev(lax.rem(y + d, n), x, k))
    for p in peers:
        pl.semaphore_signal(bar, inc=1, device_id={'cp': p}, device_id_type=pl.DeviceIdType.MESH)

    c_own = tab_in[0]
    s_own = tab_in[1]
    for b in range(CORES):
        kf = key_in[b].astype(jnp.float32)
        r1, r2 = rot_halves(kf[:, :half], kf[:, half:], c_own, s_own)
        kst[b, :, :half] = r1.astype(jnp.bfloat16)
        kst[b, :, half:] = r2.astype(jnp.bfloat16)
    tabs[k] = tab_in[...]
    mine = pl.ds(pl.multiple_of(x * blk + k * tokens, tokens), tokens)
    kbuf[y, mine] = kst[k]
    vbuf[y, mine] = val_in[k]
    pl.semaphore_wait(bar, len(peers))

    pk = rcopy(kst.at[other], kbuf.at[y, mine], sem_px_s.at[0], sem_px_r.at[0], partner)
    pv = rcopy(val_in.at[other], vbuf.at[y, mine], sem_px_s.at[1], sem_px_r.at[1], partner)
    pt = rcopy(tab_in, tabs.at[k], sem_px_s.at[2], sem_px_r.at[2], partner)
    pq = rcopy(q_hbm.at[other], qbuf.at[k], sem_px_s.at[3], sem_px_r.at[3], partner)
    pd = rcopy(do_hbm.at[other], dobuf.at[k], sem_px_s.at[4], sem_px_r.at[4], partner)
    for cp in (pk, pv, pt, pq, pd):
        cp.start()
    pk.wait_recv()
    pv.wait_recv()

    def blk_at(i):
        return pl.ds(pl.multiple_of(i * blk, blk), blk)

    xs = blk_at(x)
    kx = []
    vx0 = []
    for d in range(1, n):
        xt = lax.rem(x + d, n)
        kx.append(rcopy(kbuf.at[y, xs], kbuf.at[y, xs], sem_kx.at[0, d - 1], sem_kx.at[1, d - 1], dev(y, xt, k)))
        vx0.append(rcopy(vbuf.at[y, xs], vbuf.at[y, xs], sem_vx.at[0, 0, d - 1], sem_vx.at[1, 0, d - 1], dev(y, xt, k)))
    for cp in kx:
        cp.start()

    def vy_copy(d):
        yt = lax.rem(y + d, n)
        return rcopy(vbuf.at[y, xs], vbuf.at[y, xs], sem_vy.at[0, d - 1], sem_vy.at[1, d - 1], dev(yt, x, k))

    def ky_copy(d):
        yt = lax.rem(y + d, n)
        return rcopy(kbuf.at[y], kbuf.at[y], sem_ky.at[0, d - 1], sem_ky.at[1, d - 1], dev(yt, x, k))

    def vx_copy(dy, d):
        ys = lax.rem(y - dy + n, n)
        xt = lax.rem(x + d, n)
        return rcopy(vbuf.at[ys, xs], vbuf.at[ys, xs], sem_vx.at[0, dy, d - 1], sem_vx.at[1, dy, d - 1], dev(y, xt, k))

    for d in range(1, n):
        @pl.when(y + d < n)
        def _(d=d):
            vy_copy(d).start()
    for cp in vx0:
        cp.start()
    for cp in kx:
        cp.wait_recv()
    for d in range(1, n):
        @pl.when(y + d < n)
        def _(d=d):
            ky_copy(d).start()
    for d in range(1, n):
        @pl.when(y - d >= 0)
        def _(d=d):
            vy_copy(d).wait_recv()
            for e in range(1, n):
                vx_copy(d, e).start()

    pt.wait_recv()
    lq.wait()
    pq.wait_recv()
    def rotate_rows(tok, carry):
        for s in range(CORES):
            rows = pl.ds(pl.multiple_of(tok * heads, heads), heads)
            c = tabs[s, 0, pl.ds(tok, 1), :]
            sn = tabs[s, 1, pl.ds(tok, 1), :]
            qf = qbuf[s, rows, :].astype(jnp.float32)
            r1, r2 = rot_halves(qf[:, :half], qf[:, half:], c, sn)
            qbuf[s, rows, :half] = r1.astype(jnp.bfloat16)
            qbuf[s, rows, half:] = r2.astype(jnp.bfloat16)
        return carry
    lax.fori_loop(0, tokens, rotate_rows, 0, unroll=4)
    ld.wait()
    pd.wait_recv()

    nt = (((1,), (1,)), ((), ()))
    tn = (((0,), (0,)), ((), ()))
    f32 = jnp.float32

    for d in range(n):
        t = lax.rem(y - d + n, n)

        @pl.when(y - d >= 0)
        def _(d=d, t=t):
            if d > 0:
                ky_copy(d).wait_recv()
            for e in range(1, n):
                vx_copy(d, e).wait_recv()
            for s in range(CORES):
                sc = lax.dot_general(qbuf[s], kbuf[t], nt, preferred_element_type=f32)
                if d == 0:
                    row_tok = (x * CORES + s) * tokens + lax.broadcasted_iota(jnp.int32, sc.shape, 0) // heads
                    sc = jnp.where(lax.broadcasted_iota(jnp.int32, sc.shape, 1) <= row_tok, sc, -jnp.inf)
                sbuf[t, s] = sc
                dpbuf[t, s] = lax.dot_general(dobuf[s], vbuf[t], nt, preferred_element_type=f32)

        if d > 0:
            @pl.when(y - d < 0)
            def _(t=t):
                sbuf[t] = jnp.full(sbuf.shape[1:], -jnp.inf, f32)
                dpbuf[t] = jnp.zeros(dpbuf.shape[1:], f32)
                kbuf[t] = jnp.zeros(kbuf.shape[1:], jnp.bfloat16)
                vbuf[t] = jnp.zeros(vbuf.shape[1:], jnp.bfloat16)

    rc = 256
    for s in range(CORES):
        def fwd_rows(i, carry, s=s):
            rows = pl.ds(pl.multiple_of(i * rc, rc), rc)
            sc = [sbuf[t, s, rows, :] for t in range(n)]
            mx = sc[0]
            for t in range(1, n):
                mx = jnp.maximum(mx, sc[t])
            mx = jnp.max(mx, axis=1, keepdims=True)
            tot = None
            acc = None
            for t in range(n):
                p = jnp.exp2((sc[t] - mx) * (scale * LOG2E))
                sbuf[t, s, rows, :] = p
                tot = p if tot is None else tot + p
                o = jnp.dot(p.astype(jnp.bfloat16), vbuf[t], preferred_element_type=f32)
                acc = o if acc is None else acc + o
            tot = jnp.sum(tot, axis=1, keepdims=True)
            inv = 1.0 / tot
            ob = (acc * inv).astype(jnp.bfloat16)
            obuf[s, rows, :] = ob
            dl = jnp.sum(ob.astype(f32) * dobuf[s, rows, :].astype(f32), axis=1, keepdims=True)
            rinv[s, rows, :] = jnp.broadcast_to(inv, (rc, 128))
            delta[s, rows, :] = jnp.broadcast_to(dl, (rc, 128))
            return carry
        lax.fori_loop(0, nrow // rc, fwd_rows, 0)

    oloc = pltpu.make_async_copy(obuf.at[k], out_hbm.at[k], sem_loc.at[2])
    orem = rcopy(obuf.at[other], out_hbm.at[k], sem_o_s.at[0], sem_o_r.at[0], partner)
    oloc.start()
    orem.start()

    def dv_copy(t, d):
        xt = lax.rem(x + d, n)
        return rcopy(dv_part.at[t, blk_at(xt)], rv.at[d - 1, t], sem_dv_s.at[t, d - 1], sem_dv_r.at[t, d - 1], dev(y, xt, k))

    def dk_copy(d):
        t = lax.rem(y - d + n, n)
        return rcopy(dk_part.at[t], rk.at[d - 1], sem_dk_s.at[d - 1], sem_dk_r.at[d - 1], dev(t, x, k))

    for t in range(n):
        for s in range(CORES):
            def bwd_rows(i, carry, s=s, t=t):
                rows = pl.ds(pl.multiple_of(i * rc, rc), rc)
                iv = rinv[s, rows, :1]
                dl = delta[s, rows, :1]
                p = sbuf[t, s, rows, :] * iv
                ds = p * (dpbuf[t, s, rows, :] - dl)
                pbf[s, rows, :] = p.astype(jnp.bfloat16)
                dsbuf[t, s, rows, :] = ds.astype(jnp.bfloat16)
                return carry
            lax.fori_loop(0, nrow // rc, bwd_rows, 0)
        dva = None
        dka = None
        for s in range(CORES):
            a = lax.dot_general(pbf[s], dobuf[s], tn, preferred_element_type=f32)
            dva = a if dva is None else dva + a
        dv_part[t] = dva

        @pl.when(y >= t)
        def _(t=t):
            for d in range(1, n):
                dv_copy(t, d).start()
        for s in range(CORES):
            a = lax.dot_general(dsbuf[t, s], qbuf[s], tn, preferred_element_type=f32)
            dka = a if dka is None else dka + a
        dk_part[t] = dka * scale

        for d in range(1, n):
            @pl.when(y == t + d)
            def _(d=d):
                dk_copy(d).start()

    for s in range(CORES):
        def dq_rows(i, carry, s=s):
            rows = pl.ds(pl.multiple_of(i * rc, rc), rc)
            acc = None
            for t in range(n):
                a = jnp.dot(dsbuf[t, s, rows, :], kbuf[t], preferred_element_type=f32)
                acc = a if acc is None else acc + a
            acc = acc * scale
            for j in range(rc // heads):
                tok = i * (rc // heads) + j
                c = tabs[s, 0, pl.ds(tok, 1), :]
                sn = tabs[s, 1, pl.ds(tok, 1), :]
                g = acc[j * heads:(j + 1) * heads]
                r1, r2 = rot_halves(g[:, :half], g[:, half:], c, -sn)
                orow = pl.ds(pl.multiple_of(tok * heads, heads), heads)
                dqbuf[s, orow, :half] = r1.astype(jnp.bfloat16)
                dqbuf[s, orow, half:] = r2.astype(jnp.bfloat16)
            return carry
        lax.fori_loop(0, nrow // rc, dq_rows, 0)
    qloc = pltpu.make_async_copy(dqbuf.at[k], dq_hbm.at[k], sem_loc.at[3])
    qrem = rcopy(dqbuf.at[other], dq_hbm.at[k], sem_o_s.at[1], sem_o_r.at[1], partner)
    qloc.start()
    qrem.start()

    def dvy_copy(d):
        t = lax.rem(y - d + n, n)
        return rcopy(vsum.at[t], rvy.at[d - 1], sem_dvy_s.at[d - 1], sem_dvy_r.at[d - 1], dev(t, x, k))

    def dkx_copy(d):
        xt = lax.rem(x + d, n)
        return rcopy(ksum.at[blk_at(xt)], rkx.at[d - 1], sem_dkx_s.at[d - 1], sem_dkx_r.at[d - 1], dev(y, xt, k))

    for t in range(n):
        @pl.when(y >= t)
        def _(t=t):
            acc = dv_part[t, xs, :]
            for d in range(1, n):
                dv_copy(t, d).wait_recv()
                acc = acc + rv[d - 1, t]
            vsum[t] = acc
        for d in range(1, n):
            @pl.when(y == t + d)
            def _(d=d):
                dvy_copy(d).start()

    ksum[...] = dk_part[y]
    for d in range(1, n):
        @pl.when(y + d < n)
        def _(d=d):
            dk_copy(d).wait_recv()
            ksum[...] += rk[d - 1]
    for d in range(1, n):
        dkx_copy(d).start()

    rvsum = vsum.at[y]
    for d in range(1, n):
        @pl.when(y + d < n)
        def _(d=d):
            dvy_copy(d).wait_recv()
            vsum[y] += rvy[d - 1]
    gv = vsum[y]
    gk = ksum[xs, :]
    for d in range(1, n):
        dkx_copy(d).wait_recv()
        gk = gk + rkx[d - 1]
    for s in range(CORES):
        gvb[s] = gv[s * tokens:(s + 1) * tokens].astype(jnp.bfloat16)
        g = gk[s * tokens:(s + 1) * tokens]
        r1, r2 = rot_halves(g[:, :half], g[:, half:], tabs[s, 0], -tabs[s, 1])
        gkb[s, :, :half] = r1.astype(jnp.bfloat16)
        gkb[s, :, half:] = r2.astype(jnp.bfloat16)
    gkl = pltpu.make_async_copy(gkb.at[k], gk_hbm.at[k], sem_loc.at[4])
    gvl = pltpu.make_async_copy(gvb.at[k], gv_hbm.at[k], sem_loc.at[5])
    gkr = rcopy(gkb.at[other], gk_hbm.at[k], sem_o_s.at[2], sem_o_r.at[2], partner)
    gvr = rcopy(gvb.at[other], gv_hbm.at[k], sem_o_s.at[3], sem_o_r.at[3], partner)
    for cp in (gkl, gvl, gkr, gvr):
        cp.start()

    for cp in (pk, pv, pt, pq, pd):
        cp.wait_send()
    for cp in kx + vx0:
        cp.wait_send()
    for d in range(1, n):
        @pl.when(y + d < n)
        def _(d=d):
            vy_copy(d).wait_send()
            ky_copy(d).wait_send()

        @pl.when(y - d >= 0)
        def _(d=d):
            for e in range(1, n):
                vx_copy(d, e).wait_send()
            dk_copy(d).wait_send()
            dvy_copy(d).wait_send()
        dkx_copy(d).wait_send()
    for t in range(n):
        @pl.when(y >= t)
        def _(t=t):
            for d in range(1, n):
                dv_copy(t, d).wait_send()
    for cp in (oloc, qloc, gkl, gvl):
        cp.wait()
    for cp in (orem, qrem, gkr, gvr):
        cp.wait()


def solution(mesh):
    cp_size = mesh.shape['cp']
    side = math.isqrt(cp_size // CORES)
    query_spec = P('dp', 'cp', None, None)
    kv_spec = P('dp', 'cp', None)
    pos_spec = P(('dp', 'cp'))

    def per_device(query, key, value, positions, grad_out):
        batch, tokens, heads, head = query.shape
        nrow = tokens * heads
        tab = jnp.stack(rope_tables(positions, head))
        q2 = query.reshape(batch, nrow, head)
        d2 = grad_out.reshape(batch, nrow, head)
        n = side
        blk = CORES * tokens
        tile = n * blk
        bf16, f32 = jnp.bfloat16, jnp.float32
        V = pltpu.VMEM
        D = pltpu.SemaphoreType.DMA
        scratch = [
            V((CORES, 2, tokens, head // 2), f32),
            V((CORES, nrow, head), bf16),
            V((CORES, nrow, head), bf16),
            V((CORES, tokens, head), bf16),
            V((n, tile, head), bf16),
            V((n, tile, head), bf16),
            V((n, CORES, nrow, tile), f32),
            V((n, CORES, nrow, tile), f32),
            V((n, CORES, nrow, tile), bf16),
            V((CORES, nrow, tile), bf16),
            V((CORES, nrow, 128), f32),
            V((CORES, nrow, 128), f32),
            V((CORES, nrow, head), bf16),
            V((CORES, nrow, head), bf16),
            V((n, tile, head), f32),
            V((n, tile, head), f32),
            V((n - 1, tile, head), f32),
            V((n - 1, n, blk, head), f32),
            V((n, blk, head), f32),
            V((n - 1, blk, head), f32),
            V((tile, head), f32),
            V((n - 1, blk, head), f32),
            V((CORES, tokens, head), bf16),
            V((CORES, tokens, head), bf16),
            D((6,)), D((5,)), D((5,)),
            D((2, n - 1)), D((2, n - 1)), D((2, n - 1)), D((2, n, n - 1)),
            D((n, n - 1)), D((n, n - 1)), D((n - 1,)), D((n - 1,)),
            D((n - 1,)), D((n - 1,)), D((n - 1,)), D((n - 1,)),
            D((4,)), D((4,)),
        ]
        vmem = pl.BlockSpec(memory_space=pltpu.VMEM)
        hbm = pl.BlockSpec(memory_space=pl.ANY)
        out, dq, gk, gv = pl.pallas_call(
            functools.partial(kernel, side, tokens, heads, head),
            out_shape=[jax.ShapeDtypeStruct(q2.shape, bf16), jax.ShapeDtypeStruct(q2.shape, bf16),
                       jax.ShapeDtypeStruct(key.shape, bf16), jax.ShapeDtypeStruct(key.shape, bf16)],
            in_specs=[vmem, vmem, vmem, hbm, hbm],
            out_specs=[hbm, hbm, hbm, hbm],
            scratch_shapes=scratch,
            compiler_params=pltpu.CompilerParams(collective_id=0, has_side_effects=True,
                                                 vmem_limit_bytes=60 * 1024 * 1024),
        )(tab, key, value, q2, d2)
        return out.reshape(query.shape), dq.reshape(query.shape), gk, gv

    return jax.shard_map(per_device, mesh=mesh, in_specs=(query_spec, kv_spec, kv_spec, pos_spec, query_spec),
                         out_specs=(query_spec, query_spec, kv_spec, kv_spec), check_vma=False)
```

```python
import functools
import math

import jax
import jax.numpy as jnp
from jax import lax
from jax.experimental import pallas as pl
from jax.experimental.pallas import tpu as pltpu
from jax.sharding import PartitionSpec as P

ROPE_BASE = 10000
CORES = 2
SIDE = 4
LOG2E = math.log2(math.e)
TILE_ORDER = (1, 0, 2, 3)

KEY_MSGS = (
    (0, 0, 0, 1, 0, None), (0, 0, None, 3, 2, None), (0, 0, 1, 1, 1, None),
    (1, 1, 1, 0, 0, None), (1, 1, 0, 2, 0, None), (1, 1, 1, 2, 3, None),
    (2, 2, None, 3, 0, None),
    (0, 1, 1, 3, 3, 0), (1, 0, 0, 2, 1, 0), (1, 0, 1, 2, 2, 1), (2, 1, 0, 3, 1, 0),
)
KEY_SLOTS = {(1, 0): (0, 1), (2, 1): (0, 3), (2, 0): (1, 2), (3, 2): (0,), (3, 1): (1, 3), (3, 0): (2,)}

DK_MSGS = (
    (3, 1, 0, 2, 0, None), (3, 1, 1, 0, 0, None), (2, 1, 1, 1, 2, None),
    (3, 0, 1, 0, 2, None), (2, 0, 0, 3, 0, None), (2, 0, 1, 1, 0, None), (1, 0, 0, 0, 3, None),
    (3, 2, 0, 2, 1, None), (3, 2, 1, 2, 2, None),
    (3, 0, 0, 0, 1, 0), (2, 1, 0, 1, 1, 0), (1, 0, 1, 0, 4, 0),
)
DK_FINAL = ((2, 0, (1,)), (2, 1, (2,)), (1, 0, (1,)), (1, 1, (2, 3)), (0, 0, (1, 3)), (0, 1, (2, 4)))


def rope_tables(positions, head):
    half_dim = head // 2
    inv_freq = jnp.power(jnp.float32(ROPE_BASE), -2.0 * jnp.arange(half_dim, dtype=jnp.float32) / head)
    angles = positions.astype(jnp.float32)[..., None] * inv_freq
    return jnp.cos(angles), jnp.sin(angles)


def rot_halves(x1, x2, c, s):
    return x1 * c - x2 * s, x2 * c + x1 * s


def kernel(tokens, heads, head,
           tab_in, key_in, val_in, q_hbm, do_hbm,
           out_ref, dq_ref, gk_ref, gv_ref,
           tabs, qbuf, dobuf, kst, kbuf, vbuf, krel, sbuf, dpbuf, dsbuf, mbuf, lbuf, lse, delta, oacc, obuf, dqbuf,
           dk_part, dv_part, rk, rv, vsum, rvy, rkx,
           sem_loc, sem_px, sem_kx, sem_vy, sem_vx, sem_ky_s, sem_ky_r,
           sem_dv_s, sem_dv_r, sem_dk_s, sem_dk_r, sem_fv_s, sem_fv_r, sem_fk_s, sem_fk_r, sem_o):
    n = SIDE
    half = head // 2
    blk = CORES * tokens
    tile = n * blk
    ht = tile // 2
    nrow = tokens * heads
    scale = head ** -0.5
    c2 = scale * LOG2E
    f32, bf16 = jnp.float32, jnp.bfloat16
    me = lax.axis_index('cp')
    k = lax.rem(me, CORES)
    chip = lax.div(me, CORES)
    x = lax.rem(chip, n)
    y = lax.div(chip, n)
    other = 1 - k
    xr = lax.rem(x + 1, n)
    xo = lax.rem(x + 2, n)
    xl = lax.rem(x + 3, n)

    def dev(yy, xx, kk):
        return (yy * n + xx) * CORES + kk

    partner = dev(y, x, other)
    right, left = dev(y, xr, k), dev(y, xl, k)

    def rcopy(src, dst, ssem, rsem, target):
        return pltpu.make_async_remote_copy(src_ref=src, dst_ref=dst, send_sem=ssem, recv_sem=rsem,
                                            device_id={'cp': target}, device_id_type=pl.DeviceIdType.MESH)

    def at(i, size):
        return pl.ds(pl.multiple_of(i * size, size), size)

    lq = pltpu.make_async_copy(q_hbm.at[k], qbuf.at[k], sem_loc.at[0])
    ld = pltpu.make_async_copy(do_hbm.at[k], dobuf.at[k], sem_loc.at[1])
    lq.start()
    ld.start()
    bar = pltpu.get_barrier_semaphore()
    peers = [partner]
    for d in range(1, n):
        for b in range(CORES):
            peers.append(dev(y, lax.rem(x + d, n), b))
            peers.append(dev(lax.rem(y + d, n), x, b))
    for p in peers:
        pl.semaphore_signal(bar, inc=1, device_id={'cp': p}, device_id_type=pl.DeviceIdType.MESH)

    for b in range(CORES):
        kf = key_in[b].astype(f32)
        r1, r2 = rot_halves(kf[:, :half], kf[:, half:], tab_in[0], tab_in[1])
        kst[b, :, :half] = r1.astype(bf16)
        kst[b, :, half:] = r2.astype(bf16)
    tabs[k] = tab_in[...]
    mine = at(x * CORES + k, tokens)
    kbuf[y, mine] = kst[k]
    vbuf[y, mine] = val_in[k]
    pl.semaphore_wait(bar, len(peers))
    pk = rcopy(kst.at[other], kbuf.at[y, mine], sem_px.at[0, 0], sem_px.at[1, 0], partner)
    pv = rcopy(val_in.at[other], vbuf.at[y, mine], sem_px.at[0, 1], sem_px.at[1, 1], partner)
    pt = rcopy(tab_in, tabs.at[k], sem_px.at[0, 2], sem_px.at[1, 2], partner)
    pq = rcopy(q_hbm.at[other], qbuf.at[k], sem_px.at[0, 3], sem_px.at[1, 3], partner)
    pd = rcopy(do_hbm.at[other], dobuf.at[k], sem_px.at[0, 4], sem_px.at[1, 4], partner)

    def kx_copy(d, b, src_core=None):
        return rcopy(kst.at[b], kbuf.at[y, mine], sem_kx.at[0, d - 1, b],
                     sem_kx.at[1, d - 1, k if src_core is None else src_core], dev(y, lax.rem(x + d, n), b))

    def vy_copy(d, b, src_core=None):
        return rcopy(val_in.at[b], vbuf.at[y, mine], sem_vy.at[0, d - 1, b],
                     sem_vy.at[1, d - 1, k if src_core is None else src_core], dev(lax.rem(y + d, n), x, b))

    pv.start()
    pk.start()
    for d in (2, 1, 3):
        for b in range(CORES):
            kx_copy(d, b).start()
    for d in (2, 1, 3):
        @pl.when(y + d < n)
        def _(d=d):
            for b in range(CORES):
                vy_copy(d, b).start()
    pt.start()
    pq.start()
    pd.start()

    def vx_copy(dy, i):
        t = lax.rem(y - dy + n, n)
        if i == 0:
            ref, target = vbuf.at[t, at(x, blk)], right
        elif i == 1:
            ref, target = vbuf.at[t, at(x, blk)], left
        elif i == 2:
            ref, target = vbuf.at[t, at(xl * CORES, tokens)], right
        else:
            ref, target = vbuf.at[t, at(xr * CORES + 1, tokens)], left
        return rcopy(ref, ref, sem_vx.at[0, dy, i], sem_vx.at[1, dy, i], target)

    def vx_relay(dy):
        vx_copy(dy, 0).wait_recv()
        vx_copy(dy, 2).start()
        vx_copy(dy, 1).wait_recv()
        vx_copy(dy, 3).start()

    def key_copy(i):
        src, t, hf, dst, slot, after = KEY_MSGS[i]
        ref = kbuf.at[t] if hf is None else kbuf.at[t, pl.ds(hf * ht, ht)]
        s_ref = krel if (src == 0 and after is not None) else ref
        d_ref = krel if dst == 0 else ref
        return rcopy(s_ref, d_ref, sem_ky_s.at[i], sem_ky_r.at[slot], dev(dst, x, k))

    def key_wait(row, slot):
        for i, m in enumerate(KEY_MSGS):
            if m[3] == row and m[4] == slot:
                key_copy(i).wait_recv()
    pv.wait_recv()
    vx_copy(0, 0).start()
    vx_copy(0, 1).start()
    pk.wait_recv()
    for d in range(1, n):
        for b in range(CORES):
            kx_copy(d, b, b).wait_recv()
    for r in range(n):
        @pl.when(y == r)
        def _(r=r):
            for i, m in enumerate(KEY_MSGS):
                if m[0] == r and m[5] is None:
                    key_copy(i).start()
    for d in range(1, n):
        @pl.when(y - d >= 0)
        def _(d=d):
            for b in range(CORES):
                vy_copy(d, b, b).wait_recv()
            vx_copy(d, 0).start()
            vx_copy(d, 1).start()
    pt.wait_recv()
    lq.wait()
    pq.wait_recv()
    def rotate_rows(tok, carry):
        for s in range(CORES):
            rows = at(tok, heads)
            c = tabs[s, 0, pl.ds(tok, 1), :]
            sn = tabs[s, 1, pl.ds(tok, 1), :]
            qf = qbuf[s, rows, :].astype(f32)
            r1, r2 = rot_halves(qf[:, :half], qf[:, half:], c, sn)
            qbuf[s, rows, :half] = r1.astype(bf16)
            qbuf[s, rows, half:] = r2.astype(bf16)
        return carry
    lax.fori_loop(0, tokens, rotate_rows, 0, unroll=4)
    ld.wait()
    pd.wait_recv()
    vx_relay(0)
    vx_copy(0, 2).wait_recv()
    vx_copy(0, 3).wait_recv()

    nt = (((1,), (1,)), ((), ()))
    tn = (((0,), (0,)), ((), ()))

    rf = 1024

    def forward_tile(t, first):
        kt = kbuf.at[t]
        vt = vbuf.at[t]

        def rows_body(i, carry):
            for s in range(CORES):
                rows = at(i, rf)
                sc = lax.dot_general(qbuf[s, rows, :], kt[...], nt, preferred_element_type=f32)
                if first:
                    row_tok = (x * CORES + s) * tokens + (i * rf + lax.broadcasted_iota(jnp.int32, sc.shape, 0)) // heads
                    sc = jnp.where(lax.broadcasted_iota(jnp.int32, sc.shape, 1) <= row_tok, sc, -jnp.inf)
                sbuf[t, s, rows, :] = sc
                mx = jnp.max(sc, axis=1, keepdims=True)
                if not first:
                    old = mbuf[s, rows, :]
                    mx = jnp.maximum(old, mx)
                    fac = jnp.exp2((old - mx) * c2)
                else:
                    mx = jnp.broadcast_to(mx, (rf, 128))
                mbuf[s, rows, :] = mx
                mxw = jnp.concatenate([mx] * (tile // 128), axis=1)
                p = jnp.exp2((sc - mxw) * c2)
                tot = p[:, :128] + p[:, 128:]
                o = jnp.dot(p.astype(bf16), vt[...], preferred_element_type=f32)
                if not first:
                    tot = tot + lbuf[s, rows, :] * fac
                    o = o + oacc[s, rows, :] * jnp.concatenate([fac] * (head // 128), axis=1)
                lbuf[s, rows, :] = tot
                oacc[s, rows, :] = o
                dpbuf[t, s, rows, :] = lax.dot_general(dobuf[s, rows, :], vt[...], nt, preferred_element_type=f32)
            return carry
        if nrow == rf:
            rows_body(0, 0)
        else:
            lax.fori_loop(0, nrow // rf, rows_body, 0)
    forward_tile(y, True)
    for d in range(1, n):
        @pl.when(y - d >= 0)
        def _(d=d):
            vx_relay(d)
    for r in range(n - 1):
        @pl.when(y == r)
        def _(r=r):
            for i, m in enumerate(KEY_MSGS):
                if m[0] == r and m[5] is not None:
                    key_wait(r, m[5])
                    key_copy(i).start()
    for j, d in enumerate((1, n - 1, 2)):
        dd = jnp.where(y == n - 1, d, j + 1)

        @pl.when(y - (j + 1) >= 0)
        def _(j=j, d=d, dd=dd):
            t = y - dd
            for r in range(n):
                tr = r - (d if r == n - 1 else j + 1)
                if tr < 0:
                    continue

                @pl.when(y == r)
                def _(r=r, tr=tr):
                    for slot in KEY_SLOTS[(r, tr)]:
                        if not any(m[0] == r and m[5] == slot for m in KEY_MSGS):
                            key_wait(r, slot)
                    vx_copy(r - tr, 2).wait_recv()
                    vx_copy(r - tr, 3).wait_recv()
            forward_tile(t, False)
    rc = 256
    for s in range(CORES):
        def out_rows(i, carry, s=s):
            rows = at(i, rc)
            tot = jnp.sum(lbuf[s, rows, :], axis=1, keepdims=True)
            inv = 1.0 / tot
            ob = (oacc[s, rows, :] * inv).astype(bf16)
            obuf[s, rows, :] = ob
            dl = jnp.sum(ob.astype(f32) * dobuf[s, rows, :].astype(f32), axis=1, keepdims=True)
            lse[s, rows, :] = mbuf[s, rows, :] * c2 + jnp.broadcast_to(jnp.log2(tot), (rc, 128))
            delta[s, rows, :] = jnp.broadcast_to(dl, (rc, 128))
            return carry
        lax.fori_loop(0, nrow // rc, out_rows, 0, unroll=2)
    oloc = pltpu.make_async_copy(obuf.at[k], out_ref.at[k], sem_loc.at[2])
    orem = rcopy(obuf.at[other], out_ref.at[k], sem_o.at[0, 0], sem_o.at[1, 0], partner)
    oloc.start()
    orem.start()

    def dv_copy(t, i):
        xt = (xo, xr, xr, xo, xl, xl)[i]
        hf = (0, 1, 0, 1, 0, 1)[i]
        return rcopy(dv_part.at[t, at(xt * CORES + hf, tokens)], rv.at[t, i], sem_dv_s.at[t, i], sem_dv_r.at[t, i],
                     right if i < 3 else left)

    def dv_combine(t):
        for i in (0, 3):
            dv_copy(t, i).wait_recv()
            rows = at(xr * CORES, tokens) if i == 0 else at(xl * CORES + 1, tokens)
            dv_part[t, rows] = dv_part[t, rows] + rv[t, i]
            dv_copy(t, i + 2).start()

    def dk_copy(i):
        src, t, hf, dst, slot, after = DK_MSGS[i]
        return rcopy(dk_part.at[t, pl.ds(hf * ht, ht)], rk.at[slot], sem_dk_s.at[i], sem_dk_r.at[slot], dev(dst, x, k))

    dk_relay = rcopy(rk.at[0], rk.at[3], sem_dk_s.at[len(DK_MSGS)], sem_dk_r.at[3], dev(1, x, k))

    def dk_wait(slot):
        rcopy(rk.at[slot], rk.at[slot], sem_dk_s.at[0], sem_dk_r.at[slot], partner).wait_recv()

    def fv_copy(t, c):
        dst = dev(t, x, c)
        return rcopy(vsum.at[t, c], rvy.at[y - t, k], sem_fv_s.at[t, c], sem_fv_r.at[y - t, k], dst)

    def fv_own():
        return rcopy(vsum.at[y, other], rvy.at[0, k], sem_fv_s.at[y, other], sem_fv_r.at[0, k], partner)

    def fk_copy(d, c, src_core=None):
        xt = lax.rem(x + d, n)
        return rcopy(dk_part.at[y, at(xt * CORES + c, tokens)], rkx.at[d, k], sem_fk_s.at[d, c],
                     sem_fk_r.at[d, k if src_core is None else src_core], dev(y, xt, c))

    def fk_own(src_core=None):
        return rcopy(dk_part.at[y, at(x * CORES + other, tokens)], rkx.at[0, k], sem_fk_s.at[0, 0],
                     sem_fk_r.at[0, k if src_core is None else src_core], partner)

    def fk_start():
        for d in (2, 1, 3):
            for c in range(CORES):
                fk_copy(d, c).start()
        fk_own().start()

    rb = 512

    for idx, t in enumerate(TILE_ORDER):
        @pl.when(y >= t)
        def _(t=t):
            dva = None
            dka = None
            for s in range(CORES):
                for i in range(nrow // rb):
                    rows = pl.ds(i * rb, rb)
                    ls = lse[s, rows, :]
                    dl = delta[s, rows, :]
                    p = jnp.exp2(sbuf[t, s, rows, :] * c2 - jnp.concatenate([ls] * (tile // 128), axis=1))
                    ds = (p * (dpbuf[t, s, rows, :] - jnp.concatenate([dl] * (tile // 128), axis=1))).astype(bf16)
                    dsbuf[t, s, rows, :] = ds
                    a = lax.dot_general(p.astype(bf16), dobuf[s, rows, :], tn, preferred_element_type=f32)
                    dva = a if dva is None else dva + a
                    a = lax.dot_general(ds, qbuf[s, rows, :], tn, preferred_element_type=f32)
                    dka = a if dka is None else dka + a
            dv_part[t] = dva
            dk_part[t] = dka * scale
            for i in (0, 3, 1, 4):
                dv_copy(t, i).start()

        @pl.when(y < t)
        def _(t=t):
            dsbuf[t] = jnp.zeros(dsbuf.shape[1:], bf16)
            kbuf[t] = jnp.zeros(kbuf.shape[1:], bf16)

        for r in range(n):
            @pl.when(y == r)
            def _(r=r, t=t):
                for i, m in enumerate(DK_MSGS):
                    if m[0] == r and m[1] == t and m[5] is None:
                        dk_copy(i).start()
        if idx > 0:
            tp = TILE_ORDER[idx - 1]

            @pl.when(y >= tp)
            def _(tp=tp):
                dv_combine(tp)
        if t == 2:
            @pl.when(y == 0)
            def _():
                dk_wait(0)
                dk_relay.start()
            for r in range(1, n):
                @pl.when(y == r)
                def _(r=r):
                    for i, m in enumerate(DK_MSGS):
                        if m[0] == r and m[5] is not None:
                            dk_wait(m[5])
                            dk_part[m[1], pl.ds(m[2] * ht, ht)] = dk_part[m[1], pl.ds(m[2] * ht, ht)] + rk[m[5]]
                            dk_copy(i).start()
    @pl.when(y == n - 1)
    def _():
        fk_start()
        dv_combine(TILE_ORDER[n - 1])
    for s in range(CORES):
        def dq_rows(i, carry, s=s):
            rows = at(i, rc)
            acc = None
            for t in range(n):
                a = jnp.dot(dsbuf[t, s, rows, :], kbuf[t], preferred_element_type=f32)
                acc = a if acc is None else acc + a
            acc = acc * scale
            for j in range(rc // heads):
                tok = i * (rc // heads) + j
                c = tabs[s, 0, pl.ds(tok, 1), :]
                sn = tabs[s, 1, pl.ds(tok, 1), :]
                g = acc[j * heads:(j + 1) * heads]
                r1, r2 = rot_halves(g[:, :half], g[:, half:], c, -sn)
                orow = at(tok, heads)
                dqbuf[s, orow, :half] = r1.astype(bf16)
                dqbuf[s, orow, half:] = r2.astype(bf16)
            return carry
        lax.fori_loop(0, nrow // rc, dq_rows, 0, unroll=2)
    qloc = pltpu.make_async_copy(dqbuf.at[k], dq_ref.at[k], sem_loc.at[3])
    qrem = rcopy(dqbuf.at[other], dq_ref.at[k], sem_o.at[0, 1], sem_o.at[1, 1], partner)
    qloc.start()
    qrem.start()
    for t in TILE_ORDER:
        @pl.when(y >= t)
        def _(t=t):
            for i in (1, 2, 4, 5):
                dv_copy(t, i).wait_recv()
            own = at(x * CORES, tokens)
            own2 = at(x * CORES + 1, tokens)
            vsum[t, 0] = dv_part[t, own] + rv[t, 2] + rv[t, 4]
            vsum[t, 1] = dv_part[t, own2] + rv[t, 1] + rv[t, 5]

        @pl.when(y > t)
        def _(t=t):
            for c in range(CORES):
                fv_copy(t, c).start()
    fv_own().start()
    for r in range(n - 1):
        @pl.when(y == r)
        def _(r=r):
            for row, hf, slots in DK_FINAL:
                if row == r:
                    acc = dk_part[r, pl.ds(hf * ht, ht)]
                    for slot in slots:
                        dk_wait(slot)
                        acc = acc + rk[slot]
                    dk_part[r, pl.ds(hf * ht, ht)] = acc
            fk_start()
    def fv_wait(d, b):
        rcopy(rvy.at[d, b], rvy.at[d, b], sem_fv_s.at[0, 0], sem_fv_r.at[d, b], partner).wait_recv()

    fv_wait(0, other)
    rvy[0, k] = vsum[y, k]
    for d in range(1, n):
        @pl.when(y + d < n)
        def _(d=d):
            for b in range(CORES):
                fv_wait(d, b)
                rvy[0, b] = rvy[0, b] + rvy[d, b]
    for b in range(CORES):
        gv_ref[b] = rvy[0, b].astype(bf16)
    fk_own(other).wait_recv()
    rkx[0, k] = dk_part[y, at(x * CORES + k, tokens)]
    for d in range(1, n):
        for b in range(CORES):
            fk_copy(d, 0, b).wait_recv()
    ct, st = tab_in[0], tab_in[1]
    for b in range(CORES):
        g = rkx[0, b] + rkx[1, b] + rkx[2, b] + rkx[3, b]
        r1, r2 = rot_halves(g[:, :half], g[:, half:], ct, -st)
        gk_ref[b, :, :half] = r1.astype(bf16)
        gk_ref[b, :, half:] = r2.astype(bf16)
    for cp in (pk, pv, pt, pq, pd):
        cp.wait_send()
    for d in range(1, n):
        for b in range(CORES):
            kx_copy(d, b).wait_send()
            fk_copy(d, b).wait_send()

        @pl.when(y + d < n)
        def _(d=d):
            for b in range(CORES):
                vy_copy(d, b).wait_send()
    fk_own().wait_send()
    fv_own().wait_send()
    for d in range(n):
        @pl.when(y - d >= 0)
        def _(d=d):
            for i in range(4):
                vx_copy(d, i).wait_send()
    for r in range(n):
        @pl.when(y == r)
        def _(r=r):
            for i, m in enumerate(KEY_MSGS):
                if m[0] == r:
                    key_copy(i).wait_send()
            for i, m in enumerate(DK_MSGS):
                if m[0] == r:
                    dk_copy(i).wait_send()
            if r == 0:
                dk_relay.wait_send()
    for t in range(n):
        @pl.when(y >= t)
        def _(t=t):
            for i in range(6):
                dv_copy(t, i).wait_send()

        @pl.when(y > t)
        def _(t=t):
            for c in range(CORES):
                fv_copy(t, c).wait_send()
    oloc.wait()
    qloc.wait()
    orem.wait()
    qrem.wait()


def write_kernel(a, b, c, d, ao, bo, co, do, av, bv, sem):
    parts = 2
    loads = []
    stores = []
    for j, (src, buf, dst) in enumerate(((a, av, ao), (b, bv, bo))):
        for i in range(parts):
            loads.append(pltpu.make_async_copy(src.at[i], buf.at[i], sem.at[j * parts + i]))
            stores.append(pltpu.make_async_copy(buf.at[i], dst.at[i], sem.at[j * parts + i]))
    for cp in loads:
        cp.start()
    co[...] = c[...]
    do[...] = d[...]
    for ld, st in zip(loads, stores):
        ld.wait()
        st.start()
    for st in stores:
        st.wait()


def solution(mesh):
    cp_size = mesh.shape['cp']
    n = SIDE
    assert cp_size == n * n * CORES
    query_spec = P('dp', 'cp', None, None)
    kv_spec = P('dp', 'cp', None)
    pos_spec = P(('dp', 'cp'))

    def per_device(query, key, value, positions, grad_out):
        batch, tokens, heads, head = query.shape
        nrow = tokens * heads
        tab = jnp.stack(rope_tables(positions, head))
        q2 = query.reshape(batch, nrow, head)
        d2 = grad_out.reshape(batch, nrow, head)
        blk = CORES * tokens
        tile = n * blk
        bf16, f32 = jnp.bfloat16, jnp.float32
        V = pltpu.VMEM
        D = pltpu.SemaphoreType.DMA
        scratch = [
            V((CORES, 2, tokens, head // 2), f32),
            V((CORES, nrow, head), bf16),
            V((CORES, nrow, head), bf16),
            V((CORES, tokens, head), bf16),
            V((n, tile, head), bf16),
            V((n, tile, head), bf16),
            V((tile // 2, head), bf16),
            V((n, CORES, nrow, tile), f32),
            V((n, CORES, nrow, tile), f32),
            V((n, CORES, nrow, tile), bf16),
            V((CORES, nrow, 128), f32),
            V((CORES, nrow, 128), f32),
            V((CORES, nrow, 128), f32),
            V((CORES, nrow, 128), f32),
            V((CORES, nrow, head), f32),
            V((CORES, nrow, head), bf16),
            V((CORES, nrow, head), bf16),
            V((n, tile, head), f32),
            V((n, tile, head), f32),
            V((5, tile // 2, head), f32),
            V((n, 6, tokens, head), f32),
            V((n, CORES, tokens, head), f32),
            V((n, CORES, tokens, head), f32),
            V((n, CORES, tokens, head), f32),
            D((4,)), D((2, 5)), D((2, n - 1, CORES)), D((2, n - 1, CORES)), D((2, n, 4)),
            D((len(KEY_MSGS),)), D((4,)),
            D((n, 6)), D((n, 6)), D((len(DK_MSGS) + 1,)), D((5,)),
            D((n, CORES)), D((n, CORES)), D((n, CORES)), D((n, CORES)), D((2, 2)),
        ]
        vmem = pl.BlockSpec(memory_space=pltpu.VMEM)
        hbm = pl.BlockSpec(memory_space=pl.ANY)
        shapes = [jax.ShapeDtypeStruct(a.shape, bf16) for a in (q2, q2, key, value)]
        outs = pl.pallas_call(
            functools.partial(kernel, tokens, heads, head),
            out_shape=shapes,
            in_specs=[vmem, vmem, vmem, hbm, hbm],
            out_specs=[hbm, hbm, vmem, vmem],
            scratch_shapes=scratch,
            compiler_params=pltpu.CompilerParams(collective_id=0, has_side_effects=True,
                                                 vmem_limit_bytes=58 * 1024 * 1024),
        )(tab, key, value, q2, d2)
        outs = pl.pallas_call(
            write_kernel, out_shape=shapes,
            in_specs=[hbm, hbm, vmem, vmem], out_specs=[hbm, hbm, vmem, vmem],
            scratch_shapes=[V(q2.shape, bf16), V(q2.shape, bf16), D((4,))],
        )(*outs)
        out, dq, gk, gv = outs
        return out.reshape(query.shape), dq.reshape(query.shape), gk, gv

    return jax.shard_map(per_device, mesh=mesh, in_specs=(query_spec, kv_spec, kv_spec, pos_spec, query_spec),
                         out_specs=(query_spec, query_spec, kv_spec, kv_spec), check_vma=False)
```

```python
import functools
import math

import jax
import jax.numpy as jnp
from jax import lax
from jax.experimental import pallas as pl
from jax.experimental.pallas import tpu as pltpu
from jax.sharding import PartitionSpec as P

ROPE_BASE = 10000
CORES = 2
SIDE = 4
LOG2E = math.log2(math.e)

KEY_MSGS = (
    (0, 0, 0, 1, 0, None), (0, 0, None, 3, 2, None), (0, 0, 1, 1, 1, None),
    (1, 1, 1, 0, 0, None), (1, 1, 0, 2, 0, None), (1, 1, 1, 2, 3, None),
    (2, 2, None, 3, 0, None),
    (0, 1, 1, 3, 3, 0), (1, 0, 0, 2, 1, 0), (1, 0, 1, 2, 2, 1), (2, 1, 0, 3, 1, 0),
)
KEY_SLOTS = {(1, 0): (0, 1), (2, 1): (0, 3), (2, 0): (1, 2), (3, 2): (0,), (3, 1): (1, 3), (3, 0): (2,)}

DK_HALVES = (
    (3, 1, 0, 2, 0, None), (3, 1, 1, 0, 0, None), (2, 1, 1, 1, 2, None),
    (3, 0, 1, 0, 2, None), (2, 0, 0, 3, 0, None), (2, 0, 1, 1, 0, None), (1, 0, 0, 0, 3, None),
    (3, 2, 0, 2, 1, None), (3, 2, 1, 2, 2, None),
    (3, 0, 0, 0, 1, 0), (2, 1, 0, 1, 1, 0), (1, 0, 1, 0, 4, 0),
)
DK_MSGS = tuple((r, t, 2 * h + e, dr, 2 * sl + e, None if af is None else 2 * af + e)
                for r, t, h, dr, sl, af in DK_HALVES for e in range(2))
DK_RELAY = ((0, 6), (1, 7))
DK_FINAL = {2: ((1,), (2,)), 1: ((1,), (2, 3)), 0: ((1, 3), (2, 4))}
DK_QUARTERS = {3: (0, 1, 2, 3), 2: (0, 1, 2, 3), 1: (0, 1, 2, 3), 0: (2, 3, 0, 1)}
TILE_ORDER = {0: (0,), 1: (0, 1), 2: (0, 1, 2), 3: (1, 0, 2, 3)}


def rot_halves(x1, x2, c, s):
    return x1 * c - x2 * s, x2 * c + x1 * s


def kernel(tokens, heads, head,
           pos_ref, freq_hbm, key_hbm, val_hbm, q_hbm, do_hbm,
           out_ref, dq_ref, gk_ref, gv_ref,
           freq_in, ang, key_in, val_in, tab_in, tabs, qbuf, dobuf, kst, kbuf, vbuf, krel, sbuf, dpbuf, dsbuf, mbuf, lbuf, lse, delta, oacc, obuf, dqbuf,
           dk_part, dv_part, rk, rv, vsum, rvy, rkx,
           sem_loc, sem_px, sem_kx, sem_vy, sem_vx, sem_ky_s, sem_ky_r,
           sem_dv_s, sem_dv_r, sem_dk_s, sem_dk_r, sem_fv_s, sem_fv_r, sem_fk_s, sem_fk_r, sem_o):
    n = SIDE
    half = head // 2
    blk = CORES * tokens
    tile = n * blk
    ht = tile // 2
    nrow = tokens * heads
    scale = head ** -0.5
    c2 = scale * LOG2E
    f32, bf16 = jnp.float32, jnp.bfloat16
    me = lax.axis_index('cp')
    k = lax.rem(me, CORES)
    chip = lax.div(me, CORES)
    x = lax.rem(chip, n)
    y = lax.div(chip, n)
    other = 1 - k
    xr = lax.rem(x + 1, n)
    xo = lax.rem(x + 2, n)
    xl = lax.rem(x + 3, n)

    def dev(yy, xx, kk):
        return (yy * n + xx) * CORES + kk

    partner = dev(y, x, other)
    right, left = dev(y, xr, k), dev(y, xl, k)

    def rcopy(src, dst, ssem, rsem, target):
        return pltpu.make_async_remote_copy(src_ref=src, dst_ref=dst, send_sem=ssem, recv_sem=rsem,
                                            device_id={'cp': target}, device_id_type=pl.DeviceIdType.MESH)

    def at(i, size):
        return pl.ds(pl.multiple_of(i * size, size), size)
    bar = pltpu.get_barrier_semaphore()
    peers = [partner]
    for d in range(1, n):
        for b in range(CORES):
            peers.append(dev(y, lax.rem(x + d, n), b))
            peers.append(dev(lax.rem(y + d, n), x, b))
    for p in peers:
        pl.semaphore_signal(bar, inc=1, device_id={'cp': p}, device_id_type=pl.DeviceIdType.MESH)

    lf = pltpu.make_async_copy(freq_hbm, freq_in, sem_loc.at[4])
    lk = pltpu.make_async_copy(key_hbm, key_in, sem_loc.at[5])
    lv = pltpu.make_async_copy(val_hbm, val_in, sem_loc.at[6])
    lq = pltpu.make_async_copy(q_hbm.at[k], qbuf.at[k], sem_loc.at[0])
    ld = pltpu.make_async_copy(do_hbm.at[k], dobuf.at[k], sem_loc.at[1])
    for cp in (lf, lk, lv, lq, ld):
        cp.start()

    for i in range(tokens):
        ang[pl.ds(i, 1), :] = jnp.full((1, half), pos_ref[i], jnp.int32).astype(f32)
    lf.wait()
    angles = ang[...] * freq_in[...]
    tab_in[0] = jnp.cos(angles)
    tab_in[1] = jnp.sin(angles)

    lk.wait()
    lv.wait()
    for b in range(CORES):
        kf = key_in[b].astype(f32)
        r1, r2 = rot_halves(kf[:, :half], kf[:, half:], tab_in[0], tab_in[1])
        kst[b, :, :half] = r1.astype(bf16)
        kst[b, :, half:] = r2.astype(bf16)
    tabs[k] = tab_in[...]
    mine = at(x * CORES + k, tokens)
    kbuf[y, mine] = kst[k]
    vbuf[y, mine] = val_in[k]
    pl.semaphore_wait(bar, len(peers))
    pk = rcopy(kst.at[other], kbuf.at[y, mine], sem_px.at[0, 0], sem_px.at[1, 0], partner)
    pv = rcopy(val_in.at[other], vbuf.at[y, mine], sem_px.at[0, 1], sem_px.at[1, 1], partner)
    pt = rcopy(tab_in, tabs.at[k], sem_px.at[0, 2], sem_px.at[1, 2], partner)
    pq = rcopy(q_hbm.at[other], qbuf.at[k], sem_px.at[0, 3], sem_px.at[1, 3], partner)
    pd = rcopy(do_hbm.at[other], dobuf.at[k], sem_px.at[0, 4], sem_px.at[1, 4], partner)

    def kx_copy(d, b, src_core=None):
        return rcopy(kst.at[b], kbuf.at[y, mine], sem_kx.at[0, d - 1, b],
                     sem_kx.at[1, d - 1, k if src_core is None else src_core], dev(y, lax.rem(x + d, n), b))

    def vy_copy(d, b, src_core=None):
        return rcopy(val_in.at[b], vbuf.at[y, mine], sem_vy.at[0, d - 1, b],
                     sem_vy.at[1, d - 1, k if src_core is None else src_core], dev(lax.rem(y + d, n), x, b))

    pv.start()
    pk.start()
    for d in (2, 1, 3):
        for b in range(CORES):
            kx_copy(d, b).start()
    for d in (2, 1, 3):
        @pl.when(y + d < n)
        def _(d=d):
            for b in range(CORES):
                vy_copy(d, b).start()
    pt.start()
    pq.start()
    pd.start()

    def vx_copy(dy, i):
        t = lax.rem(y - dy + n, n)
        if i == 0:
            ref, target = vbuf.at[t, at(x, blk)], right
        elif i == 1:
            ref, target = vbuf.at[t, at(x, blk)], left
        elif i == 2:
            ref, target = vbuf.at[t, at(xl * CORES, tokens)], right
        else:
            ref, target = vbuf.at[t, at(xr * CORES + 1, tokens)], left
        return rcopy(ref, ref, sem_vx.at[0, dy, i], sem_vx.at[1, dy, i], target)

    def vx_relay(dy):
        vx_copy(dy, 0).wait_recv()
        vx_copy(dy, 2).start()
        vx_copy(dy, 1).wait_recv()
        vx_copy(dy, 3).start()

    def key_copy(i):
        src, t, hf, dst, slot, after = KEY_MSGS[i]
        ref = kbuf.at[t] if hf is None else kbuf.at[t, pl.ds(hf * ht, ht)]
        s_ref = krel if (src == 0 and after is not None) else ref
        d_ref = krel if dst == 0 else ref
        return rcopy(s_ref, d_ref, sem_ky_s.at[i], sem_ky_r.at[slot], dev(dst, x, k))

    def key_wait(row, slot):
        for i, m in enumerate(KEY_MSGS):
            if m[3] == row and m[4] == slot:
                key_copy(i).wait_recv()
    pv.wait_recv()
    vx_copy(0, 0).start()
    vx_copy(0, 1).start()
    pk.wait_recv()
    for d in range(1, n):
        for b in range(CORES):
            kx_copy(d, b, b).wait_recv()
    for r in range(n):
        @pl.when(y == r)
        def _(r=r):
            for i, m in enumerate(KEY_MSGS):
                if m[0] == r and m[5] is None:
                    key_copy(i).start()
    for d in range(1, n):
        @pl.when(y - d >= 0)
        def _(d=d):
            for b in range(CORES):
                vy_copy(d, b, b).wait_recv()
            vx_copy(d, 0).start()
            vx_copy(d, 1).start()
    pt.wait_recv()
    lq.wait()
    pq.wait_recv()
    def rotate_rows(tok, carry):
        for s in range(CORES):
            rows = at(tok, heads)
            c = tabs[s, 0, pl.ds(tok, 1), :]
            sn = tabs[s, 1, pl.ds(tok, 1), :]
            qf = qbuf[s, rows, :].astype(f32)
            r1, r2 = rot_halves(qf[:, :half], qf[:, half:], c, sn)
            qbuf[s, rows, :half] = r1.astype(bf16)
            qbuf[s, rows, half:] = r2.astype(bf16)
        return carry
    lax.fori_loop(0, tokens, rotate_rows, 0, unroll=4)
    ld.wait()
    pd.wait_recv()
    vx_relay(0)
    for d in range(1, n):
        @pl.when(y - d >= 0)
        def _(d=d):
            vx_relay(d)
    vx_copy(0, 2).wait_recv()
    vx_copy(0, 3).wait_recv()

    nt = (((1,), (1,)), ((), ()))
    tn = (((0,), (0,)), ((), ()))

    rf = 1024

    def forward_tile(t, first):
        kt = kbuf.at[t]
        vt = vbuf.at[t]

        def rows_body(i, carry):
            for s in range(CORES):
                rows = at(i, rf)
                sc = lax.dot_general(qbuf[s, rows, :], kt[...], nt, preferred_element_type=f32)
                if first:
                    row_tok = (x * CORES + s) * tokens + (i * rf + lax.broadcasted_iota(jnp.int32, sc.shape, 0)) // heads
                    sc = jnp.where(lax.broadcasted_iota(jnp.int32, sc.shape, 1) <= row_tok, sc, -jnp.inf)
                sbuf[t, s, rows, :] = sc
                mx = jnp.max(sc, axis=1, keepdims=True)
                if not first:
                    old = mbuf[s, rows, :]
                    mx = jnp.maximum(old, mx)
                    fac = jnp.exp2((old - mx) * c2)
                else:
                    mx = jnp.broadcast_to(mx, (rf, 128))
                mbuf[s, rows, :] = mx
                mxw = jnp.concatenate([mx] * (tile // 128), axis=1)
                p = jnp.exp2((sc - mxw) * c2)
                tot = p[:, :128] + p[:, 128:]
                o = jnp.dot(p.astype(bf16), vt[...], preferred_element_type=f32)
                if not first:
                    tot = tot + lbuf[s, rows, :] * fac
                    o = o + oacc[s, rows, :] * jnp.concatenate([fac] * (head // 128), axis=1)
                lbuf[s, rows, :] = tot
                oacc[s, rows, :] = o
                dpbuf[t, s, rows, :] = lax.dot_general(dobuf[s, rows, :], vt[...], nt, preferred_element_type=f32)
            return carry
        if nrow == rf:
            rows_body(0, 0)
        else:
            lax.fori_loop(0, nrow // rf, rows_body, 0)
    forward_tile(y, True)
    for r in range(n - 1):
        @pl.when(y == r)
        def _(r=r):
            for i, m in enumerate(KEY_MSGS):
                if m[0] == r and m[5] is not None:
                    key_wait(r, m[5])
                    key_copy(i).start()
    for j, d in enumerate((1, n - 1, 2)):
        dd = jnp.where(y == n - 1, d, j + 1)

        @pl.when(y - (j + 1) >= 0)
        def _(j=j, d=d, dd=dd):
            t = y - dd
            for r in range(n):
                tr = r - (d if r == n - 1 else j + 1)
                if tr < 0:
                    continue

                @pl.when(y == r)
                def _(r=r, tr=tr):
                    for slot in KEY_SLOTS[(r, tr)]:
                        if not any(m[0] == r and m[5] == slot for m in KEY_MSGS):
                            key_wait(r, slot)
                    vx_copy(r - tr, 2).wait_recv()
                    vx_copy(r - tr, 3).wait_recv()
            forward_tile(t, False)
    rc = 256
    for s in range(CORES):
        def out_rows(i, carry, s=s):
            rows = at(i, rc)
            tot = jnp.sum(lbuf[s, rows, :], axis=1, keepdims=True)
            inv = 1.0 / tot
            ob = (oacc[s, rows, :] * inv).astype(bf16)
            obuf[s, rows, :] = ob
            dl = jnp.sum(ob.astype(f32) * dobuf[s, rows, :].astype(f32), axis=1, keepdims=True)
            lse[s, rows, :] = mbuf[s, rows, :] * c2 + jnp.broadcast_to(jnp.log2(tot), (rc, 128))
            delta[s, rows, :] = jnp.broadcast_to(dl, (rc, 128))
            return carry
        lax.fori_loop(0, nrow // rc, out_rows, 0, unroll=2)
    oloc = pltpu.make_async_copy(obuf.at[k], out_ref.at[k], sem_loc.at[2])
    orem = rcopy(obuf.at[other], out_ref.at[k], sem_o.at[0, 0], sem_o.at[1, 0], partner)
    oloc.start()
    orem.start()

    def dv_copy(t, i):
        xt = (xo, xr, xr, xo, xl, xl)[i]
        hf = (0, 1, 0, 1, 0, 1)[i]
        return rcopy(dv_part.at[t, at(xt * CORES + hf, tokens)], rv.at[t, i], sem_dv_s.at[t, i], sem_dv_r.at[t, i],
                     right if i < 3 else left)

    def dv_combine(t):
        for i in (0, 3):
            dv_copy(t, i).wait_recv()
            rows = at(xr * CORES, tokens) if i == 0 else at(xl * CORES + 1, tokens)
            dv_part[t, rows] = dv_part[t, rows] + rv[t, i]
            dv_copy(t, i + 2).start()

    def dk_copy(i):
        src, t, qt, dst, slot, after = DK_MSGS[i]
        return rcopy(dk_part.at[t, pl.ds(qt * blk, blk)], rk.at[slot], sem_dk_s.at[i], sem_dk_r.at[slot], dev(dst, x, k))

    def dk_relay(i):
        src, dst = DK_RELAY[i]
        return rcopy(rk.at[src], rk.at[dst], sem_dk_s.at[len(DK_MSGS) + i], sem_dk_r.at[dst], dev(1, x, k))

    def dk_wait(slot):
        rcopy(rk.at[slot], rk.at[slot], sem_dk_s.at[0], sem_dk_r.at[slot], partner).wait_recv()

    def dk_combine(e):
        @pl.when(y == 0)
        def _():
            dk_wait(DK_RELAY[e][0])
            dk_relay(e).start()
        for r in range(1, n):
            @pl.when(y == r)
            def _(r=r):
                for i, m in enumerate(DK_MSGS):
                    if m[0] == r and m[5] is not None and m[5] % 2 == e:
                        dk_wait(m[5])
                        rows = pl.ds(m[2] * blk, blk)
                        dk_part[m[1], rows] = dk_part[m[1], rows] + rk[m[5]]
                        dk_copy(i).start()

    def fv_copy(t, c):
        dst = dev(t, x, c)
        return rcopy(vsum.at[t, c], rvy.at[y - t, k], sem_fv_s.at[t, c], sem_fv_r.at[y - t, k], dst)

    def fv_own():
        return rcopy(vsum.at[y, other], rvy.at[0, k], sem_fv_s.at[y, other], sem_fv_r.at[0, k], partner)

    def fk_copy(d, c, src_core=None):
        xt = lax.rem(x + d, n)
        return rcopy(dk_part.at[y, at(xt * CORES + c, tokens)], rkx.at[d, k], sem_fk_s.at[d, c],
                     sem_fk_r.at[d, k if src_core is None else src_core], dev(y, xt, c))

    def fk_own(src_core=None):
        return rcopy(dk_part.at[y, at(x * CORES + other, tokens)], rkx.at[0, k], sem_fk_s.at[0, 0],
                     sem_fk_r.at[0, k if src_core is None else src_core], partner)

    def fk_quarter(xt):
        @pl.when(x != xt)
        def _():
            d = lax.rem(xt - x + n, n)
            for c in range(CORES):
                rcopy(dk_part.at[y, pl.ds(xt * blk + c * tokens, tokens)], rkx.at[d, k], sem_fk_s.at[d, c],
                      sem_fk_r.at[d, k], dev(y, xt, c)).start()

        @pl.when(x == xt)
        def _():
            fk_own().start()

    rb = 512

    def backward_tile(t):
        dva = None
        dka = None
        for s in range(CORES):
            for i in range(nrow // rb):
                rows = pl.ds(i * rb, rb)
                ls = lse[s, rows, :]
                dl = delta[s, rows, :]
                p = jnp.exp2(sbuf[t, s, rows, :] * c2 - jnp.concatenate([ls] * (tile // 128), axis=1))
                ds = (p * (dpbuf[t, s, rows, :] - jnp.concatenate([dl] * (tile // 128), axis=1))).astype(bf16)
                dsbuf[t, s, rows, :] = ds
                a = lax.dot_general(p.astype(bf16), dobuf[s, rows, :], tn, preferred_element_type=f32)
                dva = a if dva is None else dva + a
                a = lax.dot_general(ds, qbuf[s, rows, :], tn, preferred_element_type=f32)
                dka = a if dka is None else dka + a
        dv_part[t] = dva
        dk_part[t] = dka * scale

    def dv_order(i):
        t = i
        for r in range(n):
            if i < len(TILE_ORDER[r]):
                t = jnp.where(y == r, TILE_ORDER[r][i], t)
        return t

    for i in range(n):
        @pl.when(y >= i)
        def _(i=i):
            t = dv_order(i)
            backward_tile(t)
            for m in (0, 3, 1, 4):
                dv_copy(t, m).start()
            for r in range(n):
                if i < len(TILE_ORDER[r]):
                    @pl.when(y == r)
                    def _(r=r):
                        for j, m in enumerate(DK_MSGS):
                            if m[0] == r and m[1] == TILE_ORDER[r][i] and m[5] is None:
                                dk_copy(j).start()

        @pl.when(y < i)
        def _(i=i):
            dsbuf[i] = jnp.zeros(dsbuf.shape[1:], bf16)
            kbuf[i] = jnp.zeros(kbuf.shape[1:], bf16)

    def dv_turn(i):
        @pl.when(y >= i)
        def _():
            dv_combine(dv_order(i))
    dv_turn(0)
    dv_turn(1)
    dk_combine(0)

    def grad_query_rows(s):
        def dq_rows(i, carry):
            rows = at(i, rc)
            acc = None
            for t in range(n):
                a = jnp.dot(dsbuf[t, s, rows, :], kbuf[t], preferred_element_type=f32)
                acc = a if acc is None else acc + a
            acc = acc * scale
            for j in range(rc // heads):
                tok = i * (rc // heads) + j
                c = tabs[s, 0, pl.ds(tok, 1), :]
                sn = tabs[s, 1, pl.ds(tok, 1), :]
                g = acc[j * heads:(j + 1) * heads]
                r1, r2 = rot_halves(g[:, :half], g[:, half:], c, -sn)
                orow = at(tok, heads)
                dqbuf[s, orow, :half] = r1.astype(bf16)
                dqbuf[s, orow, half:] = r2.astype(bf16)
            return carry
        lax.fori_loop(0, nrow // rc, dq_rows, 0, unroll=2)
    grad_query_rows(0)
    dk_combine(1)
    dv_turn(2)
    dv_turn(3)

    @pl.when(y == n - 1)
    def _():
        for xt in DK_QUARTERS[n - 1]:
            fk_quarter(xt)
    grad_query_rows(1)
    qloc = pltpu.make_async_copy(dqbuf.at[k], dq_ref.at[k], sem_loc.at[3])
    qrem = rcopy(dqbuf.at[other], dq_ref.at[k], sem_o.at[0, 1], sem_o.at[1, 1], partner)
    qloc.start()
    qrem.start()
    for j in range(n):
        @pl.when(y >= j)
        def _(j=j):
            t = dv_order(j)
            for i in (1, 2, 4, 5):
                dv_copy(t, i).wait_recv()
            own = at(x * CORES, tokens)
            own2 = at(x * CORES + 1, tokens)
            vsum[t, 0] = dv_part[t, own] + rv[t, 2] + rv[t, 4]
            vsum[t, 1] = dv_part[t, own2] + rv[t, 1] + rv[t, 5]

            @pl.when(y > t)
            def _():
                for c in range(CORES):
                    fv_copy(t, c).start()
    fv_own().start()
    for r in range(n - 1):
        @pl.when(y == r)
        def _(r=r):
            for qt in DK_QUARTERS[r]:
                rows = pl.ds(qt * blk, blk)
                acc = dk_part[r, rows]
                for slot in DK_FINAL[r][qt // 2]:
                    dk_wait(2 * slot + qt % 2)
                    acc = acc + rk[2 * slot + qt % 2]
                dk_part[r, rows] = acc
                fk_quarter(qt)
    def fv_wait(d, b):
        rcopy(rvy.at[d, b], rvy.at[d, b], sem_fv_s.at[0, 0], sem_fv_r.at[d, b], partner).wait_recv()

    fv_wait(0, other)
    rvy[0, k] = vsum[y, k]
    for d in range(1, n):
        @pl.when(y + d < n)
        def _(d=d):
            for b in range(CORES):
                fv_wait(d, b)
                rvy[0, b] = rvy[0, b] + rvy[d, b]
    for b in range(CORES):
        gv_ref[b] = rvy[0, b].astype(bf16)
    fk_own(other).wait_recv()
    rkx[0, k] = dk_part[y, at(x * CORES + k, tokens)]
    for d in range(1, n):
        for b in range(CORES):
            fk_copy(d, 0, b).wait_recv()
    ct, st = tab_in[0], tab_in[1]
    for b in range(CORES):
        g = rkx[0, b] + rkx[1, b] + rkx[2, b] + rkx[3, b]
        r1, r2 = rot_halves(g[:, :half], g[:, half:], ct, -st)
        gk_ref[b, :, :half] = r1.astype(bf16)
        gk_ref[b, :, half:] = r2.astype(bf16)
    for cp in (pk, pv, pt, pq, pd):
        cp.wait_send()
    for d in range(1, n):
        for b in range(CORES):
            kx_copy(d, b).wait_send()
            fk_copy(d, b).wait_send()

        @pl.when(y + d < n)
        def _(d=d):
            for b in range(CORES):
                vy_copy(d, b).wait_send()
    fk_own().wait_send()
    fv_own().wait_send()
    for d in range(n):
        @pl.when(y - d >= 0)
        def _(d=d):
            for i in range(4):
                vx_copy(d, i).wait_send()
    for r in range(n):
        @pl.when(y == r)
        def _(r=r):
            for i, m in enumerate(KEY_MSGS):
                if m[0] == r:
                    key_copy(i).wait_send()
            for i, m in enumerate(DK_MSGS):
                if m[0] == r:
                    dk_copy(i).wait_send()
            if r == 0:
                for i in range(len(DK_RELAY)):
                    dk_relay(i).wait_send()
    for t in range(n):
        @pl.when(y >= t)
        def _(t=t):
            for i in range(6):
                dv_copy(t, i).wait_send()

        @pl.when(y > t)
        def _(t=t):
            for c in range(CORES):
                fv_copy(t, c).wait_send()
    oloc.wait()
    qloc.wait()
    orem.wait()
    qrem.wait()


def write_kernel(a, b, c, d, ao, bo, co, do, av, bv, sem):
    parts = 2
    loads = []
    stores = []
    for j, (src, buf, dst) in enumerate(((a, av, ao), (b, bv, bo))):
        for i in range(parts):
            loads.append(pltpu.make_async_copy(src.at[i], buf.at[i], sem.at[j * parts + i]))
            stores.append(pltpu.make_async_copy(buf.at[i], dst.at[i], sem.at[j * parts + i]))
    for cp in loads:
        cp.start()
    co[...] = c[...]
    do[...] = d[...]
    for ld, st in zip(loads, stores):
        ld.wait()
        st.start()
    for st in stores:
        st.wait()


def solution(mesh):
    cp_size = mesh.shape['cp']
    n = SIDE
    assert cp_size == n * n * CORES
    query_spec = P('dp', 'cp', None, None)
    kv_spec = P('dp', 'cp', None)
    pos_spec = P(('dp', 'cp'))

    def per_device(query, key, value, positions, grad_out):
        batch, tokens, heads, head = query.shape
        nrow = tokens * heads
        freq = jnp.power(jnp.float32(ROPE_BASE), -2.0 * jnp.arange(head // 2, dtype=jnp.float32) / head)[None, :]
        q2 = query.reshape(batch, nrow, head)
        d2 = grad_out.reshape(batch, nrow, head)
        blk = CORES * tokens
        tile = n * blk
        bf16, f32 = jnp.bfloat16, jnp.float32
        V = pltpu.VMEM
        D = pltpu.SemaphoreType.DMA
        scratch = [
            V((1, head // 2), f32),
            V((tokens, head // 2), f32),
            V((batch, tokens, head), bf16),
            V((batch, tokens, head), bf16),
            V((2, tokens, head // 2), f32),
            V((CORES, 2, tokens, head // 2), f32),
            V((CORES, nrow, head), bf16),
            V((CORES, nrow, head), bf16),
            V((CORES, tokens, head), bf16),
            V((n, tile, head), bf16),
            V((n, tile, head), bf16),
            V((tile // 2, head), bf16),
            V((n, CORES, nrow, tile), f32),
            V((n, CORES, nrow, tile), f32),
            V((n, CORES, nrow, tile), bf16),
            V((CORES, nrow, 128), f32),
            V((CORES, nrow, 128), f32),
            V((CORES, nrow, 128), f32),
            V((CORES, nrow, 128), f32),
            V((CORES, nrow, head), f32),
            V((CORES, nrow, head), bf16),
            V((CORES, nrow, head), bf16),
            V((n, tile, head), f32),
            V((n, tile, head), f32),
            V((10, blk, head), f32),
            V((n, 6, tokens, head), f32),
            V((n, CORES, tokens, head), f32),
            V((n, CORES, tokens, head), f32),
            V((n, CORES, tokens, head), f32),
            D((7,)), D((2, 5)), D((2, n - 1, CORES)), D((2, n - 1, CORES)), D((2, n, 4)),
            D((len(KEY_MSGS),)), D((4,)),
            D((n, 6)), D((n, 6)), D((len(DK_MSGS) + 2,)), D((10,)),
            D((n, CORES)), D((n, CORES)), D((n, CORES)), D((n, CORES)), D((2, 2)),
        ]
        vmem = pl.BlockSpec(memory_space=pltpu.VMEM)
        hbm = pl.BlockSpec(memory_space=pl.ANY)
        shapes = [jax.ShapeDtypeStruct(a.shape, bf16) for a in (q2, q2, key, value)]
        outs = pl.pallas_call(
            functools.partial(kernel, tokens, heads, head),
            out_shape=shapes,
            in_specs=[pl.BlockSpec(memory_space=pltpu.SMEM), hbm, hbm, hbm, hbm, hbm],
            out_specs=[hbm, hbm, vmem, vmem],
            scratch_shapes=scratch,
            compiler_params=pltpu.CompilerParams(collective_id=0, has_side_effects=True,
                                                 vmem_limit_bytes=58 * 1024 * 1024),
        )(positions, freq, key, value, q2, d2)
        outs = pl.pallas_call(
            write_kernel, out_shape=shapes,
            in_specs=[hbm, hbm, vmem, vmem], out_specs=[hbm, hbm, vmem, vmem],
            scratch_shapes=[V(q2.shape, bf16), V(q2.shape, bf16), D((4,))],
        )(*outs)
        out, dq, gk, gv = outs
        return out.reshape(query.shape), dq.reshape(query.shape), gk, gv

    return jax.shard_map(per_device, mesh=mesh, in_specs=(query_spec, kv_spec, kv_spec, pos_spec, query_spec),
                         out_specs=(query_spec, query_spec, kv_spec, kv_spec), check_vma=False)
```

```python
import functools
import math

import jax
import jax.numpy as jnp
from jax import lax
from jax.experimental import pallas as pl
from jax.experimental.pallas import tpu as pltpu
from jax.sharding import PartitionSpec as P

ROPE_BASE = 10000
CORES = 2
SIDE = 4
LOG2E = math.log2(math.e)

KEY_MSGS = (
    (0, 0, 0, 1, 0, None), (0, 0, None, 3, 2, None), (0, 0, 1, 1, 1, None),
    (1, 1, 1, 0, 0, None), (1, 1, 0, 2, 0, None), (1, 1, 1, 2, 3, None),
    (2, 2, None, 3, 0, None),
    (0, 1, 1, 3, 3, 0), (1, 0, 0, 2, 1, 0), (1, 0, 1, 2, 2, 1), (2, 1, 0, 3, 1, 0),
)
KEY_SLOTS = {(1, 0): (0, 1), (2, 1): (0, 3), (2, 0): (1, 2), (3, 2): (0,), (3, 1): (1, 3), (3, 0): (2,)}

DK_MSGS = (
    (3, 1, 0, 2, 0, None, None), (3, 1, 2, 0, 0, None, None), (3, 1, 1, 2, 1, None, None), (3, 1, 3, 0, 1, None, None),
    (3, 0, 3, 0, 5, None, None),
    (3, 2, 0, 2, 2, None, None), (3, 2, 1, 2, 3, None, None), (3, 2, 2, 2, 4, None, None), (3, 2, 3, 2, 5, None, None),
    (2, 0, 3, 1, 0, None, None), (2, 0, 0, 3, 0, None, None), (2, 0, 1, 3, 1, None, None), (2, 0, 2, 3, 2, None, None),
    (2, 1, 2, 1, 3, None, None), (2, 1, 3, 1, 4, None, None),
    (1, 0, 0, 0, 6, None, None), (1, 0, 1, 0, 7, None, None), (1, 0, 2, 0, 8, None, None),
    (3, 0, 0, 0, 2, 0, 0), (3, 0, 1, 0, 3, 1, 0), (3, 0, 2, 0, 4, 2, 1),
    (2, 1, 0, 1, 1, 0, 0), (2, 1, 1, 1, 2, 1, 1), (1, 0, 3, 0, 9, 0, 0),
)
DK_RELAY = ((0, 5), (1, 6))
DK_FINAL = {2: ((0, (2,)), (1, (3,)), (2, (4,)), (3, (5,))), 1: ((2, (3, 5)), (3, (4, 6)), (0, (1,)), (1, (2,))),
            0: ((3, (5, 9)), (0, (2, 6)), (1, (3, 7)), (2, (4, 8)))}
DV_VIA = ()
TILE_ORDER = {0: (0,), 1: (0, 1), 2: (0, 1, 2), 3: (1, 0, 2, 3)}


def rot_halves(x1, x2, c, s):
    return x1 * c - x2 * s, x2 * c + x1 * s


def kernel(tokens, heads, head,
           pos_ref, freq_hbm, key_hbm, val_hbm, q_hbm, do_hbm,
           out_ref, dq_ref, gk_ref, gv_ref,
           freq_in, ang, key_in, val_in, tab_in, tabs, qbuf, dobuf, kst, kbuf, vbuf, krel, sbuf, dpbuf, dsbuf, mbuf, lbuf, lse, delta, oacc, obuf, dqbuf,
           dk_part, dv_part, rk, rv, vsum, fvb, rvy, rkx,
           sem_loc, sem_px, sem_kx, sem_vy, sem_vx, sem_ky_s, sem_ky_r,
           sem_dv_s, sem_dv_r, sem_dk_s, sem_dk_r, sem_fv_s, sem_fv_r, sem_fk_s, sem_fk_r, sem_fvb, sem_o):
    n = SIDE
    half = head // 2
    blk = CORES * tokens
    tile = n * blk
    ht = tile // 2
    nrow = tokens * heads
    scale = head ** -0.5
    c2 = scale * LOG2E
    f32, bf16 = jnp.float32, jnp.bfloat16
    me = lax.axis_index('cp')
    k = lax.rem(me, CORES)
    chip = lax.div(me, CORES)
    x = lax.rem(chip, n)
    y = lax.div(chip, n)
    other = 1 - k
    xr = lax.rem(x + 1, n)
    xo = lax.rem(x + 2, n)
    xl = lax.rem(x + 3, n)

    def dev(yy, xx, kk):
        return (yy * n + xx) * CORES + kk

    partner = dev(y, x, other)
    right, left = dev(y, xr, k), dev(y, xl, k)

    def rcopy(src, dst, ssem, rsem, target):
        return pltpu.make_async_remote_copy(src_ref=src, dst_ref=dst, send_sem=ssem, recv_sem=rsem,
                                            device_id={'cp': target}, device_id_type=pl.DeviceIdType.MESH)

    def at(i, size):
        return pl.ds(pl.multiple_of(i * size, size), size)
    bar = pltpu.get_barrier_semaphore()
    peers = [partner]
    for d in range(1, n):
        for b in range(CORES):
            peers.append(dev(y, lax.rem(x + d, n), b))
            peers.append(dev(lax.rem(y + d, n), x, b))
    for p in peers:
        pl.semaphore_signal(bar, inc=1, device_id={'cp': p}, device_id_type=pl.DeviceIdType.MESH)

    lf = pltpu.make_async_copy(freq_hbm, freq_in, sem_loc.at[4])
    lk = pltpu.make_async_copy(key_hbm, key_in, sem_loc.at[5])
    lv = pltpu.make_async_copy(val_hbm, val_in, sem_loc.at[6])
    lq = pltpu.make_async_copy(q_hbm.at[k], qbuf.at[k], sem_loc.at[0])
    ld = pltpu.make_async_copy(do_hbm.at[k], dobuf.at[k], sem_loc.at[1])
    for cp in (lf, lk, lv, lq, ld):
        cp.start()

    for i in range(tokens):
        ang[pl.ds(i, 1), :] = jnp.full((1, half), pos_ref[i], jnp.int32).astype(f32)
    lf.wait()
    angles = ang[...] * freq_in[...]
    tab_in[0] = jnp.cos(angles)
    tab_in[1] = jnp.sin(angles)

    lk.wait()
    lv.wait()
    for b in range(CORES):
        kf = key_in[b].astype(f32)
        r1, r2 = rot_halves(kf[:, :half], kf[:, half:], tab_in[0], tab_in[1])
        kst[b, :, :half] = r1.astype(bf16)
        kst[b, :, half:] = r2.astype(bf16)
    tabs[k] = tab_in[...]
    mine = at(x * CORES + k, tokens)
    kbuf[y, mine] = kst[k]
    vbuf[y, mine] = val_in[k]
    pl.semaphore_wait(bar, len(peers))
    pk = rcopy(kst.at[other], kbuf.at[y, mine], sem_px.at[0, 0], sem_px.at[1, 0], partner)
    pv = rcopy(val_in.at[other], vbuf.at[y, mine], sem_px.at[0, 1], sem_px.at[1, 1], partner)
    pt = rcopy(tab_in, tabs.at[k], sem_px.at[0, 2], sem_px.at[1, 2], partner)
    pq = rcopy(q_hbm.at[other], qbuf.at[k], sem_px.at[0, 3], sem_px.at[1, 3], partner)
    pd = rcopy(do_hbm.at[other], dobuf.at[k], sem_px.at[0, 4], sem_px.at[1, 4], partner)

    def kx_copy(d, b, src_core=None):
        return rcopy(kst.at[b], kbuf.at[y, mine], sem_kx.at[0, d - 1, b],
                     sem_kx.at[1, d - 1, k if src_core is None else src_core], dev(y, lax.rem(x + d, n), b))

    def vy_copy(d, b, src_core=None):
        return rcopy(val_in.at[b], vbuf.at[y, mine], sem_vy.at[0, d - 1, b],
                     sem_vy.at[1, d - 1, k if src_core is None else src_core], dev(lax.rem(y + d, n), x, b))

    pv.start()
    pk.start()
    for d in (2, 1, 3):
        for b in range(CORES):
            kx_copy(d, b).start()
    for d in (2, 1, 3):
        @pl.when(y + d < n)
        def _(d=d):
            for b in range(CORES):
                vy_copy(d, b).start()
    pt.start()
    pq.start()
    pd.start()

    def vx_copy(dy, i):
        t = lax.rem(y - dy + n, n)
        if i == 0:
            ref, target = vbuf.at[t, at(x, blk)], right
        elif i == 1:
            ref, target = vbuf.at[t, at(x, blk)], left
        elif i == 2:
            ref, target = vbuf.at[t, at(xl * CORES, tokens)], right
        else:
            ref, target = vbuf.at[t, at(xr * CORES + 1, tokens)], left
        return rcopy(ref, ref, sem_vx.at[0, dy, i], sem_vx.at[1, dy, i], target)

    def vx_relay(dy):
        vx_copy(dy, 0).wait_recv()
        vx_copy(dy, 2).start()
        vx_copy(dy, 1).wait_recv()
        vx_copy(dy, 3).start()

    def key_copy(i):
        src, t, hf, dst, slot, after = KEY_MSGS[i]
        ref = kbuf.at[t] if hf is None else kbuf.at[t, pl.ds(hf * ht, ht)]
        s_ref = krel if (src == 0 and after is not None) else ref
        d_ref = krel if dst == 0 else ref
        return rcopy(s_ref, d_ref, sem_ky_s.at[i], sem_ky_r.at[slot], dev(dst, x, k))

    def key_wait(row, slot):
        for i, m in enumerate(KEY_MSGS):
            if m[3] == row and m[4] == slot:
                key_copy(i).wait_recv()

    def rotate_queries(s):
        def rotate_rows(tok, carry):
            rows = at(tok, heads)
            c = tabs[s, 0, pl.ds(tok, 1), :]
            sn = tabs[s, 1, pl.ds(tok, 1), :]
            qf = qbuf[s, rows, :].astype(f32)
            r1, r2 = rot_halves(qf[:, :half], qf[:, half:], c, sn)
            qbuf[s, rows, :half] = r1.astype(bf16)
            qbuf[s, rows, half:] = r2.astype(bf16)
            return carry
        lax.fori_loop(0, tokens, rotate_rows, 0, unroll=8)
    pv.wait_recv()
    vx_copy(0, 0).start()
    vx_copy(0, 1).start()
    lq.wait()
    rotate_queries(k)
    for d in range(1, n):
        @pl.when(y - d >= 0)
        def _(d=d):
            for b in range(CORES):
                vy_copy(d, b, b).wait_recv()
            vx_copy(d, 0).start()
            vx_copy(d, 1).start()
    pt.wait_recv()
    pq.wait_recv()
    rotate_queries(other)
    vx_relay(0)
    pk.wait_recv()
    for d in range(1, n):
        for b in range(CORES):
            kx_copy(d, b, b).wait_recv()
    for r in range(n):
        @pl.when(y == r)
        def _(r=r):
            for i, m in enumerate(KEY_MSGS):
                if m[0] == r and m[5] is None:
                    key_copy(i).start()
    nt = (((1,), (1,)), ((), ()))
    tn = (((0,), (0,)), ((), ()))

    rf = 1024

    def first_scores(t):
        for s in range(CORES):
            sc = lax.dot_general(qbuf[s], kbuf[t], nt, preferred_element_type=f32)
            row_tok = (x * CORES + s) * tokens + lax.broadcasted_iota(jnp.int32, sc.shape, 0) // heads
            sc = jnp.where(lax.broadcasted_iota(jnp.int32, sc.shape, 1) <= row_tok, sc, -jnp.inf)
            sbuf[t, s] = sc
            mbuf[s] = jnp.broadcast_to(jnp.max(sc, axis=1, keepdims=True), (nrow, 128))

    def forward_tile(t, first):
        kt = kbuf.at[t]
        vt = vbuf.at[t]

        def rows_body(i, carry):
            for s in range(CORES):
                rows = at(i, rf)
                if first:
                    sc = sbuf[t, s, rows, :]
                    mx = mbuf[s, rows, :]
                else:
                    sc = lax.dot_general(qbuf[s, rows, :], kt[...], nt, preferred_element_type=f32)
                    sbuf[t, s, rows, :] = sc
                    old = mbuf[s, rows, :]
                    mx = jnp.maximum(old, jnp.max(sc, axis=1, keepdims=True))
                    fac = jnp.exp2((old - mx) * c2)
                    mbuf[s, rows, :] = mx
                mxw = jnp.concatenate([mx] * (tile // 128), axis=1)
                p = jnp.exp2((sc - mxw) * c2)
                tot = p[:, :128] + p[:, 128:]
                o = jnp.dot(p.astype(bf16), vt[...], preferred_element_type=f32)
                if not first:
                    tot = tot + lbuf[s, rows, :] * fac
                    o = o + oacc[s, rows, :] * jnp.concatenate([fac] * (head // 128), axis=1)
                lbuf[s, rows, :] = tot
                oacc[s, rows, :] = o
                dpbuf[t, s, rows, :] = lax.dot_general(dobuf[s, rows, :], vt[...], nt, preferred_element_type=f32)
            return carry
        if nrow == rf:
            rows_body(0, 0)
        else:
            lax.fori_loop(0, nrow // rf, rows_body, 0)
    first_scores(y)
    ld.wait()
    pd.wait_recv()
    for d in range(1, n):
        @pl.when(y - d >= 0)
        def _(d=d):
            vx_relay(d)
    vx_copy(0, 2).wait_recv()
    vx_copy(0, 3).wait_recv()
    forward_tile(y, True)
    for r in range(n - 1):
        @pl.when(y == r)
        def _(r=r):
            for i, m in enumerate(KEY_MSGS):
                if m[0] == r and m[5] is not None:
                    key_wait(r, m[5])
                    key_copy(i).start()
    for j, d in enumerate((1, n - 1, 2)):
        dd = jnp.where(y == n - 1, d, j + 1)

        @pl.when(y - (j + 1) >= 0)
        def _(j=j, d=d, dd=dd):
            t = y - dd
            for r in range(n):
                tr = r - (d if r == n - 1 else j + 1)
                if tr < 0:
                    continue

                @pl.when(y == r)
                def _(r=r, tr=tr):
                    for slot in KEY_SLOTS[(r, tr)]:
                        if not any(m[0] == r and m[5] == slot for m in KEY_MSGS):
                            key_wait(r, slot)
                    vx_copy(r - tr, 2).wait_recv()
                    vx_copy(r - tr, 3).wait_recv()
            forward_tile(t, False)
    rc = 256

    def output_half(s, dst):
        def out_rows(i, carry):
            rows = at(i, rc)
            tot = jnp.sum(lbuf[s, rows, :], axis=1, keepdims=True)
            inv = 1.0 / tot
            ob = (oacc[s, rows, :] * inv).astype(bf16)
            dst[rows, :] = ob
            dl = jnp.sum(ob.astype(f32) * dobuf[s, rows, :].astype(f32), axis=1, keepdims=True)
            lse[s, rows, :] = mbuf[s, rows, :] * c2 + jnp.broadcast_to(jnp.log2(tot), (rc, 128))
            delta[s, rows, :] = jnp.broadcast_to(dl, (rc, 128))
            return carry
        lax.fori_loop(0, nrow // rc, out_rows, 0, unroll=nrow // rc)

    output_half(other, obuf)
    orem = rcopy(obuf, out_ref.at[k], sem_o.at[0, 0], sem_o.at[1, 0], partner)
    orem.start()
    output_half(k, out_ref.at[k])
    def dv_copy(t, i):
        xt = (xo, xr, xr, xo, xl, xl)[i]
        hf = (0, 1, 0, 1, 0, 1)[i]
        return rcopy(dv_part.at[t, at(xt * CORES + hf, tokens)], rv.at[t, i], sem_dv_s.at[t, i], sem_dv_r.at[t, i],
                     right if i < 3 else left)

    def dv_combine(t):
        for i in (0, 3):
            dv_copy(t, i).wait_recv()
            rows = at(xr * CORES, tokens) if i == 0 else at(xl * CORES + 1, tokens)
            dv_part[t, rows] = dv_part[t, rows] + rv[t, i]
            dv_copy(t, i + 2).start()

    def dk_copy(i):
        src, t, qt, dst, slot = DK_MSGS[i][:5]
        return rcopy(dk_part.at[t, pl.ds(qt * blk, blk)], rk.at[slot], sem_dk_s.at[i], sem_dk_r.at[slot], dev(dst, x, k))

    def dk_relay(i):
        src, dst = DK_RELAY[i]
        return rcopy(rk.at[src], rk.at[dst], sem_dk_s.at[len(DK_MSGS) + i], sem_dk_r.at[dst], dev(1, x, k))

    def dk_wait(slot):
        rcopy(rk.at[slot], rk.at[slot], sem_dk_s.at[0], sem_dk_r.at[slot], partner).wait_recv()

    def dk_combine(e):
        @pl.when(y == 0)
        def _():
            dk_wait(DK_RELAY[e][0])
            dk_relay(e).start()
        for r in range(1, n):
            @pl.when(y == r)
            def _(r=r):
                for i, m in enumerate(DK_MSGS):
                    if m[0] == r and m[6] == e:
                        dk_wait(m[5])
                        rows = pl.ds(m[2] * blk, blk)
                        dk_part[m[1], rows] = dk_part[m[1], rows] + rk[m[5]]
                        dk_copy(i).start()

    def fv_copy(t, c):
        dst = dev(t, x, c)
        return rcopy(vsum.at[t, c], rvy.at[y - t, k], sem_fv_s.at[t, c], sem_fv_r.at[y - t, k], dst)

    def fv_via(row):
        t = {2: 1, 1: 0}[row]
        return rcopy(vsum.at[t], fvb, sem_fvb.at[0], sem_fvb.at[1], dev(row, x, k))

    def fv_own():
        return rcopy(vsum.at[y, other], rvy.at[0, k], sem_fv_s.at[y, other], sem_fv_r.at[0, k], partner)

    def fk_copy(d, c, src_core=None):
        xt = lax.rem(x + d, n)
        return rcopy(dk_part.at[y, at(xt * CORES + c, tokens)], rkx.at[d, k], sem_fk_s.at[d, c],
                     sem_fk_r.at[d, k if src_core is None else src_core], dev(y, xt, c))

    def fk_own(src_core=None):
        return rcopy(dk_part.at[y, at(x * CORES + other, tokens)], rkx.at[0, k], sem_fk_s.at[0, 0],
                     sem_fk_r.at[0, k if src_core is None else src_core], partner)

    def fk_quarter(xt):
        @pl.when(x != xt)
        def _():
            d = lax.rem(xt - x + n, n)
            for c in range(CORES):
                rcopy(dk_part.at[y, pl.ds(xt * blk + c * tokens, tokens)], rkx.at[d, k], sem_fk_s.at[d, c],
                      sem_fk_r.at[d, k], dev(y, xt, c)).start()

        @pl.when(x == xt)
        def _():
            fk_own().start()

    rb = 512

    def backward_tile(t):
        dva = None
        dka = None
        for s in range(CORES):
            for i in range(nrow // rb):
                rows = pl.ds(i * rb, rb)
                ls = lse[s, rows, :]
                dl = delta[s, rows, :]
                p = jnp.exp2(sbuf[t, s, rows, :] * c2 - jnp.concatenate([ls] * (tile // 128), axis=1))
                ds = (p * (dpbuf[t, s, rows, :] - jnp.concatenate([dl] * (tile // 128), axis=1))).astype(bf16)
                dsbuf[t, s, rows, :] = ds
                a = lax.dot_general(p.astype(bf16), dobuf[s, rows, :], tn, preferred_element_type=f32)
                dva = a if dva is None else dva + a
                a = lax.dot_general(ds, qbuf[s, rows, :], tn, preferred_element_type=f32)
                dka = a if dka is None else dka + a
        dv_part[t] = dva
        dk_part[t] = dka * scale

    def dv_order(i):
        t = i
        for r in range(n):
            if i < len(TILE_ORDER[r]):
                t = jnp.where(y == r, TILE_ORDER[r][i], t)
        return t

    def dv_turn(i):
        @pl.when(y >= i)
        def _():
            dv_combine(dv_order(i))

    for i in range(n):
        @pl.when(y >= i)
        def _(i=i):
            t = dv_order(i)
            backward_tile(t)
            for m in ((0, 3, 1, 4) if i < 2 else (0, 3)):
                dv_copy(t, m).start()
            for r in range(n):
                if i < len(TILE_ORDER[r]):
                    @pl.when(y == r)
                    def _(r=r):
                        for j, m in enumerate(DK_MSGS):
                            if m[0] == r and m[1] == TILE_ORDER[r][i] and m[5] is None:
                                dk_copy(j).start()

        @pl.when(y < i)
        def _(i=i):
            dsbuf[i] = jnp.zeros(dsbuf.shape[1:], bf16)
            kbuf[i] = jnp.zeros(kbuf.shape[1:], bf16)

        if i >= 2:
            dv_turn(i - 2)

            @pl.when(y >= i)
            def _(i=i):
                t = dv_order(i)
                for m in (1, 4):
                    dv_copy(t, m).start()
    dk_combine(0)

    def grad_query_half(s, dst):
        def dq_rows(i, carry):
            rows = at(i, rc)
            acc = None
            for t in range(n):
                a = jnp.dot(dsbuf[t, s, rows, :], kbuf[t], preferred_element_type=f32)
                acc = a if acc is None else acc + a
            acc = acc * scale
            for j in range(rc // heads):
                tok = i * (rc // heads) + j
                c = tabs[s, 0, pl.ds(tok, 1), :]
                sn = tabs[s, 1, pl.ds(tok, 1), :]
                g = acc[j * heads:(j + 1) * heads]
                r1, r2 = rot_halves(g[:, :half], g[:, half:], c, -sn)
                orow = at(tok, heads)
                dst[orow, :half] = r1.astype(bf16)
                dst[orow, half:] = r2.astype(bf16)
            return carry
        lax.fori_loop(0, nrow // rc, dq_rows, 0, unroll=2)
    grad_query_half(other, dqbuf)
    qrem = rcopy(dqbuf, dq_ref.at[k], sem_o.at[0, 1], sem_o.at[1, 1], partner)
    qrem.start()
    dk_combine(1)

    def dv_total(j):
        @pl.when(y >= j)
        def _():
            t = dv_order(j)
            for i in (1, 2, 4, 5):
                dv_copy(t, i).wait_recv()
            vsum[t, 0] = dv_part[t, at(x * CORES, tokens)] + rv[t, 2] + rv[t, 4]
            vsum[t, 1] = dv_part[t, at(x * CORES + 1, tokens)] + rv[t, 1] + rv[t, 5]
            for r, t_on, via in DV_VIA:
                @pl.when((y == r) & (t == t_on))
                def _(via=via):
                    fv_via(via).start()

            direct = y > t
            for r, t_on, via in DV_VIA:
                direct = direct & ((y != r) | (t != t_on)) & ((y != via) | (t != t_on))

            @pl.when(direct)
            def _():
                for c in range(CORES):
                    fv_copy(t, c).start()

    def dv_via(r, t_on):
        @pl.when(y == r)
        def _():
            fv_via(r).wait_recv()
            vsum[t_on] = vsum[t_on] + fvb[...]
            for c in range(CORES):
                fv_copy(t_on, c).start()

    def dk_final(part):
        for r in range(n - 1):
            @pl.when(y == r)
            def _(r=r):
                for qt, slots in DK_FINAL[r][2 * part:2 * part + 2]:
                    rows = pl.ds(qt * blk, blk)
                    acc = dk_part[r, rows]
                    for slot in slots:
                        dk_wait(slot)
                        acc = acc + rk[slot]
                    dk_part[r, rows] = acc
                    fk_quarter(qt)
    dv_turn(2)
    dv_total(0)
    dv_turn(3)

    @pl.when(y == n - 1)
    def _():
        for xt in range(n):
            fk_quarter(xt)
    dv_total(1)
    grad_query_half(k, dq_ref.at[k])
    dv_total(2)
    dv_total(3)
    fv_own().start()
    dk_final(0)
    for r, t_on, via in DV_VIA:
        dv_via(via, t_on)
    dk_final(1)
    def fv_wait(d, b):
        rcopy(rvy.at[d, b], rvy.at[d, b], sem_fv_s.at[0, 0], sem_fv_r.at[d, b], partner).wait_recv()

    fv_wait(0, other)
    rvy[0, k] = vsum[y, k]
    for d in range(1, n):
        expect = y + d < n
        for r, t_on, via in DV_VIA:
            if r - t_on == d:
                expect = expect & (y != t_on)

        @pl.when(expect)
        def _(d=d):
            for b in range(CORES):
                fv_wait(d, b)
                rvy[0, b] = rvy[0, b] + rvy[d, b]
    for b in range(CORES):
        gv_ref[b] = rvy[0, b].astype(bf16)
    fk_own(other).wait_recv()
    rkx[0, k] = dk_part[y, at(x * CORES + k, tokens)]
    for d in range(1, n):
        for b in range(CORES):
            fk_copy(d, 0, b).wait_recv()
    ct, st = tab_in[0], tab_in[1]
    for b in range(CORES):
        g = rkx[0, b] + rkx[1, b] + rkx[2, b] + rkx[3, b]
        r1, r2 = rot_halves(g[:, :half], g[:, half:], ct, -st)
        gk_ref[b, :, :half] = r1.astype(bf16)
        gk_ref[b, :, half:] = r2.astype(bf16)
    for cp in (pk, pv, pt, pq, pd):
        cp.wait_send()
    for d in range(1, n):
        for b in range(CORES):
            kx_copy(d, b).wait_send()
            fk_copy(d, b).wait_send()

        @pl.when(y + d < n)
        def _(d=d):
            for b in range(CORES):
                vy_copy(d, b).wait_send()
    fk_own().wait_send()
    fv_own().wait_send()
    for d in range(n):
        @pl.when(y - d >= 0)
        def _(d=d):
            for i in range(4):
                vx_copy(d, i).wait_send()
    for r in range(n):
        @pl.when(y == r)
        def _(r=r):
            for i, m in enumerate(KEY_MSGS):
                if m[0] == r:
                    key_copy(i).wait_send()
            for i, m in enumerate(DK_MSGS):
                if m[0] == r:
                    dk_copy(i).wait_send()
            if r == 0:
                for i in range(len(DK_RELAY)):
                    dk_relay(i).wait_send()
    for t in range(n):
        @pl.when(y >= t)
        def _(t=t):
            for i in range(6):
                dv_copy(t, i).wait_send()

        sent = y > t
        for r, t_on, via in DV_VIA:
            if t == t_on:
                sent = sent & (y != r)

        @pl.when(sent)
        def _(t=t):
            for c in range(CORES):
                fv_copy(t, c).wait_send()
    for r, t_on, via in DV_VIA:
        @pl.when(y == r)
        def _(via=via):
            fv_via(via).wait_send()
    orem.wait()
    qrem.wait()


def write_kernel(a, b, c, d, ao, bo, co, do, sem):
    cps = [pltpu.make_async_copy(s, t, sem.at[i]) for i, (s, t) in enumerate(((a, ao), (b, bo), (c, co), (d, do)))]
    for cp in cps:
        cp.start()
    for cp in cps:
        cp.wait()


def solution(mesh):
    cp_size = mesh.shape['cp']
    n = SIDE
    assert cp_size == n * n * CORES
    query_spec = P('dp', 'cp', None, None)
    kv_spec = P('dp', 'cp', None)
    pos_spec = P(('dp', 'cp'))

    def per_device(query, key, value, positions, grad_out):
        batch, tokens, heads, head = query.shape
        nrow = tokens * heads
        freq = jnp.power(jnp.float32(ROPE_BASE), -2.0 * jnp.arange(head // 2, dtype=jnp.float32) / head)[None, :]
        q2 = query.reshape(batch, nrow, head)
        d2 = grad_out.reshape(batch, nrow, head)
        blk = CORES * tokens
        tile = n * blk
        bf16, f32 = jnp.bfloat16, jnp.float32
        V = pltpu.VMEM
        D = pltpu.SemaphoreType.DMA
        scratch = [
            V((1, head // 2), f32),
            V((tokens, head // 2), f32),
            V((batch, tokens, head), bf16),
            V((batch, tokens, head), bf16),
            V((2, tokens, head // 2), f32),
            V((CORES, 2, tokens, head // 2), f32),
            V((CORES, nrow, head), bf16),
            V((CORES, nrow, head), bf16),
            V((CORES, tokens, head), bf16),
            V((n, tile, head), bf16),
            V((n, tile, head), bf16),
            V((tile // 2, head), bf16),
            V((n, CORES, nrow, tile), f32),
            V((n, CORES, nrow, tile), f32),
            V((n, CORES, nrow, tile), bf16),
            V((CORES, nrow, 128), f32),
            V((CORES, nrow, 128), f32),
            V((CORES, nrow, 128), f32),
            V((CORES, nrow, 128), f32),
            V((CORES, nrow, head), f32),
            V((nrow, head), bf16),
            V((nrow, head), bf16),
            V((n, tile, head), f32),
            V((n, tile, head), f32),
            V((10, blk, head), f32),
            V((n, 6, tokens, head), f32),
            V((n, CORES, tokens, head), f32),
            V((CORES, tokens, head), f32),
            V((n, CORES, tokens, head), f32),
            V((n, CORES, tokens, head), f32),
            D((7,)), D((2, 5)), D((2, n - 1, CORES)), D((2, n - 1, CORES)), D((2, n, 4)),
            D((len(KEY_MSGS),)), D((4,)),
            D((n, 6)), D((n, 6)), D((len(DK_MSGS) + 2,)), D((10,)),
            D((n, CORES)), D((n, CORES)), D((n, CORES)), D((n, CORES)), D((2,)), D((2, 2)),
        ]
        vmem = pl.BlockSpec(memory_space=pltpu.VMEM)
        hbm = pl.BlockSpec(memory_space=pl.ANY)
        shapes = [jax.ShapeDtypeStruct(a.shape, bf16) for a in (q2, q2, key, value)]
        outs = pl.pallas_call(
            functools.partial(kernel, tokens, heads, head),
            out_shape=[pltpu.VMEM(a.shape, bf16) for a in (q2, q2, key, value)],
            in_specs=[pl.BlockSpec(memory_space=pltpu.SMEM), hbm, hbm, hbm, hbm, hbm],
            out_specs=[vmem, vmem, vmem, vmem],
            scratch_shapes=scratch,
            compiler_params=pltpu.CompilerParams(collective_id=0, has_side_effects=True,
                                                 vmem_limit_bytes=58 * 1024 * 1024),
        )(positions, freq, key, value, q2, d2)
        outs = pl.pallas_call(
            write_kernel, out_shape=shapes,
            in_specs=[vmem, vmem, vmem, vmem], out_specs=[hbm, hbm, hbm, hbm],
            scratch_shapes=[D((4,))],
        )(*[pltpu.with_memory_space_constraint(o, V) for o in outs])
        out, dq, gk, gv = outs
        return out.reshape(query.shape), dq.reshape(query.shape), gk, gv

    return jax.shard_map(per_device, mesh=mesh, in_specs=(query_spec, kv_spec, kv_spec, pos_spec, query_spec),
                         out_specs=(query_spec, query_spec, kv_spec, kv_spec), check_vma=False)
```

```python
import functools
import math

import jax
import jax.numpy as jnp
from jax import lax
from jax.experimental import pallas as pl
from jax.experimental.pallas import tpu as pltpu
from jax.sharding import PartitionSpec as P

ROPE_BASE = 10000
CORES = 2
SIDE = 4
LOG2E = math.log2(math.e)

KEY_MSGS = (
    (0, 0, 0, 1, 0, None), (0, 0, None, 3, 2, None), (0, 0, 1, 1, 1, None),
    (1, 1, 1, 0, 0, None), (1, 1, 0, 2, 0, None), (1, 1, 1, 2, 3, None),
    (2, 2, None, 3, 0, None),
    (0, 1, 1, 3, 3, 0), (1, 0, 0, 2, 1, 0), (1, 0, 1, 2, 2, 1), (2, 1, 0, 3, 1, 0),
)
KEY_SLOTS = {(1, 0): (0, 1), (2, 1): (0, 3), (2, 0): (1, 2), (3, 2): (0,), (3, 1): (1, 3), (3, 0): (2,)}

DK_MSGS = (
    (3, 1, 0, 2, 0, None, None), (3, 1, 2, 0, 0, None, None), (3, 1, 1, 2, 1, None, None), (3, 1, 3, 0, 1, None, None),
    (3, 0, 3, 0, 5, None, None),
    (3, 2, 0, 2, 2, None, None), (3, 2, 1, 2, 3, None, None), (3, 2, 2, 2, 4, None, None), (3, 2, 3, 2, 5, None, None),
    (2, 0, 3, 1, 0, None, None), (2, 0, 0, 3, 0, None, None), (2, 0, 1, 3, 1, None, None), (2, 0, 2, 3, 2, None, None),
    (2, 1, 2, 1, 3, None, None), (2, 1, 3, 1, 4, None, None),
    (1, 0, 0, 0, 6, None, None), (1, 0, 1, 0, 7, None, None), (1, 0, 2, 0, 8, None, None),
    (3, 0, 0, 0, 2, 0, 0), (3, 0, 1, 0, 3, 1, 0), (3, 0, 2, 0, 4, 2, 1),
    (2, 1, 0, 1, 1, 0, 0), (2, 1, 1, 1, 2, 1, 1), (1, 0, 3, 0, 9, 0, 0),
)
DK_RELAY = ((0, 5), (1, 6))
DK_FINAL = {2: ((0, (2,)), (1, (3,)), (2, (4,)), (3, (5,))), 1: ((2, (3, 5)), (3, (4, 6)), (0, (1,)), (1, (2,))),
            0: ((3, (5, 9)), (0, (2, 6)), (1, (3, 7)), (2, (4, 8)))}
DV_VIA = ()
TILE_ORDER = {0: (0,), 1: (0, 1), 2: (0, 1, 2), 3: (1, 0, 2, 3)}


def rot_halves(x1, x2, c, s):
    return x1 * c - x2 * s, x2 * c + x1 * s


def kernel(tokens, heads, head,
           pos_hbm, key_hbm, val_hbm, q_hbm, do_hbm,
           out_ref, dq_ref, gk_ref, gv_ref,
           pos_ref, ang, key_in, val_in, tab_in, tabs, qbuf, dobuf, kst, kbuf, vbuf, krel, sbuf, dpbuf, dsbuf, mbuf, lbuf, lse, delta, oacc, obuf, dqbuf,
           dk_part, dv_part, rk, rv, vsum, fvb, rvy, rkx,
           sem_loc, sem_px, sem_kx, sem_vy, sem_vx, sem_ky_s, sem_ky_r,
           sem_dv_s, sem_dv_r, sem_dk_s, sem_dk_r, sem_fv_s, sem_fv_r, sem_fk_s, sem_fk_r, sem_fvb, sem_o):
    n = SIDE
    half = head // 2
    blk = CORES * tokens
    tile = n * blk
    ht = tile // 2
    nrow = tokens * heads
    scale = head ** -0.5
    c2 = scale * LOG2E
    f32, bf16 = jnp.float32, jnp.bfloat16
    me = lax.axis_index('cp')
    k = lax.rem(me, CORES)
    chip = lax.div(me, CORES)
    x = lax.rem(chip, n)
    y = lax.div(chip, n)
    other = 1 - k
    xr = lax.rem(x + 1, n)
    xo = lax.rem(x + 2, n)
    xl = lax.rem(x + 3, n)

    def dev(yy, xx, kk):
        return (yy * n + xx) * CORES + kk

    partner = dev(y, x, other)
    right, left = dev(y, xr, k), dev(y, xl, k)

    def rcopy(src, dst, ssem, rsem, target):
        return pltpu.make_async_remote_copy(src_ref=src, dst_ref=dst, send_sem=ssem, recv_sem=rsem,
                                            device_id={'cp': target}, device_id_type=pl.DeviceIdType.MESH)

    def at(i, size):
        return pl.ds(pl.multiple_of(i * size, size), size)
    bar = pltpu.get_barrier_semaphore()
    peers = [partner]
    for d in range(1, n):
        for b in range(CORES):
            peers.append(dev(y, lax.rem(x + d, n), b))
            peers.append(dev(lax.rem(y + d, n), x, b))
    for p in peers:
        pl.semaphore_signal(bar, inc=1, device_id={'cp': p}, device_id_type=pl.DeviceIdType.MESH)

    lf = pltpu.make_async_copy(pos_hbm, pos_ref, sem_loc.at[4])
    lk = pltpu.make_async_copy(key_hbm, key_in, sem_loc.at[5])
    lv = pltpu.make_async_copy(val_hbm, val_in, sem_loc.at[6])
    lq = pltpu.make_async_copy(q_hbm.at[k], qbuf.at[k], sem_loc.at[0])
    ld = pltpu.make_async_copy(do_hbm.at[k], dobuf.at[k], sem_loc.at[1])
    for cp in (lf, lk, lv, lq, ld):
        cp.start()

    pair = lax.broadcasted_iota(jnp.int32, (1, half), 1).astype(f32)
    freq = jnp.exp2(pair * (-2.0 * math.log2(ROPE_BASE) / head))
    lf.wait()
    for i in range(tokens):
        ang[pl.ds(i, 1), :] = jnp.full((1, half), pos_ref[i], jnp.int32).astype(f32)
    angles = ang[...] * freq
    tab_in[0] = jnp.cos(angles)
    tab_in[1] = jnp.sin(angles)

    lk.wait()
    lv.wait()
    for b in range(CORES):
        kf = key_in[b].astype(f32)
        r1, r2 = rot_halves(kf[:, :half], kf[:, half:], tab_in[0], tab_in[1])
        kst[b, :, :half] = r1.astype(bf16)
        kst[b, :, half:] = r2.astype(bf16)
    tabs[k] = tab_in[...]
    mine = at(x * CORES + k, tokens)
    kbuf[y, mine] = kst[k]
    vbuf[y, mine] = val_in[k]
    pl.semaphore_wait(bar, len(peers))
    pk = rcopy(kst.at[other], kbuf.at[y, mine], sem_px.at[0, 0], sem_px.at[1, 0], partner)
    pv = rcopy(val_in.at[other], vbuf.at[y, mine], sem_px.at[0, 1], sem_px.at[1, 1], partner)
    pt = rcopy(tab_in, tabs.at[k], sem_px.at[0, 2], sem_px.at[1, 2], partner)
    pq = rcopy(q_hbm.at[other], qbuf.at[k], sem_px.at[0, 3], sem_px.at[1, 3], partner)
    pd = rcopy(do_hbm.at[other], dobuf.at[k], sem_px.at[0, 4], sem_px.at[1, 4], partner)

    def kx_copy(d, b, src_core=None):
        return rcopy(kst.at[b], kbuf.at[y, mine], sem_kx.at[0, d - 1, b],
                     sem_kx.at[1, d - 1, k if src_core is None else src_core], dev(y, lax.rem(x + d, n), b))

    def vy_copy(d, b, src_core=None):
        return rcopy(val_in.at[b], vbuf.at[y, mine], sem_vy.at[0, d - 1, b],
                     sem_vy.at[1, d - 1, k if src_core is None else src_core], dev(lax.rem(y + d, n), x, b))

    pv.start()
    pk.start()
    for d in (2, 1, 3):
        for b in range(CORES):
            kx_copy(d, b).start()
    for d in (2, 1, 3):
        @pl.when(y + d < n)
        def _(d=d):
            for b in range(CORES):
                vy_copy(d, b).start()
    pt.start()
    pq.start()
    pd.start()

    def vx_copy(dy, i):
        t = lax.rem(y - dy + n, n)
        if i == 0:
            ref, target = vbuf.at[t, at(x, blk)], right
        elif i == 1:
            ref, target = vbuf.at[t, at(x, blk)], left
        elif i == 2:
            ref, target = vbuf.at[t, at(xl * CORES, tokens)], right
        else:
            ref, target = vbuf.at[t, at(xr * CORES + 1, tokens)], left
        return rcopy(ref, ref, sem_vx.at[0, dy, i], sem_vx.at[1, dy, i], target)

    def vx_relay(dy):
        vx_copy(dy, 0).wait_recv()
        vx_copy(dy, 2).start()
        vx_copy(dy, 1).wait_recv()
        vx_copy(dy, 3).start()

    def key_copy(i):
        src, t, hf, dst, slot, after = KEY_MSGS[i]
        ref = kbuf.at[t] if hf is None else kbuf.at[t, pl.ds(hf * ht, ht)]
        s_ref = krel if (src == 0 and after is not None) else ref
        d_ref = krel if dst == 0 else ref
        return rcopy(s_ref, d_ref, sem_ky_s.at[i], sem_ky_r.at[slot], dev(dst, x, k))

    def key_wait(row, slot):
        for i, m in enumerate(KEY_MSGS):
            if m[3] == row and m[4] == slot:
                key_copy(i).wait_recv()

    def rotate_queries(s):
        def rotate_rows(tok, carry):
            rows = at(tok, heads)
            c = tabs[s, 0, pl.ds(tok, 1), :]
            sn = tabs[s, 1, pl.ds(tok, 1), :]
            qf = qbuf[s, rows, :].astype(f32)
            r1, r2 = rot_halves(qf[:, :half], qf[:, half:], c, sn)
            qbuf[s, rows, :half] = r1.astype(bf16)
            qbuf[s, rows, half:] = r2.astype(bf16)
            return carry
        lax.fori_loop(0, tokens, rotate_rows, 0, unroll=8)
    pv.wait_recv()
    vx_copy(0, 0).start()
    vx_copy(0, 1).start()
    lq.wait()
    rotate_queries(k)
    for d in range(1, n):
        @pl.when(y - d >= 0)
        def _(d=d):
            for b in range(CORES):
                vy_copy(d, b, b).wait_recv()
            vx_copy(d, 0).start()
            vx_copy(d, 1).start()
    pt.wait_recv()
    pq.wait_recv()
    rotate_queries(other)
    vx_relay(0)
    pk.wait_recv()
    for d in range(1, n):
        for b in range(CORES):
            kx_copy(d, b, b).wait_recv()
    for r in range(n):
        @pl.when(y == r)
        def _(r=r):
            for i, m in enumerate(KEY_MSGS):
                if m[0] == r and m[5] is None:
                    key_copy(i).start()
    nt = (((1,), (1,)), ((), ()))
    tn = (((0,), (0,)), ((), ()))

    rf = 1024

    def first_scores(t):
        for s in range(CORES):
            sc = lax.dot_general(qbuf[s], kbuf[t], nt, preferred_element_type=f32)
            row_tok = (x * CORES + s) * tokens + lax.broadcasted_iota(jnp.int32, sc.shape, 0) // heads
            sc = jnp.where(lax.broadcasted_iota(jnp.int32, sc.shape, 1) <= row_tok, sc, -jnp.inf)
            sbuf[t, s] = sc
            mbuf[s] = jnp.broadcast_to(jnp.max(sc, axis=1, keepdims=True), (nrow, 128))

    def forward_tile(t, first):
        kt = kbuf.at[t]
        vt = vbuf.at[t]

        def rows_body(i, carry):
            for s in range(CORES):
                rows = at(i, rf)
                if first:
                    sc = sbuf[t, s, rows, :]
                    mx = mbuf[s, rows, :]
                else:
                    sc = lax.dot_general(qbuf[s, rows, :], kt[...], nt, preferred_element_type=f32)
                    sbuf[t, s, rows, :] = sc
                    old = mbuf[s, rows, :]
                    mx = jnp.maximum(old, jnp.max(sc, axis=1, keepdims=True))
                    fac = jnp.exp2((old - mx) * c2)
                    mbuf[s, rows, :] = mx
                mxw = jnp.concatenate([mx] * (tile // 128), axis=1)
                p = jnp.exp2((sc - mxw) * c2)
                tot = p[:, :128] + p[:, 128:]
                o = jnp.dot(p.astype(bf16), vt[...], preferred_element_type=f32)
                if not first:
                    tot = tot + lbuf[s, rows, :] * fac
                    o = o + oacc[s, rows, :] * jnp.concatenate([fac] * (head // 128), axis=1)
                lbuf[s, rows, :] = tot
                oacc[s, rows, :] = o
                dpbuf[t, s, rows, :] = lax.dot_general(dobuf[s, rows, :], vt[...], nt, preferred_element_type=f32)
            return carry
        if nrow == rf:
            rows_body(0, 0)
        else:
            lax.fori_loop(0, nrow // rf, rows_body, 0)
    first_scores(y)
    ld.wait()
    pd.wait_recv()
    for d in range(1, n):
        @pl.when(y - d >= 0)
        def _(d=d):
            vx_relay(d)
    vx_copy(0, 2).wait_recv()
    vx_copy(0, 3).wait_recv()
    forward_tile(y, True)
    for r in range(n - 1):
        @pl.when(y == r)
        def _(r=r):
            for i, m in enumerate(KEY_MSGS):
                if m[0] == r and m[5] is not None:
                    key_wait(r, m[5])
                    key_copy(i).start()
    for j, d in enumerate((1, n - 1, 2)):
        dd = jnp.where(y == n - 1, d, j + 1)

        @pl.when(y - (j + 1) >= 0)
        def _(j=j, d=d, dd=dd):
            t = y - dd
            for r in range(n):
                tr = r - (d if r == n - 1 else j + 1)
                if tr < 0:
                    continue

                @pl.when(y == r)
                def _(r=r, tr=tr):
                    for slot in KEY_SLOTS[(r, tr)]:
                        if not any(m[0] == r and m[5] == slot for m in KEY_MSGS):
                            key_wait(r, slot)
                    vx_copy(r - tr, 2).wait_recv()
                    vx_copy(r - tr, 3).wait_recv()
            forward_tile(t, False)
    rc = 256

    for i in range(nrow // rc):
        for s, dst in ((other, obuf), (k, out_ref.at[k])):
            rows = pl.ds(i * rc, rc)
            tot = jnp.sum(lbuf[s, rows, :], axis=1, keepdims=True)
            inv = 1.0 / tot
            ob = (oacc[s, rows, :] * inv).astype(bf16)
            dst[rows, :] = ob
            dl = jnp.sum(ob.astype(f32) * dobuf[s, rows, :].astype(f32), axis=1, keepdims=True)
            lse[s, rows, :] = mbuf[s, rows, :] * c2 + jnp.broadcast_to(jnp.log2(tot), (rc, 128))
            delta[s, rows, :] = jnp.broadcast_to(dl, (rc, 128))
    orem = rcopy(obuf, out_ref.at[k], sem_o.at[0, 0], sem_o.at[1, 0], partner)
    def dv_copy(t, i):
        xt = (xo, xr, xr, xo, xl, xl)[i]
        hf = (0, 1, 0, 1, 0, 1)[i]
        return rcopy(dv_part.at[t, at(xt * CORES + hf, tokens)], rv.at[t, i], sem_dv_s.at[t, i], sem_dv_r.at[t, i],
                     right if i < 3 else left)

    def dv_combine(t):
        for i in (0, 3):
            dv_copy(t, i).wait_recv()
            rows = at(xr * CORES, tokens) if i == 0 else at(xl * CORES + 1, tokens)
            dv_part[t, rows] = dv_part[t, rows] + rv[t, i]
            dv_copy(t, i + 2).start()

    def dk_copy(i):
        src, t, qt, dst, slot = DK_MSGS[i][:5]
        return rcopy(dk_part.at[t, pl.ds(qt * blk, blk)], rk.at[slot], sem_dk_s.at[i], sem_dk_r.at[slot], dev(dst, x, k))

    def dk_relay(i):
        src, dst = DK_RELAY[i]
        return rcopy(rk.at[src], rk.at[dst], sem_dk_s.at[len(DK_MSGS) + i], sem_dk_r.at[dst], dev(1, x, k))

    def dk_wait(slot):
        rcopy(rk.at[slot], rk.at[slot], sem_dk_s.at[0], sem_dk_r.at[slot], partner).wait_recv()

    def dk_combine(e):
        @pl.when(y == 0)
        def _():
            dk_wait(DK_RELAY[e][0])
            dk_relay(e).start()
        for r in range(1, n):
            @pl.when(y == r)
            def _(r=r):
                for i, m in enumerate(DK_MSGS):
                    if m[0] == r and m[6] == e:
                        dk_wait(m[5])
                        rows = pl.ds(m[2] * blk, blk)
                        dk_part[m[1], rows] = dk_part[m[1], rows] + rk[m[5]]
                        dk_copy(i).start()

    def fv_copy(t, c):
        dst = dev(t, x, c)
        return rcopy(vsum.at[t, c], rvy.at[y - t, k], sem_fv_s.at[t, c], sem_fv_r.at[y - t, k], dst)

    def fv_via(row):
        t = {2: 1, 1: 0}[row]
        return rcopy(vsum.at[t], fvb, sem_fvb.at[0], sem_fvb.at[1], dev(row, x, k))

    def fv_own():
        return rcopy(vsum.at[y, other], rvy.at[0, k], sem_fv_s.at[y, other], sem_fv_r.at[0, k], partner)

    def fk_copy(d, c, src_core=None):
        xt = lax.rem(x + d, n)
        return rcopy(dk_part.at[y, at(xt * CORES + c, tokens)], rkx.at[d, k], sem_fk_s.at[d, c],
                     sem_fk_r.at[d, k if src_core is None else src_core], dev(y, xt, c))

    def fk_own(src_core=None):
        return rcopy(dk_part.at[y, at(x * CORES + other, tokens)], rkx.at[0, k], sem_fk_s.at[0, 0],
                     sem_fk_r.at[0, k if src_core is None else src_core], partner)

    def fk_quarter(xt):
        @pl.when(x != xt)
        def _():
            d = lax.rem(xt - x + n, n)
            for c in range(CORES):
                rcopy(dk_part.at[y, pl.ds(xt * blk + c * tokens, tokens)], rkx.at[d, k], sem_fk_s.at[d, c],
                      sem_fk_r.at[d, k], dev(y, xt, c)).start()

        @pl.when(x == xt)
        def _():
            fk_own().start()

    rb = 512

    def backward_tile(t):
        dva = None
        dka = None
        for s in range(CORES):
            for i in range(nrow // rb):
                rows = pl.ds(i * rb, rb)
                ls = lse[s, rows, :]
                dl = delta[s, rows, :]
                p = jnp.exp2(sbuf[t, s, rows, :] * c2 - jnp.concatenate([ls] * (tile // 128), axis=1))
                ds = (p * (dpbuf[t, s, rows, :] - jnp.concatenate([dl] * (tile // 128), axis=1))).astype(bf16)
                dsbuf[t, s, rows, :] = ds
                a = lax.dot_general(p.astype(bf16), dobuf[s, rows, :], tn, preferred_element_type=f32)
                dva = a if dva is None else dva + a
                a = lax.dot_general(ds, qbuf[s, rows, :], tn, preferred_element_type=f32)
                dka = a if dka is None else dka + a
        dv_part[t] = dva
        dk_part[t] = dka * scale

    def dv_order(i):
        t = i
        for r in range(n):
            if i < len(TILE_ORDER[r]):
                t = jnp.where(y == r, TILE_ORDER[r][i], t)
        return t

    def dv_turn(i):
        @pl.when(y >= i)
        def _():
            dv_combine(dv_order(i))

    for i in range(n):
        if i == 0:
            backward_tile(dv_order(0))

        @pl.when(y >= i)
        def _(i=i):
            t = dv_order(i)
            if i > 0:
                backward_tile(t)
            for m in ((0, 3, 1, 4) if i < 2 else (0, 3)):
                dv_copy(t, m).start()
            for r in range(n):
                if i < len(TILE_ORDER[r]):
                    @pl.when(y == r)
                    def _(r=r):
                        for j, m in enumerate(DK_MSGS):
                            if m[0] == r and m[1] == TILE_ORDER[r][i] and m[5] is None:
                                dk_copy(j).start()

        @pl.when(y < i)
        def _(i=i):
            dsbuf[i] = jnp.zeros(dsbuf.shape[1:], bf16)
            kbuf[i] = jnp.zeros(kbuf.shape[1:], bf16)

        if i == 0:
            orem.start()
        if i >= 2:
            dv_turn(i - 2)
        if i == n - 1:
            for j in range(2, n):
                @pl.when(y >= j)
                def _(j=j):
                    t = dv_order(j)
                    for m in (1, 4):
                        dv_copy(t, m).start()
    dk_combine(0)

    def grad_query_half(s, dst):
        def dq_rows(i, carry):
            rows = at(i, rc)
            acc = None
            for t in range(n):
                a = jnp.dot(dsbuf[t, s, rows, :], kbuf[t], preferred_element_type=f32)
                acc = a if acc is None else acc + a
            acc = acc * scale
            for j in range(rc // heads):
                tok = i * (rc // heads) + j
                c = tabs[s, 0, pl.ds(tok, 1), :]
                sn = tabs[s, 1, pl.ds(tok, 1), :]
                g = acc[j * heads:(j + 1) * heads]
                r1, r2 = rot_halves(g[:, :half], g[:, half:], c, -sn)
                orow = at(tok, heads)
                dst[orow, :half] = r1.astype(bf16)
                dst[orow, half:] = r2.astype(bf16)
            return carry
        lax.fori_loop(0, nrow // rc, dq_rows, 0, unroll=2)
    grad_query_half(other, dqbuf)
    qrem = rcopy(dqbuf, dq_ref.at[k], sem_o.at[0, 1], sem_o.at[1, 1], partner)
    qrem.start()
    dk_combine(1)

    def dv_total(j):
        @pl.when(y >= j)
        def _():
            t = dv_order(j)
            for i in (1, 2, 4, 5):
                dv_copy(t, i).wait_recv()
            vsum[t, 0] = dv_part[t, at(x * CORES, tokens)] + rv[t, 2] + rv[t, 4]
            vsum[t, 1] = dv_part[t, at(x * CORES + 1, tokens)] + rv[t, 1] + rv[t, 5]
            for r, t_on, via in DV_VIA:
                @pl.when((y == r) & (t == t_on))
                def _(via=via):
                    fv_via(via).start()

            direct = y > t
            for r, t_on, via in DV_VIA:
                direct = direct & ((y != r) | (t != t_on)) & ((y != via) | (t != t_on))

            @pl.when(direct)
            def _():
                for c in range(CORES):
                    fv_copy(t, c).start()

    def dv_via(r, t_on):
        @pl.when(y == r)
        def _():
            fv_via(r).wait_recv()
            vsum[t_on] = vsum[t_on] + fvb[...]
            for c in range(CORES):
                fv_copy(t_on, c).start()

    def dk_final(part):
        for r in range(n - 1):
            @pl.when(y == r)
            def _(r=r):
                for qt, slots in DK_FINAL[r][2 * part:2 * part + 2]:
                    rows = pl.ds(qt * blk, blk)
                    acc = dk_part[r, rows]
                    for slot in slots:
                        dk_wait(slot)
                        acc = acc + rk[slot]
                    dk_part[r, rows] = acc
                    fk_quarter(qt)
    dv_turn(2)
    dv_total(0)
    dv_turn(3)

    @pl.when(y == n - 1)
    def _():
        for xt in range(n):
            fk_quarter(xt)
    dv_total(1)
    grad_query_half(k, dq_ref.at[k])
    dv_total(2)
    dv_total(3)
    fv_own().start()
    dk_final(0)
    for r, t_on, via in DV_VIA:
        dv_via(via, t_on)
    dk_final(1)
    def fv_wait(d, b):
        rcopy(rvy.at[d, b], rvy.at[d, b], sem_fv_s.at[0, 0], sem_fv_r.at[d, b], partner).wait_recv()

    fv_wait(0, other)
    rvy[0, k] = vsum[y, k]
    for d in range(1, n):
        expect = y + d < n
        for r, t_on, via in DV_VIA:
            if r - t_on == d:
                expect = expect & (y != t_on)

        @pl.when(expect)
        def _(d=d):
            for b in range(CORES):
                fv_wait(d, b)
                rvy[0, b] = rvy[0, b] + rvy[d, b]
    for b in range(CORES):
        gv_ref[b] = rvy[0, b].astype(bf16)
    fk_own(other).wait_recv()
    rkx[0, k] = dk_part[y, at(x * CORES + k, tokens)]
    for d in range(1, n):
        for b in range(CORES):
            fk_copy(d, 0, b).wait_recv()
    ct, st = tab_in[0], tab_in[1]
    for b in range(CORES):
        g = rkx[0, b] + rkx[1, b] + rkx[2, b] + rkx[3, b]
        r1, r2 = rot_halves(g[:, :half], g[:, half:], ct, -st)
        gk_ref[b, :, :half] = r1.astype(bf16)
        gk_ref[b, :, half:] = r2.astype(bf16)
    for cp in (pk, pv, pt, pq, pd):
        cp.wait_send()
    for d in range(1, n):
        for b in range(CORES):
            kx_copy(d, b).wait_send()
            fk_copy(d, b).wait_send()

        @pl.when(y + d < n)
        def _(d=d):
            for b in range(CORES):
                vy_copy(d, b).wait_send()
    fk_own().wait_send()
    fv_own().wait_send()
    for d in range(n):
        @pl.when(y - d >= 0)
        def _(d=d):
            for i in range(4):
                vx_copy(d, i).wait_send()
    for r in range(n):
        @pl.when(y == r)
        def _(r=r):
            for i, m in enumerate(KEY_MSGS):
                if m[0] == r:
                    key_copy(i).wait_send()
            for i, m in enumerate(DK_MSGS):
                if m[0] == r:
                    dk_copy(i).wait_send()
            if r == 0:
                for i in range(len(DK_RELAY)):
                    dk_relay(i).wait_send()
    for t in range(n):
        @pl.when(y >= t)
        def _(t=t):
            for i in range(6):
                dv_copy(t, i).wait_send()

        sent = y > t
        for r, t_on, via in DV_VIA:
            if t == t_on:
                sent = sent & (y != r)

        @pl.when(sent)
        def _(t=t):
            for c in range(CORES):
                fv_copy(t, c).wait_send()
    for r, t_on, via in DV_VIA:
        @pl.when(y == r)
        def _(via=via):
            fv_via(via).wait_send()
    orem.wait()
    qrem.wait()


def write_kernel(a, b, c, d, ao, bo, co, do, sem):
    pieces = 1
    cps = []
    for src, dst in ((a, ao), (b, bo)):
        rows = src.shape[1] // pieces
        for e in range(src.shape[0]):
            for i in range(pieces):
                at = (e, pl.ds(i * rows, rows))
                cps.append(pltpu.make_async_copy(src.at[at], dst.at[at], sem.at[len(cps)]))
    for src, dst in ((c, co), (d, do)):
        cps.append(pltpu.make_async_copy(src, dst, sem.at[len(cps)]))
    for cp in cps:
        cp.start()
    for cp in cps:
        cp.wait()


def solution(mesh):
    cp_size = mesh.shape['cp']
    n = SIDE
    assert cp_size == n * n * CORES
    query_spec = P('dp', 'cp', None, None)
    kv_spec = P('dp', 'cp', None)
    pos_spec = P(('dp', 'cp'))

    def per_device(query, key, value, positions, grad_out):
        batch, tokens, heads, head = query.shape
        nrow = tokens * heads
        q2 = query.reshape(batch, nrow, head)
        d2 = grad_out.reshape(batch, nrow, head)
        blk = CORES * tokens
        tile = n * blk
        bf16, f32 = jnp.bfloat16, jnp.float32
        V = pltpu.VMEM
        D = pltpu.SemaphoreType.DMA
        scratch = [
            pltpu.SMEM((tokens,), jnp.int32),
            V((tokens, head // 2), f32),
            V((batch, tokens, head), bf16),
            V((batch, tokens, head), bf16),
            V((2, tokens, head // 2), f32),
            V((CORES, 2, tokens, head // 2), f32),
            V((CORES, nrow, head), bf16),
            V((CORES, nrow, head), bf16),
            V((CORES, tokens, head), bf16),
            V((n, tile, head), bf16),
            V((n, tile, head), bf16),
            V((tile // 2, head), bf16),
            V((n, CORES, nrow, tile), f32),
            V((n, CORES, nrow, tile), f32),
            V((n, CORES, nrow, tile), bf16),
            V((CORES, nrow, 128), f32),
            V((CORES, nrow, 128), f32),
            V((CORES, nrow, 128), f32),
            V((CORES, nrow, 128), f32),
            V((CORES, nrow, head), f32),
            V((nrow, head), bf16),
            V((nrow, head), bf16),
            V((n, tile, head), f32),
            V((n, tile, head), f32),
            V((10, blk, head), f32),
            V((n, 6, tokens, head), f32),
            V((n, CORES, tokens, head), f32),
            V((CORES, tokens, head), f32),
            V((n, CORES, tokens, head), f32),
            V((n, CORES, tokens, head), f32),
            D((7,)), D((2, 5)), D((2, n - 1, CORES)), D((2, n - 1, CORES)), D((2, n, 4)),
            D((len(KEY_MSGS),)), D((4,)),
            D((n, 6)), D((n, 6)), D((len(DK_MSGS) + 2,)), D((10,)),
            D((n, CORES)), D((n, CORES)), D((n, CORES)), D((n, CORES)), D((2,)), D((2, 2)),
        ]
        vmem = pl.BlockSpec(memory_space=pltpu.VMEM)
        hbm = pl.BlockSpec(memory_space=pl.ANY)
        shapes = [jax.ShapeDtypeStruct(a.shape, bf16) for a in (q2, q2, key, value)]
        outs = pl.pallas_call(
            functools.partial(kernel, tokens, heads, head),
            out_shape=[pltpu.VMEM(a.shape, bf16) for a in (q2, q2, key, value)],
            in_specs=[hbm] * 5,
            out_specs=[vmem, vmem, vmem, vmem],
            scratch_shapes=scratch,
            compiler_params=pltpu.CompilerParams(collective_id=0, has_side_effects=True,
                                                 vmem_limit_bytes=58 * 1024 * 1024),
        )(positions, key, value, q2, d2)
        outs = pl.pallas_call(
            write_kernel, out_shape=shapes,
            in_specs=[vmem, vmem, vmem, vmem], out_specs=[hbm, hbm, hbm, hbm],
            scratch_shapes=[D((4 * 1 + 2,))],
        )(*[pltpu.with_memory_space_constraint(o, V) for o in outs])
        out, dq, gk, gv = outs
        return out.reshape(query.shape), dq.reshape(query.shape), gk, gv

    return jax.shard_map(per_device, mesh=mesh, in_specs=(query_spec, kv_spec, kv_spec, pos_spec, query_spec),
                         out_specs=(query_spec, query_spec, kv_spec, kv_spec), check_vma=False)
```

```python
import functools
import math

import jax
import jax.numpy as jnp
from jax import lax
from jax.experimental import pallas as pl
from jax.experimental.pallas import tpu as pltpu
from jax.sharding import PartitionSpec as P

ROPE_BASE = 10000
CORES = 2
SIDE = 4
LOG2E = math.log2(math.e)

KEY_MSGS = (
    (0, 0, 0, 1, 0, None), (0, 0, None, 3, 2, None), (0, 0, 1, 1, 1, None),
    (1, 1, 1, 0, 0, None), (1, 1, 0, 2, 0, None), (1, 1, 1, 2, 3, None),
    (2, 2, None, 3, 0, None),
    (0, 1, 1, 3, 3, 0), (1, 0, 0, 2, 1, 0), (1, 0, 1, 2, 2, 1), (2, 1, 0, 3, 1, 0),
)
KEY_SLOTS = {(1, 0): (0, 1), (2, 1): (0, 3), (2, 0): (1, 2), (3, 2): (0,), (3, 1): (1, 3), (3, 0): (2,)}

DK_MSGS = (
    (3, 1, 0, 2, 0, None, None), (3, 1, 2, 0, 0, None, None), (3, 1, 1, 2, 1, None, None), (3, 1, 3, 2, 6, None, None),
    (3, 0, 3, 0, 5, None, None),
    (3, 2, 0, 2, 2, None, None), (3, 2, 1, 2, 3, None, None), (3, 2, 2, 2, 4, None, None), (3, 2, 3, 2, 5, None, None),
    (2, 0, 3, 1, 0, None, None), (2, 0, 0, 3, 0, None, None), (2, 0, 1, 3, 1, None, None), (2, 0, 2, 3, 2, None, None),
    (2, 1, 2, 1, 3, None, None),
    (1, 0, 0, 0, 6, None, None), (1, 0, 1, 0, 7, None, None), (1, 0, 2, 0, 8, None, None),
    (3, 0, 0, 0, 2, 0, 0), (3, 0, 1, 0, 3, 1, 0), (3, 0, 2, 0, 4, 2, 1),
    (2, 1, 0, 1, 1, 0, 0), (2, 1, 1, 1, 2, 1, 1), (2, 1, 3, 1, 4, 6, 1), (1, 0, 3, 0, 9, 0, 0),
)
DK_RELAY = ((0, 5),)
DK_FINAL = {2: ((0, (2,)), (1, (3,)), (2, (4,)), (3, (5,))), 1: ((2, (3, 5)), (0, (1,)), (1, (2,)), (3, (4,))),
            0: ((3, (5, 9)), (0, (2, 6)), (1, (3, 7)), (2, (4, 8)))}
DV_VIA = ()
TILE_ORDER = {0: (0,), 1: (0, 1), 2: (0, 1, 2), 3: (1, 0, 2, 3)}


def rot_halves(x1, x2, c, s):
    return x1 * c - x2 * s, x2 * c + x1 * s


def kernel(tokens, heads, head,
           pos_hbm, key_hbm, val_hbm, q_hbm, do_hbm,
           out_ref, dq_ref, gk_ref, gv_ref,
           pos_ref, ang, key_in, val_in, tab_in, tabs, qbuf, dobuf, kst, kbuf, vbuf, krel, sbuf, dpbuf, dsbuf, mbuf, lbuf, lse, delta, oacc, obuf, dqbuf,
           dk_part, dv_part, rk, rv, vsum, fvb, rvy, rkx,
           sem_loc, sem_px, sem_kx, sem_vy, sem_vx, sem_ky_s, sem_ky_r,
           sem_dv_s, sem_dv_r, sem_dk_s, sem_dk_r, sem_fv_s, sem_fv_r, sem_fk_s, sem_fk_r, sem_fvb, sem_o):
    n = SIDE
    half = head // 2
    blk = CORES * tokens
    tile = n * blk
    ht = tile // 2
    nrow = tokens * heads
    scale = head ** -0.5
    c2 = scale * LOG2E
    f32, bf16 = jnp.float32, jnp.bfloat16
    me = lax.axis_index('cp')
    k = lax.rem(me, CORES)
    chip = lax.div(me, CORES)
    x = lax.rem(chip, n)
    y = lax.div(chip, n)
    other = 1 - k
    xr = lax.rem(x + 1, n)
    xo = lax.rem(x + 2, n)
    xl = lax.rem(x + 3, n)

    def dev(yy, xx, kk):
        return (yy * n + xx) * CORES + kk

    partner = dev(y, x, other)
    right, left = dev(y, xr, k), dev(y, xl, k)

    def rcopy(src, dst, ssem, rsem, target):
        return pltpu.make_async_remote_copy(src_ref=src, dst_ref=dst, send_sem=ssem, recv_sem=rsem,
                                            device_id={'cp': target}, device_id_type=pl.DeviceIdType.MESH)

    def at(i, size):
        return pl.ds(pl.multiple_of(i * size, size), size)
    bar = pltpu.get_barrier_semaphore()
    peers = [partner]
    for d in range(1, n):
        for b in range(CORES):
            peers.append(dev(y, lax.rem(x + d, n), b))
            peers.append(dev(lax.rem(y + d, n), x, b))
    for p in peers:
        pl.semaphore_signal(bar, inc=1, device_id={'cp': p}, device_id_type=pl.DeviceIdType.MESH)

    lf = pltpu.make_async_copy(pos_hbm, pos_ref, sem_loc.at[4])
    lk = pltpu.make_async_copy(key_hbm, key_in, sem_loc.at[5])
    lv = pltpu.make_async_copy(val_hbm, val_in, sem_loc.at[6])
    lq = pltpu.make_async_copy(q_hbm.at[k], qbuf.at[k], sem_loc.at[0])
    ld = pltpu.make_async_copy(do_hbm.at[k], dobuf.at[k], sem_loc.at[1])
    for cp in (lf, lk, lv, lq, ld):
        cp.start()

    pair = lax.broadcasted_iota(jnp.int32, (1, half), 1).astype(f32)
    freq = jnp.exp2(pair * (-2.0 * math.log2(ROPE_BASE) / head))
    lf.wait()
    for i in range(tokens):
        ang[pl.ds(i, 1), :] = jnp.full((1, half), pos_ref[i], jnp.int32).astype(f32)
    angles = ang[...] * freq
    tab_in[0] = jnp.cos(angles)
    tab_in[1] = jnp.sin(angles)

    lk.wait()
    lv.wait()
    for b in range(CORES):
        kf = key_in[b].astype(f32)
        r1, r2 = rot_halves(kf[:, :half], kf[:, half:], tab_in[0], tab_in[1])
        kst[b, :, :half] = r1.astype(bf16)
        kst[b, :, half:] = r2.astype(bf16)
    tabs[k] = tab_in[...]
    mine = at(x * CORES + k, tokens)
    kbuf[y, mine] = kst[k]
    vbuf[y, mine] = val_in[k]
    pl.semaphore_wait(bar, len(peers))
    pk = rcopy(kst.at[other], kbuf.at[y, mine], sem_px.at[0, 0], sem_px.at[1, 0], partner)
    pv = rcopy(val_in.at[other], vbuf.at[y, mine], sem_px.at[0, 1], sem_px.at[1, 1], partner)
    pt = rcopy(tab_in, tabs.at[k], sem_px.at[0, 2], sem_px.at[1, 2], partner)
    pq = rcopy(q_hbm.at[other], qbuf.at[k], sem_px.at[0, 3], sem_px.at[1, 3], partner)
    pd = rcopy(do_hbm.at[other], dobuf.at[k], sem_px.at[0, 4], sem_px.at[1, 4], partner)

    def kx_copy(d, b, src_core=None):
        return rcopy(kst.at[b], kbuf.at[y, mine], sem_kx.at[0, d - 1, b],
                     sem_kx.at[1, d - 1, k if src_core is None else src_core], dev(y, lax.rem(x + d, n), b))

    def vy_copy(d, b, src_core=None):
        return rcopy(val_in.at[b], vbuf.at[y, mine], sem_vy.at[0, d - 1, b],
                     sem_vy.at[1, d - 1, k if src_core is None else src_core], dev(lax.rem(y + d, n), x, b))

    pv.start()
    pk.start()
    for d in (2, 1, 3):
        for b in range(CORES):
            kx_copy(d, b).start()
    for d in (2, 1, 3):
        @pl.when(y + d < n)
        def _(d=d):
            for b in range(CORES):
                vy_copy(d, b).start()
    pt.start()
    pq.start()
    pd.start()

    def vx_copy(dy, i):
        t = lax.rem(y - dy + n, n)
        if i == 0:
            ref, target = vbuf.at[t, at(x, blk)], right
        elif i == 1:
            ref, target = vbuf.at[t, at(x, blk)], left
        elif i == 2:
            ref, target = vbuf.at[t, at(xl * CORES, tokens)], right
        else:
            ref, target = vbuf.at[t, at(xr * CORES + 1, tokens)], left
        return rcopy(ref, ref, sem_vx.at[0, dy, i], sem_vx.at[1, dy, i], target)

    def vx_relay(dy):
        vx_copy(dy, 0).wait_recv()
        vx_copy(dy, 2).start()
        vx_copy(dy, 1).wait_recv()
        vx_copy(dy, 3).start()

    def key_copy(i):
        src, t, hf, dst, slot, after = KEY_MSGS[i]
        ref = kbuf.at[t] if hf is None else kbuf.at[t, pl.ds(hf * ht, ht)]
        s_ref = krel if (src == 0 and after is not None) else ref
        d_ref = krel if dst == 0 else ref
        return rcopy(s_ref, d_ref, sem_ky_s.at[i], sem_ky_r.at[slot], dev(dst, x, k))

    def key_wait(row, slot):
        for i, m in enumerate(KEY_MSGS):
            if m[3] == row and m[4] == slot:
                key_copy(i).wait_recv()

    def rotate_queries(s):
        def rotate_rows(tok, carry):
            rows = at(tok, heads)
            c = tabs[s, 0, pl.ds(tok, 1), :]
            sn = tabs[s, 1, pl.ds(tok, 1), :]
            qf = qbuf[s, rows, :].astype(f32)
            r1, r2 = rot_halves(qf[:, :half], qf[:, half:], c, sn)
            qbuf[s, rows, :half] = r1.astype(bf16)
            qbuf[s, rows, half:] = r2.astype(bf16)
            return carry
        lax.fori_loop(0, tokens, rotate_rows, 0, unroll=8)
    pv.wait_recv()
    vx_copy(0, 0).start()
    vx_copy(0, 1).start()
    lq.wait()
    rotate_queries(k)
    for d in range(1, n):
        @pl.when(y - d >= 0)
        def _(d=d):
            for b in range(CORES):
                vy_copy(d, b, b).wait_recv()
            vx_copy(d, 0).start()
            vx_copy(d, 1).start()
    pt.wait_recv()
    pq.wait_recv()
    rotate_queries(other)
    vx_relay(0)
    pk.wait_recv()
    for d in range(1, n):
        for b in range(CORES):
            kx_copy(d, b, b).wait_recv()
    for r in range(n):
        @pl.when(y == r)
        def _(r=r):
            for i, m in enumerate(KEY_MSGS):
                if m[0] == r and m[5] is None:
                    key_copy(i).start()
    nt = (((1,), (1,)), ((), ()))
    tn = (((0,), (0,)), ((), ()))

    rf = 1024

    def first_scores(t):
        for s in range(CORES):
            sc = lax.dot_general(qbuf[s], kbuf[t], nt, preferred_element_type=f32)
            row_tok = (x * CORES + s) * tokens + lax.broadcasted_iota(jnp.int32, sc.shape, 0) // heads
            sc = jnp.where(lax.broadcasted_iota(jnp.int32, sc.shape, 1) <= row_tok, sc, -jnp.inf)
            sbuf[t, s] = sc
            mbuf[s] = jnp.broadcast_to(jnp.max(sc, axis=1, keepdims=True), (nrow, 128))

    def forward_tile(t, first):
        kt = kbuf.at[t]
        vt = vbuf.at[t]

        def rows_body(i, carry):
            for s in range(CORES):
                rows = at(i, rf)
                if first:
                    sc = sbuf[t, s, rows, :]
                    mx = mbuf[s, rows, :]
                else:
                    sc = lax.dot_general(qbuf[s, rows, :], kt[...], nt, preferred_element_type=f32)
                    sbuf[t, s, rows, :] = sc
                    old = mbuf[s, rows, :]
                    mx = jnp.maximum(old, jnp.max(sc, axis=1, keepdims=True))
                    fac = jnp.exp2((old - mx) * c2)
                    mbuf[s, rows, :] = mx
                mxw = jnp.concatenate([mx] * (tile // 128), axis=1)
                p = jnp.exp2((sc - mxw) * c2)
                tot = p[:, :128] + p[:, 128:]
                o = jnp.dot(p.astype(bf16), vt[...], preferred_element_type=f32)
                if not first:
                    tot = tot + lbuf[s, rows, :] * fac
                    o = o + oacc[s, rows, :] * jnp.concatenate([fac] * (head // 128), axis=1)
                lbuf[s, rows, :] = tot
                oacc[s, rows, :] = o
                dpbuf[t, s, rows, :] = lax.dot_general(dobuf[s, rows, :], vt[...], nt, preferred_element_type=f32)
            return carry
        if nrow == rf:
            rows_body(0, 0)
        else:
            lax.fori_loop(0, nrow // rf, rows_body, 0)
    first_scores(y)
    ld.wait()
    pd.wait_recv()
    for d in range(1, n):
        @pl.when(y - d >= 0)
        def _(d=d):
            vx_relay(d)
    vx_copy(0, 2).wait_recv()
    vx_copy(0, 3).wait_recv()
    forward_tile(y, True)
    for r in range(n - 1):
        @pl.when(y == r)
        def _(r=r):
            for i, m in enumerate(KEY_MSGS):
                if m[0] == r and m[5] is not None:
                    key_wait(r, m[5])
                    key_copy(i).start()
    for j, d in enumerate((1, n - 1, 2)):
        dd = jnp.where(y == n - 1, d, j + 1)

        @pl.when(y - (j + 1) >= 0)
        def _(j=j, d=d, dd=dd):
            t = y - dd
            for r in range(n):
                tr = r - (d if r == n - 1 else j + 1)
                if tr < 0:
                    continue

                @pl.when(y == r)
                def _(r=r, tr=tr):
                    for slot in KEY_SLOTS[(r, tr)]:
                        if not any(m[0] == r and m[5] == slot for m in KEY_MSGS):
                            key_wait(r, slot)
                    vx_copy(r - tr, 2).wait_recv()
                    vx_copy(r - tr, 3).wait_recv()
            forward_tile(t, False)
    rc = 256

    for i in range(nrow // rc):
        for s, dst in ((other, obuf), (k, out_ref.at[k])):
            rows = pl.ds(i * rc, rc)
            tot = jnp.sum(lbuf[s, rows, :], axis=1, keepdims=True)
            inv = 1.0 / tot
            ob = (oacc[s, rows, :] * inv).astype(bf16)
            dst[rows, :] = ob
            dl = jnp.sum(ob.astype(f32) * dobuf[s, rows, :].astype(f32), axis=1, keepdims=True)
            lse[s, rows, :] = mbuf[s, rows, :] * c2 + jnp.broadcast_to(jnp.log2(tot), (rc, 128))
            delta[s, rows, :] = jnp.broadcast_to(dl, (rc, 128))
    orem = rcopy(obuf, out_ref.at[k], sem_o.at[0, 0], sem_o.at[1, 0], partner)
    def dv_copy(t, i):
        xt = (xo, xr, xr, xo, xl, xl)[i]
        hf = (0, 1, 0, 1, 0, 1)[i]
        return rcopy(dv_part.at[t, at(xt * CORES + hf, tokens)], rv.at[t, i], sem_dv_s.at[t, i], sem_dv_r.at[t, i],
                     right if i < 3 else left)

    def dv_combine(t):
        for i in (0, 3):
            dv_copy(t, i).wait_recv()
            rows = at(xr * CORES, tokens) if i == 0 else at(xl * CORES + 1, tokens)
            dv_part[t, rows] = dv_part[t, rows] + rv[t, i]
            dv_copy(t, i + 2).start()

    def dk_copy(i):
        src, t, qt, dst, slot = DK_MSGS[i][:5]
        return rcopy(dk_part.at[t, pl.ds(qt * blk, blk)], rk.at[slot], sem_dk_s.at[i], sem_dk_r.at[slot], dev(dst, x, k))

    def dk_relay(i):
        src, dst = DK_RELAY[i]
        return rcopy(rk.at[src], rk.at[dst], sem_dk_s.at[len(DK_MSGS) + i], sem_dk_r.at[dst], dev(1, x, k))

    def dk_wait(slot):
        rcopy(rk.at[slot], rk.at[slot], sem_dk_s.at[0], sem_dk_r.at[slot], partner).wait_recv()

    def dk_combine(e, rows_here):
        if 0 in rows_here and e < len(DK_RELAY):
            @pl.when(y == 0)
            def _():
                dk_wait(DK_RELAY[e][0])
                dk_relay(e).start()
        for r in range(1, n):
            if r not in rows_here:
                continue
            @pl.when(y == r)
            def _(r=r):
                for i, m in enumerate(DK_MSGS):
                    if m[0] == r and m[6] == e:
                        dk_wait(m[5])
                        rows = pl.ds(m[2] * blk, blk)
                        dk_part[m[1], rows] = dk_part[m[1], rows] + rk[m[5]]
                        dk_copy(i).start()

    def fv_copy(t, c):
        dst = dev(t, x, c)
        return rcopy(vsum.at[t, c], rvy.at[y - t, k], sem_fv_s.at[t, c], sem_fv_r.at[y - t, k], dst)

    def fv_via(row):
        t = {2: 1, 1: 0}[row]
        return rcopy(vsum.at[t], fvb, sem_fvb.at[0], sem_fvb.at[1], dev(row, x, k))

    def fv_own():
        return rcopy(vsum.at[y, other], rvy.at[0, k], sem_fv_s.at[y, other], sem_fv_r.at[0, k], partner)

    def fk_copy(d, c, src_core=None):
        xt = lax.rem(x + d, n)
        return rcopy(dk_part.at[y, at(xt * CORES + c, tokens)], rkx.at[d, k], sem_fk_s.at[d, c],
                     sem_fk_r.at[d, k if src_core is None else src_core], dev(y, xt, c))

    def fk_own(src_core=None):
        return rcopy(dk_part.at[y, at(x * CORES + other, tokens)], rkx.at[0, k], sem_fk_s.at[0, 0],
                     sem_fk_r.at[0, k if src_core is None else src_core], partner)

    def fk_quarter(xt):
        @pl.when(x != xt)
        def _():
            d = lax.rem(xt - x + n, n)
            for c in range(CORES):
                rcopy(dk_part.at[y, pl.ds(xt * blk + c * tokens, tokens)], rkx.at[d, k], sem_fk_s.at[d, c],
                      sem_fk_r.at[d, k], dev(y, xt, c)).start()

        @pl.when(x == xt)
        def _():
            fk_own().start()

    rb = 512

    def backward_tile(t):
        dva = None
        dka = None
        for s in range(CORES):
            for i in range(nrow // rb):
                rows = pl.ds(i * rb, rb)
                ls = lse[s, rows, :]
                dl = delta[s, rows, :]
                p = jnp.exp2(sbuf[t, s, rows, :] * c2 - jnp.concatenate([ls] * (tile // 128), axis=1))
                ds = (p * (dpbuf[t, s, rows, :] - jnp.concatenate([dl] * (tile // 128), axis=1))).astype(bf16)
                dsbuf[t, s, rows, :] = ds
                a = lax.dot_general(p.astype(bf16), dobuf[s, rows, :], tn, preferred_element_type=f32)
                dva = a if dva is None else dva + a
                a = lax.dot_general(ds, qbuf[s, rows, :], tn, preferred_element_type=f32)
                dka = a if dka is None else dka + a
        dv_part[t] = dva
        dk_part[t] = dka * scale

    def dv_order(i):
        t = i
        for r in range(n):
            if i < len(TILE_ORDER[r]):
                t = jnp.where(y == r, TILE_ORDER[r][i], t)
        return t

    def dv_turn(i):
        @pl.when(y >= i)
        def _():
            dv_combine(dv_order(i))

    for i in range(n):
        if i == 0:
            backward_tile(dv_order(0))

        @pl.when(y >= i)
        def _(i=i):
            t = dv_order(i)
            if i > 0:
                backward_tile(t)
            for m in ((0, 3, 1, 4) if i < 2 else (0, 3)):
                dv_copy(t, m).start()
            for r in range(n):
                if i < len(TILE_ORDER[r]):
                    @pl.when(y == r)
                    def _(r=r):
                        for j, m in enumerate(DK_MSGS):
                            if m[0] == r and m[1] == TILE_ORDER[r][i] and m[5] is None:
                                dk_copy(j).start()

        @pl.when(y < i)
        def _(i=i):
            dsbuf[i] = jnp.zeros(dsbuf.shape[1:], bf16)
            kbuf[i] = jnp.zeros(kbuf.shape[1:], bf16)

        if i == 0:
            orem.start()
        if i >= 2:
            if i == n - 1:
                dk_combine(0, (3,))
            dv_turn(i - 2)
        if i == n - 1:
            for j in range(2, n):
                @pl.when(y >= j)
                def _(j=j):
                    t = dv_order(j)
                    for m in (1, 4):
                        dv_copy(t, m).start()
    dk_combine(0, (0, 1, 2))

    def grad_query_half(s, dst):
        def dq_rows(i, carry):
            rows = at(i, rc)
            acc = None
            for t in range(n):
                a = jnp.dot(dsbuf[t, s, rows, :], kbuf[t], preferred_element_type=f32)
                acc = a if acc is None else acc + a
            acc = acc * scale
            for j in range(rc // heads):
                tok = i * (rc // heads) + j
                c = tabs[s, 0, pl.ds(tok, 1), :]
                sn = tabs[s, 1, pl.ds(tok, 1), :]
                g = acc[j * heads:(j + 1) * heads]
                r1, r2 = rot_halves(g[:, :half], g[:, half:], c, -sn)
                orow = at(tok, heads)
                dst[orow, :half] = r1.astype(bf16)
                dst[orow, half:] = r2.astype(bf16)
            return carry
        lax.fori_loop(0, nrow // rc, dq_rows, 0, unroll=2)
    grad_query_half(other, dqbuf)
    qrem = rcopy(dqbuf, dq_ref.at[k], sem_o.at[0, 1], sem_o.at[1, 1], partner)
    qrem.start()
    dk_combine(1, (0, 1, 2, 3))

    def dv_total(j):
        @pl.when(y >= j)
        def _():
            t = dv_order(j)
            for i in (1, 2, 4, 5):
                dv_copy(t, i).wait_recv()
            vsum[t, 0] = dv_part[t, at(x * CORES, tokens)] + rv[t, 2] + rv[t, 4]
            vsum[t, 1] = dv_part[t, at(x * CORES + 1, tokens)] + rv[t, 1] + rv[t, 5]
            for r, t_on, via in DV_VIA:
                @pl.when((y == r) & (t == t_on))
                def _(via=via):
                    fv_via(via).start()

            direct = y > t
            for r, t_on, via in DV_VIA:
                direct = direct & ((y != r) | (t != t_on)) & ((y != via) | (t != t_on))

            @pl.when(direct)
            def _():
                for c in range(CORES):
                    fv_copy(t, c).start()

    def dv_via(r, t_on):
        @pl.when(y == r)
        def _():
            fv_via(r).wait_recv()
            vsum[t_on] = vsum[t_on] + fvb[...]
            for c in range(CORES):
                fv_copy(t_on, c).start()

    def dk_final(part):
        for r in range(n - 1):
            @pl.when(y == r)
            def _(r=r):
                for qt, slots in DK_FINAL[r][2 * part:2 * part + 2]:
                    rows = pl.ds(qt * blk, blk)
                    acc = dk_part[r, rows]
                    for slot in slots:
                        dk_wait(slot)
                        acc = acc + rk[slot]
                    dk_part[r, rows] = acc
                    fk_quarter(qt)
    dv_turn(2)
    dv_total(0)
    dv_turn(3)

    @pl.when(y == n - 1)
    def _():
        for xt in range(n):
            fk_quarter(xt)
    dv_total(1)
    grad_query_half(k, dq_ref.at[k])
    dv_total(2)
    dv_total(3)
    fv_own().start()
    dk_final(0)
    for r, t_on, via in DV_VIA:
        dv_via(via, t_on)
    dk_final(1)
    def fv_wait(d, b):
        rcopy(rvy.at[d, b], rvy.at[d, b], sem_fv_s.at[0, 0], sem_fv_r.at[d, b], partner).wait_recv()

    fv_wait(0, other)
    rvy[0, k] = vsum[y, k]
    for d in range(1, n):
        expect = y + d < n
        for r, t_on, via in DV_VIA:
            if r - t_on == d:
                expect = expect & (y != t_on)

        @pl.when(expect)
        def _(d=d):
            for b in range(CORES):
                fv_wait(d, b)
                rvy[0, b] = rvy[0, b] + rvy[d, b]
    for b in range(CORES):
        gv_ref[b] = rvy[0, b].astype(bf16)
    fk_own(other).wait_recv()
    rkx[0, k] = dk_part[y, at(x * CORES + k, tokens)]
    for d in range(1, n):
        for b in range(CORES):
            fk_copy(d, 0, b).wait_recv()
    ct, st = tab_in[0], tab_in[1]
    for b in range(CORES):
        g = rkx[0, b] + rkx[1, b] + rkx[2, b] + rkx[3, b]
        r1, r2 = rot_halves(g[:, :half], g[:, half:], ct, -st)
        gk_ref[b, :, :half] = r1.astype(bf16)
        gk_ref[b, :, half:] = r2.astype(bf16)
    for cp in (pk, pv, pt, pq, pd):
        cp.wait_send()
    for d in range(1, n):
        for b in range(CORES):
            kx_copy(d, b).wait_send()
            fk_copy(d, b).wait_send()

        @pl.when(y + d < n)
        def _(d=d):
            for b in range(CORES):
                vy_copy(d, b).wait_send()
    fk_own().wait_send()
    fv_own().wait_send()
    for d in range(n):
        @pl.when(y - d >= 0)
        def _(d=d):
            for i in range(4):
                vx_copy(d, i).wait_send()
    for r in range(n):
        @pl.when(y == r)
        def _(r=r):
            for i, m in enumerate(KEY_MSGS):
                if m[0] == r:
                    key_copy(i).wait_send()
            for i, m in enumerate(DK_MSGS):
                if m[0] == r:
                    dk_copy(i).wait_send()
            if r == 0:
                for i in range(len(DK_RELAY)):
                    dk_relay(i).wait_send()
    for t in range(n):
        @pl.when(y >= t)
        def _(t=t):
            for i in range(6):
                dv_copy(t, i).wait_send()

        sent = y > t
        for r, t_on, via in DV_VIA:
            if t == t_on:
                sent = sent & (y != r)

        @pl.when(sent)
        def _(t=t):
            for c in range(CORES):
                fv_copy(t, c).wait_send()
    for r, t_on, via in DV_VIA:
        @pl.when(y == r)
        def _(via=via):
            fv_via(via).wait_send()
    orem.wait()
    qrem.wait()


def write_kernel(a, b, c, d, ao, bo, co, do, sem):
    pieces = 1
    cps = []
    for src, dst in ((a, ao), (b, bo)):
        rows = src.shape[1] // pieces
        for e in range(src.shape[0]):
            for i in range(pieces):
                at = (e, pl.ds(i * rows, rows))
                cps.append(pltpu.make_async_copy(src.at[at], dst.at[at], sem.at[len(cps)]))
    for src, dst in ((c, co), (d, do)):
        cps.append(pltpu.make_async_copy(src, dst, sem.at[len(cps)]))
    for cp in cps:
        cp.start()
    for cp in cps:
        cp.wait()


def solution(mesh):
    cp_size = mesh.shape['cp']
    n = SIDE
    assert cp_size == n * n * CORES
    query_spec = P('dp', 'cp', None, None)
    kv_spec = P('dp', 'cp', None)
    pos_spec = P(('dp', 'cp'))

    def per_device(query, key, value, positions, grad_out):
        batch, tokens, heads, head = query.shape
        nrow = tokens * heads
        q2 = query.reshape(batch, nrow, head)
        d2 = grad_out.reshape(batch, nrow, head)
        blk = CORES * tokens
        tile = n * blk
        bf16, f32 = jnp.bfloat16, jnp.float32
        V = pltpu.VMEM
        D = pltpu.SemaphoreType.DMA
        scratch = [
            pltpu.SMEM((tokens,), jnp.int32),
            V((tokens, head // 2), f32),
            V((batch, tokens, head), bf16),
            V((batch, tokens, head), bf16),
            V((2, tokens, head // 2), f32),
            V((CORES, 2, tokens, head // 2), f32),
            V((CORES, nrow, head), bf16),
            V((CORES, nrow, head), bf16),
            V((CORES, tokens, head), bf16),
            V((n, tile, head), bf16),
            V((n, tile, head), bf16),
            V((tile // 2, head), bf16),
            V((n, CORES, nrow, tile), f32),
            V((n, CORES, nrow, tile), f32),
            V((n, CORES, nrow, tile), bf16),
            V((CORES, nrow, 128), f32),
            V((CORES, nrow, 128), f32),
            V((CORES, nrow, 128), f32),
            V((CORES, nrow, 128), f32),
            V((CORES, nrow, head), f32),
            V((nrow, head), bf16),
            V((nrow, head), bf16),
            V((n, tile, head), f32),
            V((n, tile, head), f32),
            V((10, blk, head), f32),
            V((n, 6, tokens, head), f32),
            V((n, CORES, tokens, head), f32),
            V((CORES, tokens, head), f32),
            V((n, CORES, tokens, head), f32),
            V((n, CORES, tokens, head), f32),
            D((7,)), D((2, 5)), D((2, n - 1, CORES)), D((2, n - 1, CORES)), D((2, n, 4)),
            D((len(KEY_MSGS),)), D((4,)),
            D((n, 6)), D((n, 6)), D((len(DK_MSGS) + 2,)), D((10,)),
            D((n, CORES)), D((n, CORES)), D((n, CORES)), D((n, CORES)), D((2,)), D((2, 2)),
        ]
        vmem = pl.BlockSpec(memory_space=pltpu.VMEM)
        hbm = pl.BlockSpec(memory_space=pl.ANY)
        shapes = [jax.ShapeDtypeStruct(a.shape, bf16) for a in (q2, q2, key, value)]
        outs = pl.pallas_call(
            functools.partial(kernel, tokens, heads, head),
            out_shape=[pltpu.VMEM(a.shape, bf16) for a in (q2, q2, key, value)],
            in_specs=[hbm] * 5,
            out_specs=[vmem, vmem, vmem, vmem],
            scratch_shapes=scratch,
            compiler_params=pltpu.CompilerParams(collective_id=0, has_side_effects=True,
                                                 vmem_limit_bytes=58 * 1024 * 1024),
        )(positions, key, value, q2, d2)
        outs = pl.pallas_call(
            write_kernel, out_shape=shapes,
            in_specs=[vmem, vmem, vmem, vmem], out_specs=[hbm, hbm, hbm, hbm],
            scratch_shapes=[D((4 * 1 + 2,))],
        )(*[pltpu.with_memory_space_constraint(o, V) for o in outs])
        out, dq, gk, gv = outs
        return out.reshape(query.shape), dq.reshape(query.shape), gk, gv

    return jax.shard_map(per_device, mesh=mesh, in_specs=(query_spec, kv_spec, kv_spec, pos_spec, query_spec),
                         out_specs=(query_spec, query_spec, kv_spec, kv_spec), check_vma=False)
```

```python
import functools
import math

import jax
import jax.numpy as jnp
from jax import lax
from jax.experimental import pallas as pl
from jax.experimental.pallas import tpu as pltpu
from jax.sharding import PartitionSpec as P

ROPE_BASE = 10000
CORES = 2
SIDE = 4
LOG2E = math.log2(math.e)

KEY_MSGS = (
    (0, 0, 0, 1, 0, None), (0, 0, None, 3, 2, None), (0, 0, 1, 1, 1, None),
    (1, 1, 1, 0, 0, None), (1, 1, 0, 2, 0, None), (1, 1, 1, 2, 3, None),
    (2, 2, None, 3, 0, None),
    (0, 1, 1, 3, 3, 0), (1, 0, 0, 2, 1, 0), (1, 0, 1, 2, 2, 1), (2, 1, 0, 3, 1, 0),
)
KEY_SLOTS = {(1, 0): (0, 1), (2, 1): (0, 3), (2, 0): (1, 2), (3, 2): (0,), (3, 1): (1, 3), (3, 0): (2,)}

DK_MSGS = (
    (3, 1, 0, 2, 0, None, None), (3, 1, 2, 0, 0, None, None), (3, 1, 1, 2, 1, None, None), (3, 1, 3, 2, 6, None, None),
    (3, 0, 3, 0, 5, None, None),
    (3, 2, 0, 2, 2, None, None), (3, 2, 1, 2, 3, None, None), (3, 2, 2, 2, 4, None, None), (3, 2, 3, 2, 5, None, None),
    (2, 0, 3, 1, 0, None, None), (2, 0, 0, 3, 0, None, None), (2, 0, 1, 3, 1, None, None), (2, 0, 2, 3, 2, None, None),
    (2, 1, 2, 1, 3, None, None),
    (1, 0, 0, 0, 6, None, None), (1, 0, 1, 0, 7, None, None), (1, 0, 2, 0, 8, None, None),
    (3, 0, 0, 0, 2, 0, 0), (3, 0, 1, 0, 3, 1, 0), (3, 0, 2, 0, 4, 2, 1),
    (2, 1, 0, 1, 1, 0, 0), (2, 1, 1, 1, 2, 1, 1), (2, 1, 3, 1, 4, 6, 1), (1, 0, 3, 0, 9, 0, 0),
)
DK_RELAY = ((0, 5),)
DK_FINAL = {2: ((0, (2,)), (1, (3,)), (2, (4,)), (3, (5,))), 1: ((2, (3, 5)), (0, (1,)), (1, (2,)), (3, (4,))),
            0: ((3, (5, 9)), (0, (2, 6)), (1, (3, 7)), (2, (4, 8)))}
DV_VIA = ()
TILE_ORDER = {0: (0,), 1: (0, 1), 2: (0, 1, 2), 3: (1, 0, 2, 3)}


def rot_halves(x1, x2, c, s):
    return x1 * c - x2 * s, x2 * c + x1 * s


def kernel(tokens, heads, head,
           pos_hbm, key_hbm, val_hbm, q_hbm, do_hbm,
           out_ref, dq_ref, gk_ref, gv_ref,
           pos_ref, ang, key_in, val_in, tab_in, tabs, qbuf, dobuf, kst, kbuf, vbuf, krel, sbuf, dpbuf, dsbuf, mbuf, lbuf, lse, delta, oacc, obuf, dqbuf,
           dk_part, dv_part, rk, rv, vsum, fvb, rvy, rkx,
           sem_loc, sem_px, sem_kx, sem_vy, sem_vx, sem_ky_s, sem_ky_r,
           sem_dv_s, sem_dv_r, sem_dk_s, sem_dk_r, sem_fv_s, sem_fv_r, sem_fk_s, sem_fk_r, sem_fvb, sem_o):
    n = SIDE
    half = head // 2
    blk = CORES * tokens
    tile = n * blk
    ht = tile // 2
    nrow = tokens * heads
    scale = head ** -0.5
    c2 = scale * LOG2E
    f32, bf16 = jnp.float32, jnp.bfloat16
    me = lax.axis_index('cp')
    k = lax.rem(me, CORES)
    chip = lax.div(me, CORES)
    x = lax.rem(chip, n)
    y = lax.div(chip, n)
    other = 1 - k
    xr = lax.rem(x + 1, n)
    xo = lax.rem(x + 2, n)
    xl = lax.rem(x + 3, n)

    def dev(yy, xx, kk):
        return (yy * n + xx) * CORES + kk

    partner = dev(y, x, other)
    right, left = dev(y, xr, k), dev(y, xl, k)

    def rcopy(src, dst, ssem, rsem, target):
        return pltpu.make_async_remote_copy(src_ref=src, dst_ref=dst, send_sem=ssem, recv_sem=rsem,
                                            device_id={'cp': target}, device_id_type=pl.DeviceIdType.MESH)

    def at(i, size):
        return pl.ds(pl.multiple_of(i * size, size), size)
    bar = pltpu.get_barrier_semaphore()
    peers = [partner]
    for d in range(1, n):
        for b in range(CORES):
            peers.append(dev(y, lax.rem(x + d, n), b))
            peers.append(dev(lax.rem(y + d, n), x, b))
    for p in peers:
        pl.semaphore_signal(bar, inc=1, device_id={'cp': p}, device_id_type=pl.DeviceIdType.MESH)

    lf = pltpu.make_async_copy(pos_hbm, pos_ref, sem_loc.at[4])
    lk = pltpu.make_async_copy(key_hbm, key_in, sem_loc.at[5])
    lv = pltpu.make_async_copy(val_hbm, val_in, sem_loc.at[6])
    lq = pltpu.make_async_copy(q_hbm.at[k], qbuf.at[k], sem_loc.at[0])
    ld = pltpu.make_async_copy(do_hbm.at[k], dobuf.at[k], sem_loc.at[1])
    for cp in (lf, lk, lv, lq, ld):
        cp.start()

    pair = lax.broadcasted_iota(jnp.int32, (1, half), 1).astype(f32)
    freq = jnp.exp2(pair * (-2.0 * math.log2(ROPE_BASE) / head))
    lf.wait()
    for i in range(tokens):
        ang[pl.ds(i, 1), :] = jnp.full((1, half), pos_ref[i], jnp.int32).astype(f32)
    angles = ang[...] * freq
    tab_in[0] = jnp.cos(angles)
    tab_in[1] = jnp.sin(angles)

    lk.wait()
    lv.wait()
    for b in range(CORES):
        kf = key_in[b].astype(f32)
        r1, r2 = rot_halves(kf[:, :half], kf[:, half:], tab_in[0], tab_in[1])
        kst[b, :, :half] = r1.astype(bf16)
        kst[b, :, half:] = r2.astype(bf16)
    tabs[k] = tab_in[...]
    mine = at(x * CORES + k, tokens)
    kbuf[y, mine] = kst[k]
    vbuf[y, mine] = val_in[k]
    pl.semaphore_wait(bar, len(peers))
    pk = rcopy(kst.at[other], kbuf.at[y, mine], sem_px.at[0, 0], sem_px.at[1, 0], partner)
    pv = rcopy(val_in.at[other], vbuf.at[y, mine], sem_px.at[0, 1], sem_px.at[1, 1], partner)
    pt = rcopy(tab_in, tabs.at[k], sem_px.at[0, 2], sem_px.at[1, 2], partner)
    pq = rcopy(q_hbm.at[other], qbuf.at[k], sem_px.at[0, 3], sem_px.at[1, 3], partner)
    pd = rcopy(do_hbm.at[other], dobuf.at[k], sem_px.at[0, 4], sem_px.at[1, 4], partner)

    def kx_copy(d, b, src_core=None):
        return rcopy(kst.at[b], kbuf.at[y, mine], sem_kx.at[0, d - 1, b],
                     sem_kx.at[1, d - 1, k if src_core is None else src_core], dev(y, lax.rem(x + d, n), b))

    def vy_copy(d, b, src_core=None):
        return rcopy(val_in.at[b], vbuf.at[y, mine], sem_vy.at[0, d - 1, b],
                     sem_vy.at[1, d - 1, k if src_core is None else src_core], dev(lax.rem(y + d, n), x, b))

    pv.start()
    pk.start()
    for d in (2, 1, 3):
        for b in range(CORES):
            kx_copy(d, b).start()
    for d in (2, 1, 3):
        @pl.when(y + d < n)
        def _(d=d):
            for b in range(CORES):
                vy_copy(d, b).start()
    pt.start()
    pq.start()
    pd.start()

    def vx_copy(dy, i):
        t = lax.rem(y - dy + n, n)
        if i == 0:
            ref, target = vbuf.at[t, at(x, blk)], right
        elif i == 1:
            ref, target = vbuf.at[t, at(x, blk)], left
        elif i == 2:
            ref, target = vbuf.at[t, at(xl * CORES, tokens)], right
        else:
            ref, target = vbuf.at[t, at(xr * CORES + 1, tokens)], left
        return rcopy(ref, ref, sem_vx.at[0, dy, i], sem_vx.at[1, dy, i], target)

    def vx_relay(dy):
        vx_copy(dy, 0).wait_recv()
        vx_copy(dy, 2).start()
        vx_copy(dy, 1).wait_recv()
        vx_copy(dy, 3).start()

    def key_copy(i):
        src, t, hf, dst, slot, after = KEY_MSGS[i]
        ref = kbuf.at[t] if hf is None else kbuf.at[t, pl.ds(hf * ht, ht)]
        s_ref = krel if (src == 0 and after is not None) else ref
        d_ref = krel if dst == 0 else ref
        return rcopy(s_ref, d_ref, sem_ky_s.at[i], sem_ky_r.at[slot], dev(dst, x, k))

    def key_wait(row, slot):
        for i, m in enumerate(KEY_MSGS):
            if m[3] == row and m[4] == slot:
                key_copy(i).wait_recv()

    def rotate_queries(s):
        def rotate_rows(tok, carry):
            rows = at(tok, heads)
            c = tabs[s, 0, pl.ds(tok, 1), :]
            sn = tabs[s, 1, pl.ds(tok, 1), :]
            qf = qbuf[s, rows, :].astype(f32)
            r1, r2 = rot_halves(qf[:, :half], qf[:, half:], c, sn)
            qbuf[s, rows, :half] = r1.astype(bf16)
            qbuf[s, rows, half:] = r2.astype(bf16)
            return carry
        lax.fori_loop(0, tokens, rotate_rows, 0, unroll=8)
    pv.wait_recv()
    vx_copy(0, 0).start()
    vx_copy(0, 1).start()
    lq.wait()
    rotate_queries(k)
    for d in range(1, n):
        @pl.when(y - d >= 0)
        def _(d=d):
            for b in range(CORES):
                vy_copy(d, b, b).wait_recv()
            vx_copy(d, 0).start()
            vx_copy(d, 1).start()
    pt.wait_recv()
    pq.wait_recv()
    rotate_queries(other)
    vx_relay(0)
    pk.wait_recv()
    for d in range(1, n):
        for b in range(CORES):
            kx_copy(d, b, b).wait_recv()
    for r in range(n):
        @pl.when(y == r)
        def _(r=r):
            for i, m in enumerate(KEY_MSGS):
                if m[0] == r and m[5] is None:
                    key_copy(i).start()
    nt = (((1,), (1,)), ((), ()))
    tn = (((0,), (0,)), ((), ()))

    rf = 1024

    def first_scores(t):
        for s in range(CORES):
            sc = lax.dot_general(qbuf[s], kbuf[t], nt, preferred_element_type=f32)
            row_tok = (x * CORES + s) * tokens + lax.broadcasted_iota(jnp.int32, sc.shape, 0) // heads
            sc = jnp.where(lax.broadcasted_iota(jnp.int32, sc.shape, 1) <= row_tok, sc, -jnp.inf)
            sbuf[t, s] = sc
            mbuf[s] = jnp.broadcast_to(jnp.max(sc, axis=1, keepdims=True), (nrow, 128))

    def forward_tile(t, first):
        kt = kbuf.at[t]
        vt = vbuf.at[t]

        def rows_body(i, carry):
            for s in range(CORES):
                rows = at(i, rf)
                if first:
                    sc = sbuf[t, s, rows, :]
                    mx = mbuf[s, rows, :]
                else:
                    sc = lax.dot_general(qbuf[s, rows, :], kt[...], nt, preferred_element_type=f32)
                    sbuf[t, s, rows, :] = sc
                    old = mbuf[s, rows, :]
                    mx = jnp.maximum(old, jnp.max(sc, axis=1, keepdims=True))
                    fac = jnp.exp2((old - mx) * c2)
                    mbuf[s, rows, :] = mx
                mxw = jnp.concatenate([mx] * (tile // 128), axis=1)
                p = jnp.exp2((sc - mxw) * c2)
                tot = p[:, :128] + p[:, 128:]
                o = jnp.dot(p.astype(bf16), vt[...], preferred_element_type=f32)
                if not first:
                    tot = tot + lbuf[s, rows, :] * fac
                    o = o + oacc[s, rows, :] * jnp.concatenate([fac] * (head // 128), axis=1)
                lbuf[s, rows, :] = tot
                oacc[s, rows, :] = o
                dpbuf[t, s, rows, :] = lax.dot_general(dobuf[s, rows, :], vt[...], nt, preferred_element_type=f32)
            return carry
        if nrow == rf:
            rows_body(0, 0)
        else:
            lax.fori_loop(0, nrow // rf, rows_body, 0)
    first_scores(y)
    ld.wait()
    pd.wait_recv()
    for d in range(1, n):
        @pl.when(y - d >= 0)
        def _(d=d):
            vx_relay(d)
    vx_copy(0, 2).wait_recv()
    vx_copy(0, 3).wait_recv()
    forward_tile(y, True)
    for r in range(n - 1):
        @pl.when(y == r)
        def _(r=r):
            for i, m in enumerate(KEY_MSGS):
                if m[0] == r and m[5] is not None:
                    key_wait(r, m[5])
                    key_copy(i).start()
    for j, d in enumerate((1, n - 1, 2)):
        dd = jnp.where(y == n - 1, d, j + 1)

        @pl.when(y - (j + 1) >= 0)
        def _(j=j, d=d, dd=dd):
            t = y - dd
            for r in range(n):
                tr = r - (d if r == n - 1 else j + 1)
                if tr < 0:
                    continue

                @pl.when(y == r)
                def _(r=r, tr=tr):
                    for slot in KEY_SLOTS[(r, tr)]:
                        if not any(m[0] == r and m[5] == slot for m in KEY_MSGS):
                            key_wait(r, slot)
                    vx_copy(r - tr, 2).wait_recv()
                    vx_copy(r - tr, 3).wait_recv()
            forward_tile(t, False)
    rc = 256

    for i in range(nrow // rc):
        for s, dst in ((other, obuf), (k, out_ref.at[k])):
            rows = pl.ds(i * rc, rc)
            tot = jnp.sum(lbuf[s, rows, :], axis=1, keepdims=True)
            inv = 1.0 / tot
            ob = (oacc[s, rows, :] * inv).astype(bf16)
            dst[rows, :] = ob
            dl = jnp.sum(ob.astype(f32) * dobuf[s, rows, :].astype(f32), axis=1, keepdims=True)
            lse[s, rows, :] = mbuf[s, rows, :] * c2 + jnp.broadcast_to(jnp.log2(tot), (rc, 128))
            delta[s, rows, :] = jnp.broadcast_to(dl, (rc, 128))
    orem = rcopy(obuf, out_ref.at[k], sem_o.at[0, 0], sem_o.at[1, 0], partner)
    def dv_copy(t, i):
        xt = (xo, xr, xr, xo, xl, xl)[i]
        hf = (0, 1, 0, 1, 0, 1)[i]
        return rcopy(dv_part.at[t, at(xt * CORES + hf, tokens)], rv.at[t, i], sem_dv_s.at[t, i], sem_dv_r.at[t, i],
                     right if i < 3 else left)

    def dv_combine(t):
        for i in (0, 3):
            dv_copy(t, i).wait_recv()
            rows = at(xr * CORES, tokens) if i == 0 else at(xl * CORES + 1, tokens)
            dv_part[t, rows] = dv_part[t, rows] + rv[t, i]
            dv_copy(t, i + 2).start()

    def dk_copy(i):
        src, t, qt, dst, slot = DK_MSGS[i][:5]
        return rcopy(dk_part.at[t, pl.ds(qt * blk, blk)], rk.at[slot], sem_dk_s.at[i], sem_dk_r.at[slot], dev(dst, x, k))

    def dk_relay(i):
        src, dst = DK_RELAY[i]
        return rcopy(rk.at[src], rk.at[dst], sem_dk_s.at[len(DK_MSGS) + i], sem_dk_r.at[dst], dev(1, x, k))

    def dk_wait(slot):
        rcopy(rk.at[slot], rk.at[slot], sem_dk_s.at[0], sem_dk_r.at[slot], partner).wait_recv()

    def dk_combine(e, rows_here):
        if 0 in rows_here and e < len(DK_RELAY):
            @pl.when(y == 0)
            def _():
                dk_wait(DK_RELAY[e][0])
                dk_relay(e).start()
        for r in range(1, n):
            if r not in rows_here:
                continue
            @pl.when(y == r)
            def _(r=r):
                for i, m in enumerate(DK_MSGS):
                    if m[0] == r and m[6] == e:
                        dk_wait(m[5])
                        rows = pl.ds(m[2] * blk, blk)
                        dk_part[m[1], rows] = dk_part[m[1], rows] + rk[m[5]]
                        dk_copy(i).start()

    def fv_copy(t, c):
        dst = dev(t, x, c)
        return rcopy(vsum.at[t, c], rvy.at[y - t, k], sem_fv_s.at[t, c], sem_fv_r.at[y - t, k], dst)

    def fv_via(row):
        t = {2: 1, 1: 0}[row]
        return rcopy(vsum.at[t], fvb, sem_fvb.at[0], sem_fvb.at[1], dev(row, x, k))

    def fv_own():
        return rcopy(vsum.at[y, other], rvy.at[0, k], sem_fv_s.at[y, other], sem_fv_r.at[0, k], partner)

    def fk_copy(d, c, src_core=None):
        xt = lax.rem(x + d, n)
        return rcopy(dk_part.at[y, at(xt * CORES + c, tokens)], rkx.at[d, k], sem_fk_s.at[d, c],
                     sem_fk_r.at[d, k if src_core is None else src_core], dev(y, xt, c))

    def fk_own(src_core=None):
        return rcopy(dk_part.at[y, at(x * CORES + other, tokens)], rkx.at[0, k], sem_fk_s.at[0, 0],
                     sem_fk_r.at[0, k if src_core is None else src_core], partner)

    def fk_quarter(xt):
        @pl.when(x != xt)
        def _():
            d = lax.rem(xt - x + n, n)
            for c in range(CORES):
                rcopy(dk_part.at[y, pl.ds(xt * blk + c * tokens, tokens)], rkx.at[d, k], sem_fk_s.at[d, c],
                      sem_fk_r.at[d, k], dev(y, xt, c)).start()

        @pl.when(x == xt)
        def _():
            fk_own().start()

    rb = 512

    def backward_tile(t):
        dva = None
        dka = None
        for s in range(CORES):
            for i in range(nrow // rb):
                rows = pl.ds(i * rb, rb)
                ls = lse[s, rows, :]
                dl = delta[s, rows, :]
                p = jnp.exp2(sbuf[t, s, rows, :] * c2 - jnp.concatenate([ls] * (tile // 128), axis=1))
                ds = (p * (dpbuf[t, s, rows, :] - jnp.concatenate([dl] * (tile // 128), axis=1))).astype(bf16)
                dsbuf[t, s, rows, :] = ds
                a = lax.dot_general(p.astype(bf16), dobuf[s, rows, :], tn, preferred_element_type=f32)
                dva = a if dva is None else dva + a
                a = lax.dot_general(ds, qbuf[s, rows, :], tn, preferred_element_type=f32)
                dka = a if dka is None else dka + a
        dv_part[t] = dva
        dk_part[t] = dka * scale

    def dv_order(i):
        t = i
        for r in range(n):
            if i < len(TILE_ORDER[r]):
                t = jnp.where(y == r, TILE_ORDER[r][i], t)
        return t

    def dv_turn(i):
        @pl.when(y >= i)
        def _():
            dv_combine(dv_order(i))

    for i in range(n):
        if i == 0:
            backward_tile(dv_order(0))

        @pl.when(y >= i)
        def _(i=i):
            t = dv_order(i)
            if i > 0:
                backward_tile(t)
            for m in ((0, 3, 1, 4) if i < 2 else (0, 3)):
                dv_copy(t, m).start()
            for r in range(n):
                if i < len(TILE_ORDER[r]):
                    @pl.when(y == r)
                    def _(r=r):
                        for j, m in enumerate(DK_MSGS):
                            if m[0] == r and m[1] == TILE_ORDER[r][i] and m[5] is None:
                                dk_copy(j).start()

        @pl.when(y < i)
        def _(i=i):
            dsbuf[i] = jnp.zeros(dsbuf.shape[1:], bf16)
            kbuf[i] = jnp.zeros(kbuf.shape[1:], bf16)

        if i == 0:
            orem.start()
        if i >= 2:
            if i == n - 1:
                dk_combine(0, (3,))
            dv_turn(i - 2)
        if i == n - 1:
            for j in range(2, n):
                @pl.when(y >= j)
                def _(j=j):
                    t = dv_order(j)
                    for m in (1, 4):
                        dv_copy(t, m).start()
    dk_combine(0, (0, 1, 2))

    def grad_query_half(s, dst):
        def dq_rows(i, carry):
            rows = at(i, rc)
            acc = None
            for t in range(n):
                a = jnp.dot(dsbuf[t, s, rows, :], kbuf[t], preferred_element_type=f32)
                acc = a if acc is None else acc + a
            acc = acc * scale
            for j in range(rc // heads):
                tok = i * (rc // heads) + j
                c = tabs[s, 0, pl.ds(tok, 1), :]
                sn = tabs[s, 1, pl.ds(tok, 1), :]
                g = acc[j * heads:(j + 1) * heads]
                r1, r2 = rot_halves(g[:, :half], g[:, half:], c, -sn)
                orow = at(tok, heads)
                dst[orow, :half] = r1.astype(bf16)
                dst[orow, half:] = r2.astype(bf16)
            return carry
        lax.fori_loop(0, nrow // rc, dq_rows, 0, unroll=2)
    grad_query_half(other, dqbuf)
    qrem = rcopy(dqbuf, dq_ref.at[k], sem_o.at[0, 1], sem_o.at[1, 1], partner)
    qrem.start()
    dk_combine(1, (0, 1, 2, 3))

    def dv_total(j):
        @pl.when(y >= j)
        def _():
            t = dv_order(j)
            for i in (1, 2, 4, 5):
                dv_copy(t, i).wait_recv()
            vsum[t, 0] = dv_part[t, at(x * CORES, tokens)] + rv[t, 2] + rv[t, 4]
            vsum[t, 1] = dv_part[t, at(x * CORES + 1, tokens)] + rv[t, 1] + rv[t, 5]
            for r, t_on, via in DV_VIA:
                @pl.when((y == r) & (t == t_on))
                def _(via=via):
                    fv_via(via).start()

            direct = y > t
            for r, t_on, via in DV_VIA:
                direct = direct & ((y != r) | (t != t_on)) & ((y != via) | (t != t_on))

            @pl.when(direct)
            def _():
                for c in range(CORES):
                    fv_copy(t, c).start()

    def dv_via(r, t_on):
        @pl.when(y == r)
        def _():
            fv_via(r).wait_recv()
            vsum[t_on] = vsum[t_on] + fvb[...]
            for c in range(CORES):
                fv_copy(t_on, c).start()

    def dk_final(part):
        for r in range(n - 1):
            @pl.when(y == r)
            def _(r=r):
                for qt, slots in DK_FINAL[r][2 * part:2 * part + 2]:
                    rows = pl.ds(qt * blk, blk)
                    acc = dk_part[r, rows]
                    for slot in slots:
                        dk_wait(slot)
                        acc = acc + rk[slot]
                    dk_part[r, rows] = acc
                    fk_quarter(qt)
    dv_turn(2)
    dv_total(0)
    dv_turn(3)
    dv_total(1)
    grad_query_half(k, dq_ref.at[k])
    dv_total(2)
    dv_total(3)
    fv_own().start()

    @pl.when(y == n - 1)
    def _():
        for xt in range(n):
            fk_quarter(xt)
    dk_final(0)
    for r, t_on, via in DV_VIA:
        dv_via(via, t_on)
    dk_final(1)
    def fv_wait(d, b):
        rcopy(rvy.at[d, b], rvy.at[d, b], sem_fv_s.at[0, 0], sem_fv_r.at[d, b], partner).wait_recv()

    fv_wait(0, other)
    rvy[0, k] = vsum[y, k]
    for d in range(1, n):
        expect = y + d < n
        for r, t_on, via in DV_VIA:
            if r - t_on == d:
                expect = expect & (y != t_on)

        @pl.when(expect)
        def _(d=d):
            for b in range(CORES):
                fv_wait(d, b)
                rvy[0, b] = rvy[0, b] + rvy[d, b]
    for b in range(CORES):
        gv_ref[b] = rvy[0, b].astype(bf16)
    fk_own(other).wait_recv()
    rkx[0, k] = dk_part[y, at(x * CORES + k, tokens)]
    for d in range(1, n):
        for b in range(CORES):
            fk_copy(d, 0, b).wait_recv()
    ct, st = tab_in[0], tab_in[1]
    for b in range(CORES):
        g = rkx[0, b] + rkx[1, b] + rkx[2, b] + rkx[3, b]
        r1, r2 = rot_halves(g[:, :half], g[:, half:], ct, -st)
        gk_ref[b, :, :half] = r1.astype(bf16)
        gk_ref[b, :, half:] = r2.astype(bf16)
    for cp in (pk, pv, pt, pq, pd):
        cp.wait_send()
    for d in range(1, n):
        for b in range(CORES):
            kx_copy(d, b).wait_send()
            fk_copy(d, b).wait_send()

        @pl.when(y + d < n)
        def _(d=d):
            for b in range(CORES):
                vy_copy(d, b).wait_send()
    fk_own().wait_send()
    fv_own().wait_send()
    for d in range(n):
        @pl.when(y - d >= 0)
        def _(d=d):
            for i in range(4):
                vx_copy(d, i).wait_send()
    for r in range(n):
        @pl.when(y == r)
        def _(r=r):
            for i, m in enumerate(KEY_MSGS):
                if m[0] == r:
                    key_copy(i).wait_send()
            for i, m in enumerate(DK_MSGS):
                if m[0] == r:
                    dk_copy(i).wait_send()
            if r == 0:
                for i in range(len(DK_RELAY)):
                    dk_relay(i).wait_send()
    for t in range(n):
        @pl.when(y >= t)
        def _(t=t):
            for i in range(6):
                dv_copy(t, i).wait_send()

        sent = y > t
        for r, t_on, via in DV_VIA:
            if t == t_on:
                sent = sent & (y != r)

        @pl.when(sent)
        def _(t=t):
            for c in range(CORES):
                fv_copy(t, c).wait_send()
    for r, t_on, via in DV_VIA:
        @pl.when(y == r)
        def _(via=via):
            fv_via(via).wait_send()
    orem.wait()
    qrem.wait()


def write_kernel(a, b, c, d, ao, bo, co, do, sem):
    pieces = 1
    cps = []
    for src, dst in ((a, ao), (b, bo)):
        rows = src.shape[1] // pieces
        for e in range(src.shape[0]):
            for i in range(pieces):
                at = (e, pl.ds(i * rows, rows))
                cps.append(pltpu.make_async_copy(src.at[at], dst.at[at], sem.at[len(cps)]))
    for src, dst in ((c, co), (d, do)):
        cps.append(pltpu.make_async_copy(src, dst, sem.at[len(cps)]))
    for cp in cps:
        cp.start()
    for cp in cps:
        cp.wait()


def solution(mesh):
    cp_size = mesh.shape['cp']
    n = SIDE
    assert cp_size == n * n * CORES
    query_spec = P('dp', 'cp', None, None)
    kv_spec = P('dp', 'cp', None)
    pos_spec = P(('dp', 'cp'))

    def per_device(query, key, value, positions, grad_out):
        batch, tokens, heads, head = query.shape
        nrow = tokens * heads
        q2 = query.reshape(batch, nrow, head)
        d2 = grad_out.reshape(batch, nrow, head)
        blk = CORES * tokens
        tile = n * blk
        bf16, f32 = jnp.bfloat16, jnp.float32
        V = pltpu.VMEM
        D = pltpu.SemaphoreType.DMA
        scratch = [
            pltpu.SMEM((tokens,), jnp.int32),
            V((tokens, head // 2), f32),
            V((batch, tokens, head), bf16),
            V((batch, tokens, head), bf16),
            V((2, tokens, head // 2), f32),
            V((CORES, 2, tokens, head // 2), f32),
            V((CORES, nrow, head), bf16),
            V((CORES, nrow, head), bf16),
            V((CORES, tokens, head), bf16),
            V((n, tile, head), bf16),
            V((n, tile, head), bf16),
            V((tile // 2, head), bf16),
            V((n, CORES, nrow, tile), f32),
            V((n, CORES, nrow, tile), f32),
            V((n, CORES, nrow, tile), bf16),
            V((CORES, nrow, 128), f32),
            V((CORES, nrow, 128), f32),
            V((CORES, nrow, 128), f32),
            V((CORES, nrow, 128), f32),
            V((CORES, nrow, head), f32),
            V((nrow, head), bf16),
            V((nrow, head), bf16),
            V((n, tile, head), f32),
            V((n, tile, head), f32),
            V((10, blk, head), f32),
            V((n, 6, tokens, head), f32),
            V((n, CORES, tokens, head), f32),
            V((CORES, tokens, head), f32),
            V((n, CORES, tokens, head), f32),
            V((n, CORES, tokens, head), f32),
            D((7,)), D((2, 5)), D((2, n - 1, CORES)), D((2, n - 1, CORES)), D((2, n, 4)),
            D((len(KEY_MSGS),)), D((4,)),
            D((n, 6)), D((n, 6)), D((len(DK_MSGS) + 2,)), D((10,)),
            D((n, CORES)), D((n, CORES)), D((n, CORES)), D((n, CORES)), D((2,)), D((2, 2)),
        ]
        vmem = pl.BlockSpec(memory_space=pltpu.VMEM)
        hbm = pl.BlockSpec(memory_space=pl.ANY)
        shapes = [jax.ShapeDtypeStruct(a.shape, bf16) for a in (q2, q2, key, value)]
        outs = pl.pallas_call(
            functools.partial(kernel, tokens, heads, head),
            out_shape=[pltpu.VMEM(a.shape, bf16) for a in (q2, q2, key, value)],
            in_specs=[hbm] * 5,
            out_specs=[vmem, vmem, vmem, vmem],
            scratch_shapes=scratch,
            compiler_params=pltpu.CompilerParams(collective_id=0, has_side_effects=True,
                                                 vmem_limit_bytes=58 * 1024 * 1024),
        )(positions, key, value, q2, d2)
        outs = pl.pallas_call(
            write_kernel, out_shape=shapes,
            in_specs=[vmem, vmem, vmem, vmem], out_specs=[hbm, hbm, hbm, hbm],
            scratch_shapes=[D((4 * 1 + 2,))],
        )(*[pltpu.with_memory_space_constraint(o, V) for o in outs])
        out, dq, gk, gv = outs
        return out.reshape(query.shape), dq.reshape(query.shape), gk, gv

    return jax.shard_map(per_device, mesh=mesh, in_specs=(query_spec, kv_spec, kv_spec, pos_spec, query_spec),
                         out_specs=(query_spec, query_spec, kv_spec, kv_spec), check_vma=False)
```
